32 devices in a mesh: data: 8 (over z, y), model: 4 (over x, core).
Axes of the slice: x: 2, y: 2, z: 4, core: 2. Of those that a mesh axis runs over, the one named last changes fastest.
Arguments:
- tokens: bfloat16 [12288, 2048], P('data')
- w_query: bfloat16 [2048, 2048], P('data', 'model')
- w_kv: bfloat16 [2048, 512], P('data')
- w_out: bfloat16 [2048, 2048], P('model', 'data')
- ln_gain: float32 [2048], replicated
- positions: int32 [128], replicated
- grad_out: bfloat16 [12288, 2048], P('data')
Outputs:
- output 1: bfloat16 [12288, 2048], P('data')
- output 2: bfloat16 [12288, 2048], P('data')
- output 3: bfloat16 [2048, 2048], P('data', 'model')
- output 4: bfloat16 [2048, 512], P('data')
- output 5: bfloat16 [2048, 2048], P('model', 'data')
All inputs are finite; a program needn't handle non-finite values.
Results may differ from the reference program's by a relative error of at most 0.0139353.
Values are sent between devices in bfloat16 or wider.
A program may use at most 1 GiB of HBM per device.

```python
import jax
import jax.numpy as jnp
from jax import lax

D = 2048
HEADS = 8
HEAD = 256
SEQ_LEN = 128
SEQ_COUNT = 96
NORM_EPS = 1e-6
TOTAL_TOK = SEQ_COUNT * SEQ_LEN


def setup_inputs(seed: int = 0) -> dict:
    keys = jax.random.split(jax.random.key(seed), 7)
    out_scale = (SEQ_LEN / (16.0 * HEADS * HEAD)) ** 0.5
    tokens = jax.random.normal(keys[0], (TOTAL_TOK, D), jnp.float32)
    w_query = jax.random.normal(keys[1], (D, HEADS * HEAD), jnp.float32) * D ** -0.5
    w_kv = jax.random.normal(keys[2], (D, 2 * HEAD), jnp.float32) * D ** -0.5
    w_out = jax.random.normal(keys[3], (HEADS * HEAD, D), jnp.float32) * out_scale
    ln_gain = jax.random.uniform(keys[4], (D,), jnp.float32, 0.5, 1.5)
    positions = jax.random.permutation(keys[5], SEQ_LEN).astype(jnp.int32)
    grad_out = jax.random.normal(keys[6], (TOTAL_TOK, D), jnp.float32)
    return {
        "tokens": tokens.astype(jnp.bfloat16),
        "w_query": w_query.astype(jnp.bfloat16),
        "w_kv": w_kv.astype(jnp.bfloat16),
        "w_out": w_out.astype(jnp.bfloat16),
        "ln_gain": ln_gain,
        "positions": positions,
        "grad_out": grad_out.astype(jnp.bfloat16),
    }


def reference(tokens, w_query, w_kv, w_out, ln_gain, positions, grad_out):
    visible = positions[None, :] <= positions[:, None]
    score_scale = HEAD ** -0.5

    def attend_one(pair):
        q_seq, kv_seq = pair
        scores = jnp.einsum("qhe,ke->hqk", q_seq.astype(jnp.float32), kv_seq[:, :HEAD].astype(jnp.float32)) * score_scale
        probs = jax.nn.softmax(jnp.where(visible[None], scores, -1e30), axis=-1).astype(jnp.bfloat16)
        mixed = jnp.einsum("hqk,ke->qhe", probs.astype(jnp.float32), kv_seq[:, HEAD:].astype(jnp.float32))
        return mixed.astype(jnp.bfloat16)

    def forward(tok_rows, q_weight, kv_weight, o_weight):
        rows_f = tok_rows.astype(jnp.float32)
        centred = rows_f - jnp.mean(rows_f, axis=-1, keepdims=True)
        inv_std = lax.rsqrt(jnp.mean(centred * centred, axis=-1, keepdims=True) + NORM_EPS)
        hidden = (centred * inv_std * ln_gain).astype(jnp.bfloat16)
        queries = jnp.dot(hidden, q_weight, preferred_element_type=jnp.float32).astype(jnp.bfloat16)
        key_vals = jnp.dot(hidden, kv_weight, preferred_element_type=jnp.float32).astype(jnp.bfloat16)
        mixed = lax.map(jax.checkpoint(attend_one), (queries.reshape(SEQ_COUNT, SEQ_LEN, HEADS, HEAD), key_vals.reshape(SEQ_COUNT, SEQ_LEN, 2 * HEAD)))
        mixed = mixed.reshape(TOTAL_TOK, HEADS * HEAD)
        return jnp.dot(mixed, o_weight, preferred_element_type=jnp.float32).astype(jnp.bfloat16)

    result, pullback = jax.vjp(forward, tokens, w_query, w_kv, w_out)
    grad_tokens, grad_query, grad_kv, grad_o = pullback(grad_out)
    return (result, grad_tokens, grad_query, grad_kv, grad_o)
```

```python
import functools

import jax
import jax.numpy as jnp
from jax import lax
from jax.experimental import pallas as pl
from jax.experimental.pallas import tpu as pltpu
from jax.sharding import PartitionSpec as P

NORM_EPS = 1e-6
ROWS = 512
BF = jnp.bfloat16
F32 = jnp.float32


def dot(a, b):
    return jnp.dot(a, b, preferred_element_type=F32)


def dot_t(a, b):
    return lax.dot_general(a, b, (((1,), (1,)), ((), ())), preferred_element_type=F32)


def t_dot(a, b):
    return lax.dot_general(a, b, (((0,), (0,)), ((), ())), preferred_element_type=F32)


def at(offs, p):
    return pl.ds(pl.multiple_of(offs[p], 256), 256)


def softmax(q, k, mask):
    s = dot_t(q, k) * (q.shape[-1] ** -0.5)
    s = jnp.where(mask > 0, s, -1e30)
    e = jnp.exp(s - jnp.max(s, axis=-1, keepdims=True))
    return e / jnp.sum(e, axis=-1, keepdims=True)


def fwd_tile(q_ref, k_ref, v_ref, mask, o_ref):
    for b in range(ROWS // 128):
        r = slice(b * 128, (b + 1) * 128)
        k, v = k_ref[r, :], v_ref[r, :]
        for h in range(2):
            c = slice(h * 256, (h + 1) * 256)
            o_ref[r, c] = dot(softmax(q_ref[r, c], k, mask).astype(BF), v).astype(BF)


def bwd_tile(q_ref, k_ref, v_ref, do_ref, mask, dq_ref, dkv_ref, add_ref=None):
    for b in range(ROWS // 128):
        r = slice(b * 128, (b + 1) * 128)
        k, v = k_ref[r, :], v_ref[r, :]
        dk = dv = None
        for h in range(2):
            c = slice(h * 256, (h + 1) * 256)
            q, do = q_ref[r, c], do_ref[r, c]
            p = softmax(q, k, mask)
            dp = dot_t(do, v)
            ds = p * (dp - jnp.sum(p * dp, axis=-1, keepdims=True))
            ds = (ds * (256 ** -0.5)).astype(BF)
            dq_ref[r, c] = dot(ds, k).astype(BF)
            dkh, dvh = t_dot(ds, q), t_dot(p.astype(BF), do)
            dk = dkh if dk is None else dk + dkh
            dv = dvh if dv is None else dv + dvh
        if add_ref is not None:
            dk = dk + add_ref[r, :256]
            dv = dv + add_ref[r, 256:]
        dkv_ref[r, :256] = dk
        dkv_ref[r, 256:] = dv


def fwd_kernel(offs, x_ref, g_ref, wa_ref, wb_ref, mask_ref, h_ref, q_ref, k_ref, v_ref, o_ref):
    x = x_ref[...].astype(F32)
    c = x - jnp.mean(x, axis=-1, keepdims=True)
    inv = lax.rsqrt(jnp.mean(c * c, axis=-1, keepdims=True) + NORM_EPS)
    h_ref[...] = (c * inv * g_ref[...]).astype(BF)
    qa = kva = kvb = 0.0
    for p in range(8):
        hp = h_ref[:, at(offs, p)]
        qa = qa + dot(hp, wa_ref[p, :, :512])
        kva = kva + dot(hp, wa_ref[p, :, 512:])
        kvb = kvb + dot(hp, wb_ref[p])
    q_ref[...] = qa.astype(BF)
    first = offs[8] == 0
    k_ref[...] = jnp.where(first, kva, kvb).astype(BF)
    v_ref[...] = jnp.where(first, kvb, kva).astype(BF)
    fwd_tile(q_ref, k_ref, v_ref, mask_ref[...], o_ref)


def bwd_kernel(offs, dy_ref, wo_ref, q_ref, k_ref, v_ref, mask_ref, dq_ref, dkv_ref, do_ref):
    acc = 0.0
    for p in range(8):
        acc = acc + dot_t(dy_ref[:, at(offs, p)], wo_ref[p])
    do_ref[...] = acc.astype(BF)
    bwd_tile(q_ref, k_ref, v_ref, do_ref, mask_ref[...], dq_ref, dkv_ref)


def mirror_kernel(offs, h_ref, dy_ref, wa_ref, wo_ref, k_ref, v_ref, add_ref, mask_ref, o_ref, dq_ref, dkv_ref, q_ref, do_ref):
    qa = acc = 0.0
    for p in range(8):
        qa = qa + dot(h_ref[:, at(offs, p)], wa_ref[p, :, :512])
    q_ref[...] = qa.astype(BF)
    for p in range(8):
        acc = acc + dot_t(dy_ref[:, at(offs, p)], wo_ref[p])
    do_ref[...] = acc.astype(BF)
    fwd_tile(q_ref, k_ref, v_ref, mask_ref[...], o_ref)
    bwd_tile(q_ref, k_ref, v_ref, do_ref, mask_ref[...], dq_ref, dkv_ref, add_ref)


def wo_grad_kernel(offs, o_ref, dy_ref, *outs):
    step = pl.program_id(0)
    ot = o_ref[...].T
    for p, out in enumerate(outs):
        part = dot(ot, dy_ref[:, at(offs, p)])

        @pl.when(step == 0)
        def _():
            out[...] = part

        @pl.when(step > 0)
        def _():
            out[...] += part


def in_grad_kernel(offs, h_ref, b_ref, *outs):
    step = pl.program_id(0)
    b = b_ref[...]
    for p, out in enumerate(outs):
        part = t_dot(h_ref[:, at(offs, p)], b)

        @pl.when(step == 0)
        def _():
            out[...] = part

        @pl.when(step > 0)
        def _():
            out[...] += part


def load_canonical(me, srcs, scr, sem, width=None):
    copies = []
    for r, s in enumerate(srcs):
        sub = me // 2 * 2 if r < 2 else 2 - me // 2 * 2
        idx = sub + (me % 2 if r % 2 == 0 else 1 - me % 2)
        src = s if width is None else s.at[:, :, pl.ds(0, width)]
        copies.append(pltpu.make_async_copy(src, scr.at[idx], sem.at[r]))
    for c in copies:
        c.start()
    for c in copies:
        c.wait()


def canon(me, refs, scr):
    for r, s in enumerate(refs):
        sub = me // 2 * 2 if r < 2 else 2 - me // 2 * 2
        idx = sub + (me % 2 if r % 2 == 0 else 1 - me % 2)
        scr[idx] = s[...]


def y_kernel(offs, o0, o1, o2, o3, w0, w1, w2, w3, y_ref, wscr, oscr, sem):
    me = offs[9]

    @pl.when(pl.program_id(0) == 0)
    def _():
        load_canonical(me, (w0, w1, w2, w3), wscr, sem)

    canon(me, (o0, o1, o2, o3), oscr)
    for p in range(8):
        acc = 0.0
        for m in range(4):
            acc = acc + dot(oscr[m], wscr[m, p])
        y_ref[:, at(offs, p)] = acc.astype(BF)


def dx_kernel(offs, x_ref, g_ref, d0, d1, d2, d3, dkv_ref, w0, w1, w2, w3, wb_ref, dx_ref, wscr, dscr, gh, sem):
    me = offs[9]

    @pl.when(pl.program_id(0) == 0)
    def _():
        load_canonical(me, (w0, w1, w2, w3), wscr, sem, 512)

    canon(me, (d0, d1, d2, d3), dscr)
    for p in range(8):
        acc = 0.0
        for m in range(4):
            acc = acc + dot_t(dscr[m], wscr[m, p])
        acc = acc + dot_t(dkv_ref[...], wb_ref[p])
        gh[:, at(offs, p)] = acc
    x = x_ref[...].astype(F32)
    c = x - jnp.mean(x, axis=-1, keepdims=True)
    inv = lax.rsqrt(jnp.mean(c * c, axis=-1, keepdims=True) + NORM_EPS)
    n = c * inv
    gn = gh[...] * g_ref[...]
    dx = inv * (gn - jnp.mean(gn, axis=-1, keepdims=True) - n * jnp.mean(gn * n, axis=-1, keepdims=True))
    dx_ref[...] = dx.astype(BF)


SMEM = pl.BlockSpec(memory_space=pltpu.SMEM)
ANY = pl.BlockSpec(memory_space=pl.ANY)


def tile(width, rows=ROWS):
    return pl.BlockSpec((rows, width), lambda i: (i, 0))


def whole(*shape):
    return pl.BlockSpec(shape, lambda i: (0,) * len(shape))


def call(kernel, name, toks, in_specs, outs, flops, scratch=(), rows=ROWS):
    shapes = [s for s, _ in outs]
    specs = [b for _, b in outs]
    return pl.pallas_call(
        kernel,
        name=name,
        grid=(toks // rows,),
        in_specs=[SMEM] + in_specs,
        out_specs=specs,
        out_shape=shapes,
        scratch_shapes=list(scratch),
        cost_estimate=pl.CostEstimate(flops=flops, bytes_accessed=20_000_000, transcendentals=0),
        compiler_params=pltpu.CompilerParams(dimension_semantics=("arbitrary",), vmem_limit_bytes=60 * 2**20),
    )


def solution(mesh):
    def zshift(a, k):
        return lax.ppermute(a, "data", [(i, (i + 2 * k) % 8) for i in range(8)])

    def yswap(a):
        return lax.ppermute(a, "data", [(i, i ^ 1) for i in range(8)])

    def xswap(a):
        return lax.ppermute(a, "model", [(i, i ^ 2) for i in range(4)])

    def cswap(a):
        return lax.ppermute(a, "model", [(i, i ^ 1) for i in range(4)])

    def gather(shard):
        near = [shard] + [zshift(shard, -k) for k in (1, 2, 3)]
        far = [yswap(a) for a in near]
        return jnp.stack(near + far)

    def reduce(pieces):
        near, far = pieces[:4], pieces[4:]
        total = {}
        for k in (1, 2, 3, 0):
            total[k] = near[k] + yswap(far[k])
        got = [zshift(total[k], k) for k in (1, 2, 3)]
        return (total[0] + got[0] + got[1] + got[2]).astype(BF)

    def device_step(x, wq, wkv, wo, gain, positions, dy):
        toks = x.shape[0]
        d, m = lax.axis_index("data"), lax.axis_index("model")
        z, y = d // 2, d % 2
        core = m % 2
        offs = [(((z + k) % 4) * 2 + (y + j) % 2) * 256 for j in (0, 1) for k in range(4)]
        offs = jnp.stack([*offs, core, m]).astype(jnp.int32)
        mask = (positions[None, :] <= positions[:, None]).astype(F32)
        gain2 = gain.reshape(1, -1)
        sd = jax.ShapeDtypeStruct

        kv_half = lax.dynamic_slice_in_dim(wkv, core * 256, 256, axis=1)
        wa = gather(jnp.concatenate([wq, kv_half], axis=1))
        wb = cswap(wa[:, :, 512:])
        wos = gather(wo)

        act = lambda w, dt=BF: (sd((toks, w), dt), tile(w))
        h, q, k, v, o = call(
            fwd_kernel, "fwd", toks,
            [tile(2048), whole(1, 2048), whole(8, 256, 768), whole(8, 256, 256), whole(128, 128)],
            [act(2048), act(512), act(256), act(256), act(512)], 8_000_000_000,
        )(offs, x, gain2, wa, wb, mask)

        gouts = lambda r, c: [(sd((r, c), F32), whole(r, c))] * 8
        wo_pieces = call(wo_grad_kernel, "wo_grad", toks, [tile(512), tile(2048)], gouts(512, 256), 3_300_000_000)(offs, o, dy)
        g_wo = reduce(wo_pieces)

        dq, dkv1 = call(
            bwd_kernel, "bwd", toks,
            [tile(2048), whole(8, 512, 256), tile(512), tile(256), tile(256), whole(128, 128)],
            [act(512), act(512, F32)], 8_000_000_000, [pltpu.VMEM((ROWS, 512), BF)],
        )(offs, dy, wos, q, k, v, mask)
        wq_pieces = call(in_grad_kernel, "wq_grad", toks, [tile(2048), tile(512)], gouts(256, 512), 3_300_000_000)(offs, h, dq)
        g_wq = reduce(wq_pieces)

        wa_x, wo_x = xswap(wa[:, :, :512]), xswap(wos)
        o_x, dq_x, dkv2 = call(
            mirror_kernel, "mirror", toks,
            [tile(2048), tile(2048), whole(8, 256, 512), whole(8, 512, 256), tile(256), tile(256), tile(512), whole(128, 128)],
            [act(512), act(512), act(512, F32)], 16_000_000_000,
            [pltpu.VMEM((ROWS, 512), BF), pltpu.VMEM((ROWS, 512), BF)],
        )(offs, h, dy, wa_x, wo_x, k, v, dkv1, mask)
        dkv = (dkv2 + cswap(dkv2)).astype(BF)
        dkv_part = lax.dynamic_slice_in_dim(dkv, m * 128, 128, axis=1)
        kv_pieces = call(in_grad_kernel, "kv_grad", toks, [tile(2048), tile(128)], gouts(256, 128), 1_600_000_000)(offs, h, dkv_part)
        g_kv = reduce(kv_pieces)
        g_kv = jnp.stack([g_kv, cswap(g_kv), xswap(g_kv), xswap(cswap(g_kv))])
        order = jnp.array([[0, 1, 2, 3], [1, 0, 3, 2], [2, 3, 0, 1], [3, 2, 1, 0]])[m]
        g_kv = jnp.concatenate([lax.dynamic_index_in_dim(g_kv, order[i], keepdims=False) for i in range(4)], axis=1)

        wo_c, wo_xc = cswap(wos), cswap(wo_x)
        wa_c, wa_xc = cswap(wa[:, :, :512]), cswap(wa_x)
        o_c, o_xc = cswap(o), cswap(o_x)
        dq_c, dq_xc = cswap(dq), cswap(dq_x)
        (out,) = call(
            y_kernel, "y", toks, [tile(512)] * 4 + [ANY] * 4, [act(2048)], 13_000_000_000,
            [pltpu.VMEM((4, 8, 512, 256), BF), pltpu.VMEM((4, ROWS, 512), BF), pltpu.SemaphoreType.DMA((4,))],
        )(offs, o, o_c, o_x, o_xc, wos, wo_c, wo_x, wo_xc)

        wb_k = jnp.where(core == 0, wa[:, :, 512:], wb)
        wb_v = jnp.where(core == 0, wb, wa[:, :, 512:])
        (dx,) = call(
            dx_kernel, "dx", toks,
            [tile(2048), whole(1, 2048)] + [tile(512)] * 5 + [ANY] * 4 + [whole(8, 256, 512)], [act(2048)], 16_000_000_000,
            [pltpu.VMEM((4, 8, 256, 512), BF), pltpu.VMEM((4, ROWS, 512), BF), pltpu.VMEM((ROWS, 2048), F32), pltpu.SemaphoreType.DMA((4,))],
        )(offs, x, gain2, dq, dq_c, dq_x, dq_xc, dkv, wa[:, :, :512], wa_c, wa_x, wa_xc, jnp.concatenate([wb_k, wb_v], axis=2))
        return out, dx, g_wq, g_kv, g_wo

    return jax.shard_map(
        device_step,
        mesh=mesh,
        in_specs=(P("data", None), P("data", "model"), P("data", None), P("model", "data"), P(), P(), P("data", None)),
        out_specs=(P("data", None), P("data", None), P("data", "model"), P("data", None), P("model", "data")),
        check_vma=False,
    )
```

```python
import functools

import jax
import jax.numpy as jnp
from jax import lax
from jax.experimental import pallas as pl
from jax.experimental.pallas import tpu as pltpu
from jax.sharding import PartitionSpec as P

NORM_EPS = 1e-6
ROWS = 512
TOKS = 1536
SEQ = 128
BF = jnp.bfloat16
F32 = jnp.float32


def dot(a, b):
    return jnp.dot(a, b, preferred_element_type=F32)


def dot_t(a, b):
    return lax.dot_general(a, b, (((1,), (1,)), ((), ())), preferred_element_type=F32)


def t_dot(a, b):
    return lax.dot_general(a, b, (((0,), (0,)), ((), ())), preferred_element_type=F32)


MESH = pl.DeviceIdType.MESH


def cols(i, width=256):
    return pl.ds(pl.multiple_of(i * width, width), width)


def norm(x):
    c = x - jnp.mean(x, axis=-1, keepdims=True)
    inv = lax.rsqrt(jnp.mean(c * c, axis=-1, keepdims=True) + NORM_EPS)
    return c * inv, inv


def stack_heads(a):
    return jnp.concatenate([a[:, :256], a[:, 256:]], axis=0)


def spread_heads(a):
    return jnp.concatenate([a[:SEQ], a[SEQ:]], axis=1)


def softmax(s, mask2):
    s = jnp.where(mask2 > 0, s * (256 ** -0.5), -1e30)
    e = jnp.exp(s - jnp.max(s, axis=-1, keepdims=True))
    return e / jnp.sum(e, axis=-1, keepdims=True)


def attend(qs, ks, vs, mask2):
    scores = [dot_t(q, k) for q, k in zip(qs, ks)]
    probs = [softmax(s, mask2) for s in scores]
    return probs, [dot(p.astype(BF), v).astype(BF) for p, v in zip(probs, vs)]


def attend_back(qs, ks, vs, probs, dos):
    dps = [dot_t(do, v) for do, v in zip(dos, vs)]
    dvs = [t_dot(p.astype(BF), do) for p, do in zip(probs, dos)]
    dss = [p * (dp - jnp.sum(p * dp, axis=-1, keepdims=True)) for p, dp in zip(probs, dps)]
    dss = [(ds * (256 ** -0.5)).astype(BF) for ds in dss]
    dqs = [dot(ds, k).astype(BF) for ds, k in zip(dss, ks)]
    dks = [t_dot(ds, q) for ds, q in zip(dss, qs)]
    return dqs, dks, dvs


def gather_kernel(
    x_hbm, gain, wq_hbm, wkv_hbm, wo_hbm, dy_hbm, mask,
    h_out, q_out, k_out, v_out, o_out, p_out, wq_out, wkv_out, wo_out, g0, g1, g2, g3, g4, g5, g6, g7,
    xh, dyv, wq, wkv, wo, q, k, v, o, ot, probs, gwo, lsem, osem, ssem, rsem,
):
    d, m = lax.axis_index("data"), lax.axis_index("model")
    z, y = d // 2, d % 2
    core = m % 2
    zpeer = [((z + s) % 4) * 2 + y for s in range(4)]
    zfrom = [((z + 4 - s) % 4) * 2 + y for s in range(4)]
    ypeer = z * 2 + 1 - y
    mate = m + 1 - 2 * core

    loads = []
    for t in range(3):
        r = slice(t * ROWS, (t + 1) * ROWS)
        loads.append(pltpu.make_async_copy(x_hbm.at[r], xh.at[r], lsem.at[t]))
    for c in loads:
        c.start()
    half = cols(core)
    own = [
        pltpu.make_async_copy(wq_hbm, wq.at[cols(d)], lsem.at[3]),
        pltpu.make_async_copy(wkv_hbm.at[:, half], wkv.at[core, cols(d)], lsem.at[4]),
        pltpu.make_async_copy(wo_hbm, wo.at[:, cols(d)], lsem.at[5]),
    ]
    for c in own:
        c.start()
    dy_load = pltpu.make_async_copy(dy_hbm, dyv, lsem.at[6])
    dy_load.start()

    barrier = pltpu.get_barrier_semaphore()
    for peer in zpeer[1:] + [ypeer]:
        pl.semaphore_signal(barrier, inc=1, device_id={"data": peer}, device_id_type=MESH)
    pl.semaphore_signal(barrier, inc=1, device_id={"model": mate}, device_id_type=MESH)
    pl.semaphore_wait(barrier, 5)

    def slot(a, blk):
        return wq.at[cols(blk)] if a == 0 else wkv.at[core, cols(blk)] if a == 1 else wo.at[:, cols(blk)]

    shard = [wq_hbm, wkv_hbm.at[:, half], wo_hbm]

    def send(a, src, blk, n, peer):
        return pltpu.make_async_remote_copy(
            src_ref=src, dst_ref=slot(a, blk), send_sem=ssem.at[a, n], recv_sem=rsem.at[a, n],
            device_id={"data": peer}, device_id_type=MESH,
        )

    zsend = {(a, s): send(a, shard[a], d, s, zpeer[s]) for a in range(3) for s in (1, 2, 3)}
    ysend = {(a, s): send(a, shard[a] if s == 0 else slot(a, zfrom[s]), zfrom[s], 4 + s, ypeer) for a in range(3) for s in range(4)}
    zrecv = {(a, s): send(a, slot(a, zfrom[s]), zfrom[s], s, zpeer[s]) for a in range(3) for s in (1, 2, 3)}
    yblk = [zfrom[s] + 1 - 2 * y for s in range(4)]
    yrecv = {(a, s): send(a, slot(a, yblk[s]), yblk[s], 4 + s, ypeer) for a in range(3) for s in range(4)}

    for s in (1, 2, 3):
        zsend[0, s].start()
        zsend[1, s].start()
    for a in range(3):
        ysend[a, 0].start()
    for s in (1, 2, 3):
        zsend[2, s].start()

    for t in range(3):
        loads[t].wait()

        @pl.loop(t * 4, t * 4 + 4)
        def _(i):
            r = cols(i, SEQ)
            n, _inv = norm(xh[r, :].astype(F32))
            xh[r, :] = (n * gain[...]).astype(BF)

    outs = [pltpu.make_async_copy(xh, h_out, osem.at[0])]
    outs[0].start()
    for c in own:
        c.wait()

    def forward(a, s):
        zrecv[a, s].wait_recv()
        ysend[a, s].start()

    for s in (1, 2, 3):
        forward(0, s)
        forward(1, s)
    for s in (0, 1, 2):
        yrecv[0, s].wait_recv()
        yrecv[1, s].wait_recv()
    forward(2, 1)
    yrecv[1, 3].wait_recv()
    across = pltpu.make_async_remote_copy(
        src_ref=wkv.at[core], dst_ref=wkv.at[core], send_sem=ssem.at[0, 0], recv_sem=rsem.at[0, 0],
        device_id={"model": mate}, device_id_type=MESH,
    )
    across.start()
    yrecv[0, 3].wait_recv()

    @pl.loop(0, 3)
    def _(t):
        r = cols(t, ROWS)
        q[r, :] = dot(xh[r, :], wq[...]).astype(BF)

    forward(2, 2)
    pltpu.make_async_remote_copy(
        src_ref=wkv.at[1 - core], dst_ref=wkv.at[1 - core], send_sem=ssem.at[0, 0], recv_sem=rsem.at[0, 0],
        device_id={"model": mate}, device_id_type=MESH,
    ).wait_recv()

    @pl.loop(0, 3)
    def _(t):
        r = cols(t, ROWS)
        k[r, :] = dot(xh[r, :], wkv[0]).astype(BF)
        v[r, :] = dot(xh[r, :], wkv[1]).astype(BF)

    forward(2, 3)
    mask2 = jnp.concatenate([mask[...], mask[...]], axis=0)

    @pl.loop(0, 3)
    def _(t):
        rows = [cols(t * 4 + b, SEQ) for b in range(4)]
        qs = [stack_heads(q[r, :]) for r in rows]
        ps, os = attend(qs, [k[r, :] for r in rows], [v[r, :] for r in rows], mask2)
        for b in range(4):
            probs[t * 4 + b] = ps[b]
            wide = spread_heads(os[b])
            o[rows[b], :] = wide
            ot[:, rows[b]] = wide.T

    pairs = [(q, q_out), (k, k_out), (v, v_out), (o, o_out), (probs, p_out), (wq, wq_out), (wkv, wkv_out)]
    for i, (a, b) in enumerate(pairs):
        outs.append(pltpu.make_async_copy(a, b, osem.at[1 + i]))
        outs[-1].start()

    dy_load.wait()

    @pl.loop(0, 8)
    def _(i):
        blk = ((z + i % 4) % 4) * 2 + (y + i // 4) % 2
        gwo[i] = dot(ot[...], dyv[:, cols(blk)])

    for i, g in enumerate((g0, g1, g2, g3, g4, g5, g6, g7)):
        outs.append(pltpu.make_async_copy(gwo.at[i], g, osem.at[8 + i]))
        outs[-1].start()
    for s in range(4):
        yrecv[2, s].wait_recv()
    outs.append(pltpu.make_async_copy(wo, wo_out, osem.at[16]))
    outs[-1].start()
    for c in zsend.values():
        c.wait_send()
    for c in ysend.values():
        c.wait_send()
    across.wait_send()
    for c in outs:
        c.wait()


def bwd_kernel(dy_ref, wo_ref, q_ref, k_ref, v_ref, p_ref, dq_ref, dkv_ref):
    do = dot_t(dy_ref[...], wo_ref[...]).astype(BF)
    rows = [slice(b * SEQ, (b + 1) * SEQ) for b in range(4)]
    dqs, dks, dvs = attend_back(
        [stack_heads(q_ref[r, :]) for r in rows], [k_ref[r, :] for r in rows], [v_ref[r, :] for r in rows],
        [p_ref[b] for b in range(4)], [stack_heads(do[r]) for r in rows],
    )
    for b, r in enumerate(rows):
        dq_ref[r, :] = spread_heads(dqs[b])
        dkv_ref[r, :256] = dks[b]
        dkv_ref[r, 256:] = dvs[b]


def mirror_kernel(h_ref, dy_ref, wq_ref, wo_ref, k_ref, v_ref, add_ref, mask_ref, _dep, o_ref, dq_ref, dkv_ref):
    q = dot(h_ref[...], wq_ref[...]).astype(BF)
    do = dot_t(dy_ref[...], wo_ref[...]).astype(BF)
    mask2 = jnp.concatenate([mask_ref[...], mask_ref[...]], axis=0)
    rows = [slice(b * SEQ, (b + 1) * SEQ) for b in range(4)]
    qs = [stack_heads(q[r]) for r in rows]
    ks, vs = [k_ref[r, :] for r in rows], [v_ref[r, :] for r in rows]
    ps, os = attend(qs, ks, vs, mask2)
    for b, r in enumerate(rows):
        o_ref[r, :] = spread_heads(os[b])
    dqs, dks, dvs = attend_back(qs, ks, vs, ps, [stack_heads(do[r]) for r in rows])
    for b, r in enumerate(rows):
        dq_ref[r, :] = spread_heads(dqs[b])
        dkv_ref[r, :256] = add_ref[r, :256] + dks[b]
        dkv_ref[r, 256:] = add_ref[r, 256:] + dvs[b]


def in_grad_kernel(offs, h_ref, b_ref, *outs):
    b = b_ref[...]
    for p, out in enumerate(outs):
        out[...] = t_dot(h_ref[:, cols(offs[p])], b)


def canon(me, refs, place):
    for r, s in enumerate(refs):
        sub = me // 2 * 2 if r < 2 else 2 - me // 2 * 2
        place(sub + (me % 2 if r % 2 == 0 else 1 - me % 2), r, s)


def y_kernel(offs, o0, o1, o2, o3, w0, w1, w2, w3, y_ref, wscr, oscr, sem):
    me = offs[9]

    @pl.when(pl.program_id(0) == 0)
    def _():
        copies = []
        canon(me, (w0, w1, w2, w3), lambda i, r, s: copies.append(pltpu.make_async_copy(s, wscr.at[cols(i, 512)], sem.at[r])))
        for c in copies:
            c.start()
        for c in copies:
            c.wait()

    def place(i, r, s):
        oscr[:, cols(i, 512)] = s[...]

    canon(me, (o0, o1, o2, o3), place)

    @pl.loop(0, 4)
    def _(i):
        y_ref[:, cols(i, 512)] = dot(oscr[...], wscr[:, cols(i, 512)]).astype(BF)


def dx_kernel(offs, x_ref, g_ref, d0, d1, d2, d3, dkv_ref, w0, w1, w2, w3, wkv_ref, dx_ref, wscr, dscr, gh, sem):
    me = offs[9]

    @pl.when(pl.program_id(0) == 0)
    def _():
        copies = []
        canon(me, (w0, w1, w2, w3), lambda i, r, s: copies.append(pltpu.make_async_copy(s, wscr.at[:, cols(i, 512)], sem.at[r])))
        for n in range(2):
            copies.append(pltpu.make_async_copy(wkv_ref.at[n], wscr.at[:, pl.ds(2048 + 256 * n, 256)], sem.at[4 + n]))
        for c in copies:
            c.start()
        for c in copies:
            c.wait()

    def place(i, r, s):
        dscr[:, cols(i, 512)] = s[...]

    canon(me, (d0, d1, d2, d3), place)
    dscr[:, 2048:] = dkv_ref[...]

    @pl.loop(0, 4)
    def _(i):
        gh[:, cols(i, 512)] = dot_t(dscr[...], wscr[cols(i, 512), :])

    @pl.loop(0, 4)
    def _(i):
        r = cols(i, SEQ)
        n, inv = norm(x_ref[r, :].astype(F32))
        gn = gh[r, :] * g_ref[...]
        dx = inv * (gn - jnp.mean(gn, axis=-1, keepdims=True) - n * jnp.mean(gn * n, axis=-1, keepdims=True))
        dx_ref[r, :] = dx.astype(BF)


SMEM = pl.BlockSpec(memory_space=pltpu.SMEM)
ANY = pl.BlockSpec(memory_space=pl.ANY)
VM = pl.BlockSpec(memory_space=pltpu.VMEM)
PARAMS = dict(vmem_limit_bytes=60 * 2**20)


def tile(width, rows=ROWS):
    return pl.BlockSpec((rows, width), lambda i: (i, 0))


def whole(*shape):
    return pl.BlockSpec(shape, lambda i: (0,) * len(shape))


PTILE = pl.BlockSpec((4, 256, SEQ), lambda i: (i, 0, 0))


def call(kernel, name, in_specs, outs, flops, scratch=(), steps=3):
    return pl.pallas_call(
        kernel,
        name=name,
        grid=(steps,),
        in_specs=in_specs,
        out_specs=[b for _, b in outs],
        out_shape=[s for s, _ in outs],
        scratch_shapes=list(scratch),
        cost_estimate=pl.CostEstimate(flops=flops, bytes_accessed=20_000_000, transcendentals=0),
        compiler_params=pltpu.CompilerParams(dimension_semantics=("arbitrary",), **PARAMS),
    )


def solution(mesh):
    sd = jax.ShapeDtypeStruct
    DMA = pltpu.SemaphoreType.DMA

    def zshift(a, k):
        return lax.ppermute(a, "data", [(i, (i + 2 * k) % 8) for i in range(8)])

    def yswap(a):
        return lax.ppermute(a, "data", [(i, i ^ 1) for i in range(8)])

    def xswap(a):
        return lax.ppermute(a, "model", [(i, i ^ 2) for i in range(4)])

    def cswap(a):
        return lax.ppermute(a, "model", [(i, i ^ 1) for i in range(4)])

    def reduce(pieces):
        near, far = pieces[:4], pieces[4:]
        total = {}
        for k in (1, 2, 3, 0):
            total[k] = near[k] + yswap(far[k])
        got = [zshift(total[k], k) for k in (1, 2, 3)]
        return (total[0] + got[0] + got[1] + got[2]).astype(BF)

    def device_step(x, wq, wkv, wo, gain, positions, dy):
        d, m = lax.axis_index("data"), lax.axis_index("model")
        z, y = d // 2, d % 2
        core = m % 2
        offs = [((z + k) % 4) * 2 + (y + j) % 2 for j in (0, 1) for k in range(4)]
        offs = jnp.stack([*offs, core, m]).astype(jnp.int32)
        mask = (positions[None, :] <= positions[:, None]).astype(F32)
        gain2 = gain.reshape(1, -1)

        res = pl.pallas_call(
            gather_kernel,
            name="gather",
            in_specs=[ANY, VM, ANY, ANY, ANY, ANY, VM],
            out_specs=[ANY] * 17,
            out_shape=[
                sd((TOKS, 2048), BF), sd((TOKS, 512), BF), sd((TOKS, 256), BF), sd((TOKS, 256), BF), sd((TOKS, 512), BF),
                sd((12, 256, SEQ), F32), sd((2048, 512), BF), sd((2, 2048, 256), BF), sd((512, 2048), BF),
            ] + [sd((512, 256), F32)] * 8,
            scratch_shapes=[
                pltpu.VMEM((TOKS, 2048), BF), pltpu.VMEM((TOKS, 2048), BF), pltpu.VMEM((2048, 512), BF),
                pltpu.VMEM((2, 2048, 256), BF), pltpu.VMEM((512, 2048), BF), pltpu.VMEM((TOKS, 512), BF),
                pltpu.VMEM((TOKS, 256), BF), pltpu.VMEM((TOKS, 256), BF), pltpu.VMEM((TOKS, 512), BF),
                pltpu.VMEM((512, TOKS), BF), pltpu.VMEM((12, 256, SEQ), F32), pltpu.VMEM((8, 512, 256), F32),
                DMA((7,)), DMA((17,)), DMA((3, 8)), DMA((3, 8)),
            ],
            cost_estimate=pl.CostEstimate(flops=40_000_000_000, bytes_accessed=40_000_000, transcendentals=0),
            compiler_params=pltpu.CompilerParams(collective_id=0, has_side_effects=True, **PARAMS),
        )(x, gain2, wq, wkv, wo, dy, mask)
        h, q, k, v, o, p, wqs, wkvs, wos = res[:9]
        g_wo = reduce(res[9:])
        wq_x, wo_x = xswap(wqs), xswap(wos)

        act = lambda w, dt=BF: (sd((TOKS, w), dt), tile(w))
        dq, dkv1 = call(
            bwd_kernel, "bwd",
            [tile(2048), whole(512, 2048), tile(512), tile(256), tile(256), PTILE],
            [act(512), act(512, F32)], 8_000_000_000,
        )(dy, wos, q, k, v, p)
        gouts = lambda r, c: [(sd((r, c), F32), whole(r, c))] * 8
        wq_pieces = call(
            in_grad_kernel, "wq_grad", [SMEM, whole(TOKS, 2048), whole(TOKS, 512)], gouts(256, 512), 4_000_000_000, steps=1,
        )(offs, h, dq)
        g_wq = reduce(wq_pieces)

        o_x, dq_x, dkv2 = call(
            mirror_kernel, "mirror",
            [tile(2048), tile(2048), whole(2048, 512), whole(512, 2048), tile(256), tile(256), tile(512), whole(SEQ, SEQ), ANY],
            [act(512), act(512), act(512, F32)], 16_000_000_000,
        )(h, dy, wq_x, wo_x, k, v, dkv1, mask, wq_pieces[0])
        dkv = (dkv2 + cswap(dkv2)).astype(BF)
        dkv_part = lax.dynamic_slice_in_dim(dkv, m * 128, 128, axis=1)
        kv_pieces = call(
            in_grad_kernel, "kv_grad", [SMEM, whole(TOKS, 2048), whole(TOKS, 128)], gouts(256, 128), 3_000_000_000, steps=1,
        )(offs, h, dkv_part)
        g_kv = reduce(kv_pieces)
        g_kv = jnp.stack([g_kv, cswap(g_kv), xswap(g_kv), xswap(cswap(g_kv))])
        order = jnp.array([[0, 1, 2, 3], [1, 0, 3, 2], [2, 3, 0, 1], [3, 2, 1, 0]])[m]
        g_kv = jnp.concatenate([lax.dynamic_index_in_dim(g_kv, order[i], keepdims=False) for i in range(4)], axis=1)

        (out,) = call(
            y_kernel, "y", [SMEM] + [tile(512)] * 4 + [ANY] * 4, [act(2048)], 13_000_000_000,
            [pltpu.VMEM((2048, 2048), BF), pltpu.VMEM((ROWS, 2048), BF), DMA((4,))],
        )(offs, o, cswap(o), o_x, cswap(o_x), wos, cswap(wos), wo_x, cswap(wo_x))
        (dx,) = call(
            dx_kernel, "dx",
            [SMEM, tile(2048), whole(1, 2048)] + [tile(512)] * 5 + [ANY] * 5, [act(2048)], 16_000_000_000,
            [pltpu.VMEM((2048, 2560), BF), pltpu.VMEM((ROWS, 2560), BF), pltpu.VMEM((ROWS, 2048), F32), DMA((6,))],
        )(offs, x, gain2, dq, cswap(dq), dq_x, cswap(dq_x), dkv, wqs, cswap(wqs), wq_x, cswap(wq_x), wkvs)
        return out, dx, g_wq, g_kv, g_wo

    return jax.shard_map(
        device_step,
        mesh=mesh,
        in_specs=(P("data", None), P("data", "model"), P("data", None), P("model", "data"), P(), P(), P("data", None)),
        out_specs=(P("data", None), P("data", None), P("data", "model"), P("data", None), P("model", "data")),
        check_vma=False,
    )
```

```python
import functools

import jax
import jax.numpy as jnp
from jax import lax
from jax.experimental import pallas as pl
from jax.experimental.pallas import tpu as pltpu
from jax.sharding import PartitionSpec as P

NORM_EPS = 1e-6
ROWS = 512
TOKS = 1536
SEQ = 128
BF = jnp.bfloat16
F32 = jnp.float32


def dot(a, b):
    return jnp.dot(a, b, preferred_element_type=F32)


def dot_t(a, b):
    return lax.dot_general(a, b, (((1,), (1,)), ((), ())), preferred_element_type=F32)


def t_dot(a, b):
    return lax.dot_general(a, b, (((0,), (0,)), ((), ())), preferred_element_type=F32)


MESH = pl.DeviceIdType.MESH


def cols(i, width=256):
    return pl.ds(pl.multiple_of(i * width, width), width)


def norm(x):
    c = x - jnp.mean(x, axis=-1, keepdims=True)
    inv = lax.rsqrt(jnp.mean(c * c, axis=-1, keepdims=True) + NORM_EPS)
    return c * inv, inv


def stack_heads(a):
    return jnp.concatenate([a[:, :256], a[:, 256:]], axis=0)


def spread_heads(a):
    return jnp.concatenate([a[:SEQ], a[SEQ:]], axis=1)


def softmax(s, mask2):
    s = jnp.where(mask2 > 0, s * (256 ** -0.5), -1e30)
    e = jnp.exp(s - jnp.max(s, axis=-1, keepdims=True))
    return e / jnp.sum(e, axis=-1, keepdims=True)


def attend(qs, ks, vs, mask2):
    scores = [dot_t(q, k) for q, k in zip(qs, ks)]
    probs = [softmax(s, mask2) for s in scores]
    return probs, [dot(p.astype(BF), v).astype(BF) for p, v in zip(probs, vs)]


def attend_back(qs, ks, vs, probs, dos):
    dps = [dot_t(do, v) for do, v in zip(dos, vs)]
    dvs = [t_dot(p.astype(BF), do) for p, do in zip(probs, dos)]
    dss = [p * (dp - jnp.sum(p * dp, axis=-1, keepdims=True)) for p, dp in zip(probs, dps)]
    dss = [(ds * (256 ** -0.5)).astype(BF) for ds in dss]
    dqs = [dot(ds, k).astype(BF) for ds, k in zip(dss, ks)]
    dks = [t_dot(ds, q) for ds, q in zip(dss, qs)]
    return dqs, dks, dvs


def drop(items, item):
    items[:] = [i for i in items if i is not item]


def layer_kernel(
    x_hbm, gain, wq_hbm, wkv_hbm, wo_hbm, dy_hbm, mask,
    y_out, dx_out, gq_out, gkv_out, go_out, wq_all, wo_all, o_all, dq_all, dkv_mate,
    xh, big, wq, wkv, wo, wqx, wox, q, k, v, probs, o, ox, dq, dqx, dkv,
    ofar, ory, orz, qfar, qry, qrz, kfar, kry, krz, acc, xt, stage, dkvt, go_st, gq_st, gk_st,
    lsem, ssem, rsem, gss, gsr, dks, dkr,
):
    d, m = lax.axis_index("data"), lax.axis_index("model")
    z, y = d // 2, d % 2
    core = m % 2
    zpeer = [((z + s) % 4) * 2 + y for s in range(4)]
    zfrom = [((z + 4 - s) % 4) * 2 + y for s in range(4)]
    yblk = [zfrom[s] + 1 - 2 * y for s in range(4)]
    ypeer = z * 2 + 1 - y
    mate = m + 1 - 2 * core
    across = (m + 2) % 4
    diag = (mate + 2) % 4
    mine = pl.ds(pl.multiple_of(core * 768, 768), 768)
    theirs = pl.ds(pl.multiple_of((1 - core) * 768, 768), 768)
    used = {"l": 0, "r": 0}
    sends = []

    def local(src, dst):
        i = used["l"]
        used["l"] += 1
        return pltpu.make_async_copy(src, dst, lsem.at[i])

    def remote(src, dst, land, axis, peer):
        i = used["r"]
        used["r"] += 1
        args = dict(send_sem=ssem.at[i], recv_sem=rsem.at[i], device_id={axis: peer}, device_id_type=MESH)
        out = pltpu.make_async_remote_copy(src_ref=src, dst_ref=dst, **args)
        back = pltpu.make_async_remote_copy(src_ref=land, dst_ref=land, **args)
        sends.append(out)
        return out, back

    loads = [local(x_hbm.at[cols(t, ROWS)], xh.at[cols(t, ROWS)]) for t in range(3)]
    half = cols(core)
    own = [local(wq_hbm, wq.at[cols(d)]), local(wkv_hbm.at[:, half], wkv.at[core, cols(d)]), local(wo_hbm, wo.at[:, cols(d)])]
    dy_load = local(dy_hbm, big.at[pl.ds(0, TOKS)])
    for c in loads + own + [dy_load]:
        c.start()

    barrier = pltpu.get_barrier_semaphore()
    for peer in zpeer[1:] + [ypeer]:
        pl.semaphore_signal(barrier, inc=1, device_id={"data": peer}, device_id_type=MESH)
    for peer in (mate, across, diag):
        pl.semaphore_signal(barrier, inc=1, device_id={"model": peer}, device_id_type=MESH)
    pl.semaphore_wait(barrier, 7)

    shard = [wq_hbm, wkv_hbm.at[:, half], wo_hbm]

    def slot(a, blk):
        return wq.at[cols(blk)] if a == 0 else wkv.at[core, cols(blk)] if a == 1 else wo.at[:, cols(blk)]

    def xslot(a, blk):
        return wqx.at[cols(blk)] if a == 0 else wox.at[:, cols(blk)]

    zs = {(a, s): remote(shard[a], slot(a, d), slot(a, zfrom[s]), "data", zpeer[s]) for a in range(3) for s in (1, 2, 3)}
    ys = {}
    xs = {}
    for a in range(3):
        for s in range(4):
            src = shard[a] if s == 0 else slot(a, zfrom[s])
            ys[a, s] = remote(src, slot(a, zfrom[s]), slot(a, yblk[s]), "data", ypeer)
            if a != 1:
                xs[a, s] = remote(src, xslot(a, zfrom[s]), xslot(a, zfrom[s]), "model", across)
                xs[a, 4 + s] = remote(slot(a, yblk[s]), xslot(a, yblk[s]), xslot(a, yblk[s]), "model", across)

    for s in (1, 2, 3):
        zs[0, s][0].start()
        zs[1, s][0].start()
    for a in range(3):
        ys[a, 0][0].start()
    for s in (1, 2, 3):
        zs[2, s][0].start()
    xs[0, 0][0].start()
    xs[2, 0][0].start()

    for t in range(3):
        loads[t].wait()

        @pl.loop(t * 4, t * 4 + 4)
        def _(i):
            r = cols(i, SEQ)
            n, _inv = norm(xh[r, :].astype(F32))
            xh[r, :] = (n * gain[...]).astype(BF)

    for c in own:
        c.wait()

    def forward(a, s):
        zs[a, s][1].wait_recv()
        ys[a, s][0].start()
        if a != 1:
            xs[a, s][0].start()

    def arrive(a, s):
        ys[a, s][1].wait_recv()
        if a != 1:
            xs[a, 4 + s][0].start()

    for s in (1, 2, 3):
        forward(0, s)
        forward(1, s)
    for s in (0, 1, 2):
        arrive(0, s)
        arrive(1, s)
    forward(2, 1)
    arrive(1, 3)
    kv_x = remote(wkv.at[core], wkv.at[core], wkv.at[1 - core], "model", mate)
    kv_x[0].start()
    arrive(0, 3)

    locals_ = []

    def share(src, dst, slot_of):
        c = local(src, dst.at[slot_of(0)])
        out, back = remote(src, dst.at[slot_of(0)], dst.at[slot_of(1)], "model", mate)
        c.start()
        out.start()
        locals_.append(c)
        return c, out, back

    def colslot(base):
        other = base + 1 - 2 * (base % 2)
        return lambda n: (slice(None), cols(base if n == 0 else other, 512))

    def rowslot(base):
        other = base + 1 - 2 * (base % 2)
        return lambda n: (cols(base if n == 0 else other, 512),)

    def share_rows(src, dst, base):
        other = base + 1 - 2 * (base % 2)
        c = local(src.at[mine], dst.at[:, cols(base, 512)])
        out, back = remote(src.at[theirs], dst.at[:, cols(base, 512)], dst.at[:, cols(other, 512)], "model", mate)
        c.start()
        out.start()
        locals_.append(c)
        return c, out, back

    wq_sh = share(wq, wq_all, colslot(m))

    @pl.loop(0, 3)
    def _(t):
        r = cols(t, ROWS)
        q[r, :] = dot(xh[r, :], wq[...]).astype(BF)

    forward(2, 2)
    kv_x[1].wait_recv()

    @pl.loop(0, 3)
    def _(t):
        r = cols(t, ROWS)
        k[r, :] = dot(xh[r, :], wkv[0]).astype(BF)
        v[r, :] = dot(xh[r, :], wkv[1]).astype(BF)

    forward(2, 3)
    mask2 = jnp.concatenate([mask[...], mask[...]], axis=0)

    @pl.loop(0, 3)
    def _(t):
        rows = [cols(t * 4 + b, SEQ) for b in range(4)]
        qs = [stack_heads(q[r, :]) for r in rows]
        ps, os = attend(qs, [k[r, :] for r in rows], [v[r, :] for r in rows], mask2)
        for b in range(4):
            probs[t * 4 + b] = ps[b]
            wide = spread_heads(os[b])
            o[rows[b], :] = wide
            big[pl.ds(TOKS, 512), rows[b]] = wide.T

    dy_load.wait()
    o_sh = share_rows(o, o_all, m)

    far = [qfar, kfar, ofar]
    ry = [qry, kry, ory]
    rz = [qrz, krz, orz]

    def piece(g, blk):
        if g == 2:
            return dot(big[pl.ds(TOKS, 512), pl.ds(0, TOKS)], big[pl.ds(0, TOKS), cols(blk)])
        return t_dot(xh[:, cols(blk)], dq[...] if g == 0 else q[:, cols(m, 128)])

    def ysend(g, kk):
        return pltpu.make_async_remote_copy(
            src_ref=far[g].at[kk], dst_ref=ry[g].at[kk], send_sem=gss.at[g, kk], recv_sem=gsr.at[g, kk],
            device_id={"data": ypeer}, device_id_type=MESH,
        )

    def zsend(g, kk):
        return pltpu.make_async_remote_copy(
            src_ref=ry[g].at[kk], dst_ref=rz[g].at[kk - 1], send_sem=gss.at[g, 4 + kk], recv_sem=gsr.at[g, 4 + kk],
            device_id={"data": zpeer[kk]}, device_id_type=MESH,
        )

    def send_far(g):
        @pl.loop(0, 4)
        def _(i):
            kk = (i + 1) % 4
            far[g][kk] = piece(g, ((z + kk) % 4) * 2 + 1 - y)
            ysend(g, kk).start()

    def near(g, kk):
        ysend(g, kk).wait_recv()
        ry[g][kk] = ry[g][kk] + piece(g, zpeer[kk])
        if kk:
            zsend(g, kk).start()

    def finish(g, st):
        for kk in (1, 2, 3):
            zsend(g, kk).wait_recv()
        st[...] = (ry[g][0] + rz[g][0] + rz[g][1] + rz[g][2]).astype(BF)

    send_far(2)
    for s in range(4):
        arrive(2, s)
    wo_sh = share(wo, wo_all, rowslot(m))

    def back_tile(t, q_of, ps, do, add):
        rows = [cols(t * 4 + b, SEQ) for b in range(4)]
        qs, ks, vs = q_of, [k[r, :] for r in rows], [v[r, :] for r in rows]
        dqs, dks, dvs = attend_back(qs, ks, vs, ps, [stack_heads(do[b * SEQ : (b + 1) * SEQ]) for b in range(4)])
        to = dqx if add else dq
        for b, r in enumerate(rows):
            to[r, :] = spread_heads(dqs[b])
            dkv[r, :256] = dkv[r, :256] + dks[b] if add else dks[b]
            dkv[r, 256:] = dkv[r, 256:] + dvs[b] if add else dvs[b]

    @pl.loop(0, 3)
    def _(t):
        do = dot_t(big[cols(t, ROWS), :], wo[...]).astype(BF)
        qs = [stack_heads(q[cols(t * 4 + b, SEQ), :]) for b in range(4)]
        back_tile(t, qs, [probs[t * 4 + b] for b in range(4)], do, False)

    dq_sh = share_rows(dq, dq_all, m)
    send_far(0)
    near(2, 1)
    near(2, 2)

    for n in range(8):
        xs[0, n][1].wait_recv()
        xs[2, n][1].wait_recv()
    wqx_sh = share(wqx, wq_all, colslot(across))
    wox_sh = share(wox, wo_all, rowslot(across))

    def dkv_send(t):
        r = cols(t, ROWS)
        return pltpu.make_async_remote_copy(
            src_ref=dkv.at[r], dst_ref=dkv_mate.at[r], send_sem=dks.at[t], recv_sem=dkr.at[t],
            device_id={"model": mate}, device_id_type=MESH,
        )

    @pl.loop(0, 3)
    def _(t):
        rows = [cols(t * 4 + b, SEQ) for b in range(4)]
        qm = dot(xh[cols(t, ROWS), :], wqx[...]).astype(BF)
        do = dot_t(big[cols(t, ROWS), :], wox[...]).astype(BF)
        qs = [stack_heads(qm[b * SEQ : (b + 1) * SEQ]) for b in range(4)]
        ps, os = attend(qs, [k[r, :] for r in rows], [v[r, :] for r in rows], mask2)
        for b in range(4):
            ox[rows[b], :] = spread_heads(os[b])
        back_tile(t, qs, ps, do, True)
        dkv_send(t).start()

    ox_sh = share_rows(ox, o_all, across)
    dqx_sh = share_rows(dqx, dq_all, across)
    near(2, 3)
    near(2, 0)

    tiles = []
    for t in range(3):
        dkv_send(t).wait_recv()
        tiles.append(local(dkv_mate.at[cols(t, ROWS)], dkvt.at[t % 2]))
        if t < 2:
            tiles[t].start()
    for t in range(3):
        tiles[t].wait()
        q[cols(t, ROWS), :] = (dkv[cols(t, ROWS), :] + dkvt[t % 2]).astype(BF)
        if t == 0:
            tiles[2].start()
    send_far(1)

    for sh in (wo_sh, wox_sh, o_sh, ox_sh):
        sh[0].wait()
        sh[1].wait_send()
        sh[2].wait_recv()
    for sh in (wo_sh, wox_sh, o_sh, ox_sh):
        drop(sends, sh[1])
        drop(locals_, sh[0])
    for c in [ys[2, s][0] for s in range(4)] + [xs[2, n][0] for n in range(8)]:
        c.wait_send()
        drop(sends, c)
    tin = [wox.at[pl.ds(0, 256)], wox.at[pl.ds(256, 256)], wo.at[pl.ds(0, 256)]]
    fill = local(wo_all, big)
    fill.start()
    ins = [local(o_all.at[cols(t)], tin[t]) for t in range(3)]
    for c in ins:
        c.start()
    near(0, 1)
    fill.wait()
    done = []

    def emit(t, dst):
        r = pl.ds(pl.multiple_of(core * 768 + t * 256, 256), 256)
        other = pl.ds(pl.multiple_of((1 - core) * 768 + t * 256, 256), 256)
        c = local(stage.at[t], dst.at[r])
        out, back = remote(stage.at[t], dst.at[r], dst.at[other], "model", mate)
        c.start()
        out.start()
        done.append((c, out, back))

    def tile_rows(t):
        return (wox, 256 * t) if t < 2 else (wo, 0)

    for t in range(3):
        ins[t].wait()
        ref, at = tile_rows(t)

        @pl.loop(0, 4)
        def _(i):
            stage[t, :, cols(i, 512)] = dot(ref[pl.ds(at, 256), :], big[:, cols(i, 512)]).astype(BF)

        emit(t, y_out)
        if t == 0:
            near(0, 2)

    for sh in (wq_sh, wqx_sh, dq_sh, dqx_sh):
        sh[0].wait()
        sh[1].wait_send()
        sh[2].wait_recv()
        drop(sends, sh[1])
        drop(locals_, sh[0])
    fill = local(wq_all, big)
    fill.start()
    ins = [local(dq_all.at[cols(t)], tin[t]) for t in range(3)]
    xin = [local(x_hbm.at[pl.ds(pl.multiple_of(core * 768 + t * 256, 256), 256)], xt.at[t % 2]) for t in range(3)]
    for c in ins + xin[:2]:
        c.start()
    near(0, 3)
    fill.wait()
    for t in range(3):
        ins[t].wait()
        ref, at = tile_rows(t)
        r = pl.ds(pl.multiple_of(core * 768 + t * 256, 256), 256)

        @pl.loop(0, 4)
        def _(i):
            c = cols(i, 512)
            g = dot_t(ref[pl.ds(at, 256), :], big[c, :])
            g = g + dot_t(q[r, :256], wkv[0, c, :])
            acc[:, c] = g + dot_t(q[r, 256:], wkv[1, c, :])

        xin[t].wait()
        done[t][0].wait()
        done[t][1].wait_send()
        drop(sends, done[t][1])

        @pl.loop(0, 2)
        def _(i):
            s = cols(i, SEQ)
            n, inv = norm(xt[t % 2, s, :].astype(F32))
            gn = acc[s, :] * gain[...]
            g = inv * (gn - jnp.mean(gn, axis=-1, keepdims=True) - n * jnp.mean(gn * n, axis=-1, keepdims=True))
            stage[t, s, :] = g.astype(BF)

        if t == 0:
            xin[2].start()
        emit(t, dx_out)
        if t == 0:
            near(0, 0)

    finish(2, go_st)
    fin = [local(go_st, go_out)]
    fin[0].start()
    for kk in (1, 2, 3, 0):
        near(1, kk)
    finish(0, gq_st)
    fin.append(local(gq_st, gq_out))
    fin[1].start()
    finish(1, gk_st)
    fin.append(local(gk_st, gkv_out.at[:, cols(m, 128)]))
    fin[2].start()
    backs = []
    for peer in (mate, across, diag):
        out, back = remote(gk_st, gkv_out.at[:, cols(m, 128)], gkv_out.at[:, cols(peer, 128)], "model", peer)
        out.start()
        backs.append(back)

    for b in backs:
        b.wait_recv()
    for t, (c, out, back) in enumerate(done):
        if t >= 3:
            c.wait()
        back.wait_recv()
    for c in sends:
        c.wait_send()
    for c in locals_ + fin:
        c.wait()
    for g in range(3):
        for kk in range(4):
            ysend(g, kk).wait_send()
            if kk:
                zsend(g, kk).wait_send()
    for t in range(3):
        dkv_send(t).wait_send()


def solution(mesh):
    sd = jax.ShapeDtypeStruct
    DMA = pltpu.SemaphoreType.DMA
    VM = pltpu.VMEM
    ANY = pl.BlockSpec(memory_space=pl.ANY)
    IN_VM = pl.BlockSpec(memory_space=pltpu.VMEM)

    def device_step(x, wq, wkv, wo, gain, positions, dy):
        mask = (positions[None, :] <= positions[:, None]).astype(F32)
        outs = [
            sd((TOKS, 2048), BF), sd((TOKS, 2048), BF), sd((256, 512), BF), sd((256, 512), BF), sd((512, 256), BF),
            sd((2048, 2048), BF), sd((2048, 2048), BF), sd((768, 2048), BF), sd((768, 2048), BF), sd((TOKS, 512), F32),
        ]
        wide, narrow = VM((TOKS, 512), BF), VM((TOKS, 256), BF)
        scratch = [
            VM((TOKS, 2048), BF), VM((2048, 2048), BF), VM((2048, 512), BF), VM((2, 2048, 256), BF), VM((512, 2048), BF),
            VM((2048, 512), BF), VM((512, 2048), BF), wide, narrow, narrow, VM((12, 256, SEQ), F32),
            wide, wide, wide, wide, VM((TOKS, 512), F32),
            VM((4, 512, 256), F32), VM((4, 512, 256), F32), VM((3, 512, 256), F32),
            VM((4, 256, 512), F32), VM((4, 256, 512), F32), VM((3, 256, 512), F32),
            VM((4, 256, 128), F32), VM((4, 256, 128), F32), VM((3, 256, 128), F32),
            VM((256, 2048), F32), VM((2, 256, 2048), BF), VM((3, 256, 2048), BF), VM((2, 512, 512), F32),
            VM((512, 256), BF), VM((256, 512), BF), VM((256, 128), BF),
            DMA((40,)), DMA((64,)), DMA((64,)), DMA((3, 8)), DMA((3, 8)), DMA((3,)), DMA((3,)),
        ]
        res = pl.pallas_call(
            layer_kernel,
            name="layer",
            in_specs=[ANY, IN_VM, ANY, ANY, ANY, ANY, IN_VM],
            out_specs=[ANY] * len(outs),
            out_shape=outs,
            scratch_shapes=scratch,
            cost_estimate=pl.CostEstimate(flops=80_000_000_000, bytes_accessed=100_000_000, transcendentals=0),
            compiler_params=pltpu.CompilerParams(collective_id=0, has_side_effects=True, vmem_limit_bytes=67043328),
        )(x, gain.reshape(1, -1), wq, wkv, wo, dy, mask)
        return tuple(res[:5])

    return jax.shard_map(
        device_step,
        mesh=mesh,
        in_specs=(P("data", None), P("data", "model"), P("data", None), P("model", "data"), P(), P(), P("data", None)),
        out_specs=(P("data", None), P("data", None), P("data", "model"), P("data", None), P("model", "data")),
        check_vma=False,
    )
```

```python
import functools

import jax
import jax.numpy as jnp
from jax import lax
from jax.experimental import pallas as pl
from jax.experimental.pallas import tpu as pltpu
from jax.sharding import PartitionSpec as P

NORM_EPS = 1e-6
ROWS = 512
TOKS = 1536
SEQ = 128
D = 2048
CORE = 768
W = 512
PASS = 384
H = 256
WAYS = (1, -1)
HOPS = (1, 2, 3)
BF = jnp.bfloat16
F32 = jnp.float32


def dot(a, b):
    return jnp.dot(a, b, preferred_element_type=F32)


def dot_t(a, b):
    return lax.dot_general(a, b, (((1,), (1,)), ((), ())), preferred_element_type=F32)


def t_dot(a, b):
    return lax.dot_general(a, b, (((0,), (0,)), ((), ())), preferred_element_type=F32)


MESH = pl.DeviceIdType.MESH


def cols(i, width=H):
    return pl.ds(pl.multiple_of(i * width, width), width)


def norm(x):
    c = x - jnp.mean(x, axis=-1, keepdims=True)
    inv = lax.rsqrt(jnp.mean(c * c, axis=-1, keepdims=True) + NORM_EPS)
    return c * inv, inv


def stack_heads(a):
    return jnp.concatenate([a[:, :H], a[:, H:]], axis=0)


def spread_heads(a):
    return jnp.concatenate([a[:SEQ], a[SEQ:]], axis=1)


def softmax(s, mask2):
    s = jnp.where(mask2 > 0, s * (H ** -0.5), -1e30)
    e = jnp.exp(s - jnp.max(s, axis=-1, keepdims=True))
    return e / jnp.sum(e, axis=-1, keepdims=True)


def attend(qs, ks, vs, mask2):
    scores = [dot_t(q, k) for q, k in zip(qs, ks)]
    probs = [softmax(s, mask2) for s in scores]
    return probs, [dot(p.astype(BF), v).astype(BF) for p, v in zip(probs, vs)]


def attend_back(qs, ks, vs, probs, dos):
    dps = [dot_t(do, v) for do, v in zip(dos, vs)]
    dvs = [t_dot(p.astype(BF), do) for p, do in zip(probs, dos)]
    dss = [p * (dp - jnp.sum(p * dp, axis=-1, keepdims=True)) for p, dp in zip(probs, dps)]
    dss = [(ds * (H ** -0.5)).astype(BF) for ds in dss]
    dqs = [dot(ds, k).astype(BF) for ds, k in zip(dss, ks)]
    dks = [t_dot(ds, q) for ds, q in zip(dss, qs)]
    return dqs, dks, dvs


def drop(items, item):
    items[:] = [i for i in items if i is not item]


def layer_kernel(
    x_hbm, gain, wq_hbm, wkv_hbm, wo_hbm, dy_hbm, pos,
    y_out, dx_out, gq_out, gkv_out, go_out, wq_all, wo_all, o_all, dq_all, dkv_mate,
    xh, big, wq, wkv, wo, wqx, wox, q, k, v, probs, o, ox, dq, dqx, dkv,
    ofar, ory, orz, qfar, qry, qrz, kfar, kry, krz, tin, stage, dkvt, go_st, gq_st, gk_st,
    lsem, ssem, rsem, gss, gsr, dks, dkr,
):
    d, m = lax.axis_index("data"), lax.axis_index("model")
    z, y = d // 2, d % 2
    core = m % 2
    zpeer = [((z + s) % 4) * 2 + y for s in range(4)]
    ypeer = z * 2 + 1 - y
    mate = m + 1 - 2 * core
    across = (m + 2) % 4
    diag = (mate + 2) % 4
    mine = pl.ds(pl.multiple_of(core * CORE, CORE), CORE)
    theirs = pl.ds(pl.multiple_of((1 - core) * CORE, CORE), CORE)
    used = {"l": 0, "r": 0}
    sends = []

    def local(src, dst):
        i = used["l"]
        used["l"] += 1
        return pltpu.make_async_copy(src, dst, lsem.at[i])

    def remote(src, dst, land, axis, peer, when=None):
        i = used["r"]
        used["r"] += 1
        args = dict(send_sem=ssem.at[i], recv_sem=rsem.at[i], device_id={axis: peer}, device_id_type=MESH)
        out = pltpu.make_async_remote_copy(src_ref=src, dst_ref=dst, **args)
        back = pltpu.make_async_remote_copy(src_ref=land, dst_ref=land, **args)
        sends.append((when, out))
        return out, back

    loads = [local(x_hbm.at[cols(t, ROWS)], xh.at[cols(t, ROWS)]) for t in range(3)]
    half = cols(core)
    own = [local(wq_hbm, wq.at[cols(d)]), local(wkv_hbm.at[:, half], wkv.at[core, cols(d)]), local(wo_hbm, wo.at[:, cols(d)])]
    dy_load = local(dy_hbm, big.at[pl.ds(0, TOKS)])
    for c in loads + own + [dy_load]:
        c.start()

    barrier = pltpu.get_barrier_semaphore()
    for peer in zpeer[1:] + [ypeer]:
        pl.semaphore_signal(barrier, inc=1, device_id={"data": peer}, device_id_type=MESH)
    for peer in (mate, across, diag):
        pl.semaphore_signal(barrier, inc=1, device_id={"model": peer}, device_id_type=MESH)
    pl.semaphore_wait(barrier, 7)

    shard = [wq_hbm, wkv_hbm.at[:, half], wo_hbm]

    def slot(a, zz):
        mineblk, otherblk = zz * 2 + y, zz * 2 + 1 - y
        return (
            wq.at[cols(mineblk)] if a == 0 else wkv.at[core, cols(mineblk)] if a == 1 else
            wo.at[:, cols(mineblk)] if a == 2 else wo.at[:, cols(otherblk)]
        )

    def other(a, zz):
        blk = zz * 2 + 1 - y
        return wq.at[cols(blk)] if a == 0 else wkv.at[core, cols(blk)] if a == 1 else wo.at[:, cols(blk)]

    def xslot(a, zz):
        blk = zz * 2 + (y if a in (0, 2) else 1 - y)
        return wqx.at[cols(blk)] if a in (0, 4) else wox.at[:, cols(blk)]

    def got(way, r):
        return z >= r if way > 0 else z + r <= 3

    def origin(way, r):
        return (z + 4 - r) % 4 if way > 0 else (z + r) % 4

    def goes(way):
        return z < 3 if way > 0 else z > 0

    def sent(way, r):
        return goes(way) if r == 1 else jnp.logical_and(got(way, r - 1), goes(way))

    hops, ys, xs = {}, {}, {}
    for r in HOPS:
        for way in WAYS:
            for a in range(4):
                here = origin(way, r - 1)
                src = shard[a] if r == 1 and a < 3 else slot(a, here)
                to = ((z + way + 4) % 4) * 2 + y
                hops[a, way, r] = remote(src, slot(a, here), slot(a, origin(way, r)), "data", to, sent(way, r))
    keys = [None] + [(way, r) for r in HOPS for way in WAYS]
    for key in keys:
        zz = z if key is None else origin(*key)
        cond = None if key is None else got(*key)
        for a in (0, 1):
            src = shard[a] if key is None else slot(a, zz)
            ys[a, key] = remote(src, slot(a, zz), other(a, zz), "data", ypeer, cond)
        if key is None:
            ys[2, None] = remote(shard[2], slot(2, z), slot(3, z), "data", ypeer)
        for a in (0, 2, 3, 4):
            src = shard[a] if key is None and a in (0, 2) else other(0, zz) if a == 4 else slot(a, zz)
            xs[a, key] = remote(src, xslot(a, zz), xslot(a, zz), "model", across, cond)

    def on(cond, fn):
        if cond is None:
            fn()
        else:
            pl.when(cond)(fn)

    def start_hop(a, way, r):
        on(sent(way, r), lambda: hops[a, way, r][0].start())

    for way in WAYS:
        for a in (0, 1):
            start_hop(a, way, 1)
    for a in (0, 1, 2):
        ys[a, None][0].start()
    xs[0, None][0].start()
    xs[2, None][0].start()

    for t in range(3):
        loads[t].wait()

        @pl.loop(t * 4, t * 4 + 4)
        def _(i):
            r = cols(i, SEQ)
            n, _inv = norm(xh[r, :].astype(F32))
            xh[r, :] = (n * gain[...]).astype(BF)

    for c in own:
        c.wait()

    for r in HOPS:
        for way in WAYS:

            @pl.when(got(way, r))
            def _():
                for a in (0, 1):
                    hops[a, way, r][1].wait_recv()
                    if r < 3:
                        start_hop(a, way, r + 1)
                    ys[a, (way, r)][0].start()
                xs[0, (way, r)][0].start()

        if r == 2:
            for way in WAYS:
                start_hop(2, way, 1)
            ys[2, None][1].wait_recv()
            for way in WAYS:
                start_hop(3, way, 1)
            xs[3, None][0].start()

    def take_wo(way, r):
        for a in (2, 3):
            hops[a, way, r][1].wait_recv()
            if r < 3:
                start_hop(a, way, r + 1)
            xs[a, (way, r)][0].start()

    def relay_wo(r):
        for way in WAYS:
            on(jnp.logical_and(got(way, r), goes(way)), lambda way=way: take_wo(way, r))

    def keep_wo():
        for r in HOPS:
            for way in WAYS:
                on(jnp.logical_and(got(way, r), jnp.logical_not(goes(way))), lambda way=way, r=r: take_wo(way, r))

    def arrive(key):
        def go():
            ys[0, key][1].wait_recv()
            ys[1, key][1].wait_recv()
            xs[4, key][0].start()

        on(None if key is None else got(*key), go)

    for key in keys[:5]:
        arrive(key)
    relay_wo(1)
    for key in keys[5:]:
        arrive(key)
    kv_x = remote(wkv.at[core], wkv.at[core], wkv.at[1 - core], "model", mate)
    kv_x[0].start()

    locals_ = []

    def share(src, dst, slot_of):
        c = local(src, dst.at[slot_of(0)])
        out, back = remote(src, dst.at[slot_of(0)], dst.at[slot_of(1)], "model", mate)
        c.start()
        out.start()
        locals_.append(c)
        return c, out, back

    def colslot(base):
        other = base + 1 - 2 * (base % 2)
        return lambda n: (slice(None), cols(base if n == 0 else other, W))

    def rowslot(base):
        other = base + 1 - 2 * (base % 2)
        return lambda n: (cols(base if n == 0 else other, W),)

    def share_rows(src, dst, base):
        other = base + 1 - 2 * (base % 2)
        c = local(src.at[mine], dst.at[:, cols(base, W)])
        out, back = remote(src.at[theirs], dst.at[:, cols(base, W)], dst.at[:, cols(other, W)], "model", mate)
        c.start()
        out.start()
        locals_.append(c)
        return c, out, back

    wq_sh = share(wq, wq_all, colslot(m))

    @pl.loop(0, 3)
    def _(t):
        r = cols(t, ROWS)
        q[r, :] = dot(xh[r, :], wq[...]).astype(BF)

    relay_wo(2)
    kv_x[1].wait_recv()

    @pl.loop(0, 3)
    def _(t):
        r = cols(t, ROWS)
        k[r, :] = dot(xh[r, :], wkv[0]).astype(BF)
        v[r, :] = dot(xh[r, :], wkv[1]).astype(BF)

    posm = jnp.broadcast_to(pos[...].astype(F32), (SEQ, SEQ))
    mask = (posm <= posm.T).astype(F32)
    mask2 = jnp.concatenate([mask, mask], axis=0)

    @pl.loop(0, 3)
    def _(t):
        rows = [cols(t * 4 + b, SEQ) for b in range(4)]
        qs = [stack_heads(q[r, :]) for r in rows]
        ps, os = attend(qs, [k[r, :] for r in rows], [v[r, :] for r in rows], mask2)
        for b in range(4):
            probs[t * 4 + b] = ps[b]
            wide = spread_heads(os[b])
            o[rows[b], :] = wide
            big[pl.ds(TOKS, W), rows[b]] = wide.T

    dy_load.wait()
    o_sh = share_rows(o, o_all, m)

    far = [qfar, kfar, ofar]
    ry = [qry, kry, ory]
    rz = [qrz, krz, orz]

    def piece(g, blk):
        if g == 2:
            return dot(big[pl.ds(TOKS, W), pl.ds(0, TOKS)], big[pl.ds(0, TOKS), cols(blk)])
        return t_dot(xh[:, cols(blk)], dq[...] if g == 0 else q[:, cols(m, SEQ)])

    def ysend(g, kk):
        return pltpu.make_async_remote_copy(
            src_ref=far[g].at[kk], dst_ref=ry[g].at[kk], send_sem=gss.at[g, kk], recv_sem=gsr.at[g, kk],
            device_id={"data": ypeer}, device_id_type=MESH,
        )

    def zsend(g, kk):
        return pltpu.make_async_remote_copy(
            src_ref=ry[g].at[kk], dst_ref=rz[g].at[kk - 1], send_sem=gss.at[g, 4 + kk], recv_sem=gsr.at[g, 4 + kk],
            device_id={"data": zpeer[kk]}, device_id_type=MESH,
        )

    def send_far(g, lo, hi):
        @pl.loop(lo, hi)
        def _(i):
            kk = 2 + i + (i // 2) * (1 - 2 * i)
            far[g][kk] = piece(g, ((z + kk) % 4) * 2 + 1 - y)
            ysend(g, kk).start()

    def near(g, kk):
        ysend(g, kk).wait_recv()
        ry[g][kk] = ry[g][kk] + piece(g, zpeer[kk])
        if kk:
            zsend(g, kk).start()

    def finish(g, st):
        for kk in HOPS:
            zsend(g, kk).wait_recv()
        st[...] = (ry[g][0] + rz[g][0] + rz[g][1] + rz[g][2]).astype(BF)

    send_far(2, 0, 4)
    relay_wo(3)
    keep_wo()
    wo_sh = share(wo, wo_all, rowslot(m))

    def back_tile(t, q_of, ps, do, add):
        rows = [cols(t * 4 + b, SEQ) for b in range(4)]
        qs, ks, vs = q_of, [k[r, :] for r in rows], [v[r, :] for r in rows]
        dqs, dks, dvs = attend_back(qs, ks, vs, ps, [stack_heads(do[b * SEQ : (b + 1) * SEQ]) for b in range(4)])
        to = dqx if add else dq
        for b, r in enumerate(rows):
            to[r, :] = spread_heads(dqs[b])
            dkv[r, :H] = dkv[r, :H] + dks[b] if add else dks[b]
            dkv[r, H:] = dkv[r, H:] + dvs[b] if add else dvs[b]

    @pl.loop(0, 3)
    def _(t):
        do = dot_t(big[cols(t, ROWS), :], wo[...]).astype(BF)
        qs = [stack_heads(q[cols(t * 4 + b, SEQ), :]) for b in range(4)]
        back_tile(t, qs, [probs[t * 4 + b] for b in range(4)], do, False)

    dq_sh = share_rows(dq, dq_all, m)
    send_far(0, 0, 2)
    near(2, 2)
    near(2, 3)
    near(2, 1)

    for key in keys:
        on(None if key is None else got(*key), lambda key=key: [xs[a, key][1].wait_recv() for a in (0, 2, 3, 4)] and None)
    wqx_sh = share(wqx, wq_all, colslot(across))
    wox_sh = share(wox, wo_all, rowslot(across))

    def dkv_send(t):
        r = cols(t, ROWS)
        return pltpu.make_async_remote_copy(
            src_ref=dkv.at[r], dst_ref=dkv_mate.at[r], send_sem=dks.at[t], recv_sem=dkr.at[t],
            device_id={"model": mate}, device_id_type=MESH,
        )

    @pl.loop(0, 3)
    def _(t):
        rows = [cols(t * 4 + b, SEQ) for b in range(4)]
        qm = dot(xh[cols(t, ROWS), :], wqx[...]).astype(BF)
        do = dot_t(big[cols(t, ROWS), :], wox[...]).astype(BF)
        qs = [stack_heads(qm[b * SEQ : (b + 1) * SEQ]) for b in range(4)]
        ps, os = attend(qs, [k[r, :] for r in rows], [v[r, :] for r in rows], mask2)
        for b in range(4):
            ox[rows[b], :] = spread_heads(os[b])
        back_tile(t, qs, ps, do, True)
        dkv_send(t).start()

    ox_sh = share_rows(ox, o_all, across)
    dqx_sh = share_rows(dqx, dq_all, across)

    tiles = []
    for t in range(3):
        dkv_send(t).wait_recv()
        tiles.append(local(dkv_mate.at[cols(t, ROWS)], dkvt.at[t % 2]))
        if t < 2:
            tiles[t].start()
    for t in range(3):
        tiles[t].wait()
        q[cols(t, ROWS), :] = (dkv[cols(t, ROWS), :] + dkvt[t % 2]).astype(BF)
        if t == 0:
            tiles[2].start()
    send_far(1, 0, 4)
    send_far(0, 2, 4)
    near(2, 0)

    for sh in (wo_sh, wox_sh, o_sh, ox_sh):
        sh[0].wait()
        sh[2].wait_recv()
        drop(locals_, sh[0])
    fill = local(wo_all, big)
    fill.start()
    fetch = local(o_all, tin)
    fetch.start()
    fill.wait()
    fetch.wait()

    def y_cols(lo, hi):
        @pl.loop(lo, hi)
        def _(i):
            stage[:, cols(i)] = dot(tin[...], big[:, cols(i)]).astype(BF)

    done = []

    def emit(dst):
        c = local(stage, dst.at[mine])
        out, back = remote(stage, dst.at[mine], dst.at[theirs], "model", mate)
        c.start()
        out.start()
        done.append((c, out, back))

    y_cols(0, 4)
    near(0, 2)
    y_cols(4, 8)
    emit(y_out)

    for sh in (wq_sh, wqx_sh, dq_sh, dqx_sh):
        sh[0].wait()
        sh[2].wait_recv()
        drop(locals_, sh[0])
    fill = local(wq_all, big)
    fill.start()
    fetch = local(dq_all, tin)
    fetch.start()
    wox_sh[1].wait_send()
    sends[:] = [s for s in sends if s[1] is not wox_sh[1]]
    xin = [local(x_hbm.at[pl.ds(pl.multiple_of(core * CORE + p * PASS, PASS), PASS)], wox.at[pl.ds(0, PASS)]) for p in range(2)]
    xin[0].start()
    for t in range(3):
        dkv_send(t).wait_send()
    near(0, 3)
    fill.wait()
    fetch.wait()
    for p in range(2):
        rows = pl.ds(pl.multiple_of(core * CORE + p * PASS, PASS), PASS)

        @pl.loop(0, 4)
        def _(i):
            c = cols(i, W)
            g = dot_t(tin[pl.ds(p * PASS, PASS), :], big[c, :])
            g = g + dot_t(q[rows, :H], wkv[0, c, :])
            dkv[cols(i, PASS), :] = g + dot_t(q[rows, H:], wkv[1, c, :])

        xin[p].wait()
        if p == 0:
            done[0][0].wait()
            done[0][1].wait_send()
            sends[:] = [s for s in sends if s[1] is not done[0][1]]

        @pl.loop(0, 3)
        def _(i):
            n, inv = norm(wox[cols(i, SEQ), :].astype(F32))
            gn = jnp.concatenate([dkv[pl.ds(pl.multiple_of(c * PASS + i * SEQ, SEQ), SEQ), :] for c in range(4)], axis=1) * gain[...]
            g = inv * (gn - jnp.mean(gn, axis=-1, keepdims=True) - n * jnp.mean(gn * n, axis=-1, keepdims=True))
            stage[pl.ds(pl.multiple_of(p * PASS + i * SEQ, SEQ), SEQ), :] = g.astype(BF)

        if p == 0:
            xin[1].start()
            for kk in (2, 3, 1, 0):
                near(1, kk)
    emit(dx_out)

    near(0, 1)
    finish(2, go_st)
    fin = [local(go_st, go_out)]
    fin[0].start()
    finish(1, gk_st)
    fin.append(local(gk_st, gkv_out.at[:, cols(m, SEQ)]))
    fin[1].start()
    backs = []
    for peer in (mate, across, diag):
        out, back = remote(gk_st, gkv_out.at[:, cols(m, SEQ)], gkv_out.at[:, cols(peer, SEQ)], "model", peer)
        out.start()
        backs.append(back)
    near(0, 0)
    finish(0, gq_st)
    fin.append(local(gq_st, gq_out))
    fin[2].start()

    for b in backs:
        b.wait_recv()
    done[1][0].wait()
    for c, out, back in done:
        back.wait_recv()
    for cond, c in sends:
        on(cond, c.wait_send)
    for c in locals_ + fin:
        c.wait()
    for g in range(3):
        for kk in range(4):
            ysend(g, kk).wait_send()
            if kk:
                zsend(g, kk).wait_send()


def copy_kernel(*refs):
    srcs, dsts, bufs, rsem, wsem = refs[:5], refs[5:10], refs[10:15], refs[15], refs[16]
    ins, outs = [], []
    for a in range(5):
        rows = srcs[a].shape[0]
        parts = 8 if a < 2 else 1
        for c in range(parts):
            r = pl.ds(c * (rows // parts), rows // parts)
            i = len(ins)
            ins.append(pltpu.make_async_copy(srcs[a].at[r], bufs[a].at[r], rsem.at[i]))
            outs.append(pltpu.make_async_copy(bufs[a].at[r], dsts[a].at[r], wsem.at[i]))
    for c in ins:
        c.start()
    for i, o in zip(ins, outs):
        i.wait()
        o.start()
    for o in outs:
        o.wait()


def solution(mesh):
    sd = jax.ShapeDtypeStruct
    DMA = pltpu.SemaphoreType.DMA
    VM = pltpu.VMEM
    ANY = pl.BlockSpec(memory_space=pl.ANY)
    IN_VM = pl.BlockSpec(memory_space=pltpu.VMEM)

    def device_step(x, wq, wkv, wo, gain, positions, dy):
        results = [
            sd((TOKS, D), BF), sd((TOKS, D), BF), sd((H, W), BF), sd((H, W), BF), sd((W, H), BF),
        ]
        outs = results + [
            sd((D, D), BF), sd((D, D), BF), sd((CORE, D), BF), sd((CORE, D), BF), sd((TOKS, W), F32),
        ]
        wide, narrow = VM((TOKS, W), BF), VM((TOKS, H), BF)
        scratch = [
            VM((TOKS, D), BF), VM((D, D), BF), VM((D, W), BF), VM((2, D, H), BF), VM((W, D), BF),
            VM((D, W), BF), VM((W, D), BF), wide, narrow, narrow, VM((12, H, SEQ), F32),
            wide, wide, wide, wide, VM((TOKS, W), F32),
            VM((4, W, H), F32), VM((4, W, H), F32), VM((3, W, H), F32),
            VM((4, H, W), F32), VM((4, H, W), F32), VM((3, H, W), F32),
            VM((4, H, SEQ), F32), VM((4, H, SEQ), F32), VM((3, H, SEQ), F32),
            VM((CORE, D), BF), VM((CORE, D), BF), VM((2, W, W), F32),
            VM((W, H), BF), VM((H, W), BF), VM((H, SEQ), BF),
            DMA((40,)), DMA((100,)), DMA((100,)), DMA((3, 8)), DMA((3, 8)), DMA((3,)), DMA((3,)),
        ]
        res = pl.pallas_call(
            layer_kernel,
            name="layer",
            in_specs=[ANY, IN_VM, ANY, ANY, ANY, ANY, IN_VM],
            out_specs=[ANY] * len(outs),
            out_shape=outs,
            scratch_shapes=scratch,
            cost_estimate=pl.CostEstimate(flops=80_000_000_000, bytes_accessed=100_000_000, transcendentals=0),
            compiler_params=pltpu.CompilerParams(collective_id=0, has_side_effects=True, vmem_limit_bytes=67043328),
        )(x, gain.reshape(1, -1), wq, wkv, wo, dy, positions.reshape(1, -1))
        return pl.pallas_call(
            copy_kernel,
            name="emit",
            in_specs=[ANY] * 5,
            out_specs=[ANY] * 5,
            out_shape=results,
            scratch_shapes=[VM(r.shape, r.dtype) for r in results] + [DMA((19,)), DMA((19,))],
            cost_estimate=pl.CostEstimate(flops=1_000_000, bytes_accessed=27_000_000, transcendentals=0),
            compiler_params=pltpu.CompilerParams(vmem_limit_bytes=60 * 2**20),
        )(*res[:5])

    return jax.shard_map(
        device_step,
        mesh=mesh,
        in_specs=(P("data", None), P("data", "model"), P("data", None), P("model", "data"), P(), P(), P("data", None)),
        out_specs=(P("data", None), P("data", None), P("data", "model"), P("data", None), P("model", "data")),
        check_vma=False,
    )
```

```python
import functools

import jax
import jax.numpy as jnp
from jax import lax
from jax.experimental import pallas as pl
from jax.experimental.pallas import tpu as pltpu
from jax.sharding import PartitionSpec as P

NORM_EPS = 1e-6
ROWS = 512
TOKS = 1536
SEQ = 128
D = 2048
CORE = 768
W = 512
PASS = 384
H = 256
WAYS = (1, -1)
HOPS = (1, 2, 3)
BF = jnp.bfloat16
F32 = jnp.float32


def dot(a, b):
    return jnp.dot(a, b, preferred_element_type=F32)


def dot_t(a, b):
    return lax.dot_general(a, b, (((1,), (1,)), ((), ())), preferred_element_type=F32)


def t_dot(a, b):
    return lax.dot_general(a, b, (((0,), (0,)), ((), ())), preferred_element_type=F32)


MESH = pl.DeviceIdType.MESH


def cols(i, width=H):
    return pl.ds(pl.multiple_of(i * width, width), width)


def norm(x):
    c = x - jnp.mean(x, axis=-1, keepdims=True)
    inv = lax.rsqrt(jnp.mean(c * c, axis=-1, keepdims=True) + NORM_EPS)
    return c * inv, inv


def stack_heads(a):
    return jnp.concatenate([a[:, :H], a[:, H:]], axis=0)


def spread_heads(a):
    return jnp.concatenate([a[:SEQ], a[SEQ:]], axis=1)


def softmax(s, mask2):
    s = jnp.where(mask2 > 0, s * (H ** -0.5), -1e30)
    e = jnp.exp(s - jnp.max(s, axis=-1, keepdims=True))
    return e / jnp.sum(e, axis=-1, keepdims=True)


def attend(qs, ks, vs, mask2):
    scores = [dot_t(q, k) for q, k in zip(qs, ks)]
    probs = [softmax(s, mask2) for s in scores]
    return probs, [dot(p.astype(BF), v).astype(BF) for p, v in zip(probs, vs)]


def attend_back(qs, ks, vs, probs, dos):
    dps = [dot_t(do, v) for do, v in zip(dos, vs)]
    dvs = [t_dot(p.astype(BF), do) for p, do in zip(probs, dos)]
    dss = [p * (dp - jnp.sum(p * dp, axis=-1, keepdims=True)) for p, dp in zip(probs, dps)]
    dss = [(ds * (H ** -0.5)).astype(BF) for ds in dss]
    dqs = [dot(ds, k).astype(BF) for ds, k in zip(dss, ks)]
    dks = [t_dot(ds, q) for ds, q in zip(dss, qs)]
    return dqs, dks, dvs


def drop(items, item):
    items[:] = [i for i in items if i is not item]


def layer_kernel(
    x_hbm, gain, wq_hbm, wkv_hbm, wo_hbm, dy_hbm, pos,
    y_out, dx_out, gq_out, gkv_out, go_out, wq_all, wo_all, o_all, dq_all, dkv_mate,
    xh, big, wq, wkv, wo, wqx, wox, q, k, v, probs, o, ox, dq, dqx, dkv,
    ofar, ory, orz, qfar, qry, qrz, kfar, kry, krz, tin, stage, dkvt, go_st, gq_st, gk_st,
    lsem, ssem, rsem, gss, gsr, dks, dkr,
):
    d, m = lax.axis_index("data"), lax.axis_index("model")
    z, y = d // 2, d % 2
    core = m % 2
    zpeer = [((z + s) % 4) * 2 + y for s in range(4)]
    ypeer = z * 2 + 1 - y
    mate = m + 1 - 2 * core
    across = (m + 2) % 4
    diag = (mate + 2) % 4
    mine = pl.ds(pl.multiple_of(core * CORE, CORE), CORE)
    theirs = pl.ds(pl.multiple_of((1 - core) * CORE, CORE), CORE)
    used = {"l": 0, "r": 0}
    sends = []

    def local(src, dst):
        i = used["l"]
        used["l"] += 1
        return pltpu.make_async_copy(src, dst, lsem.at[i])

    def remote(src, dst, land, axis, peer, when=None):
        i = used["r"]
        used["r"] += 1
        args = dict(send_sem=ssem.at[i], recv_sem=rsem.at[i], device_id={axis: peer}, device_id_type=MESH)
        out = pltpu.make_async_remote_copy(src_ref=src, dst_ref=dst, **args)
        back = pltpu.make_async_remote_copy(src_ref=land, dst_ref=land, **args)
        sends.append((when, out))
        return out, back

    loads = [local(x_hbm.at[cols(t, ROWS)], xh.at[cols(t, ROWS)]) for t in range(3)]
    half = cols(core)
    own = [local(wq_hbm, wq.at[cols(d)]), local(wkv_hbm.at[:, half], wkv.at[core, cols(d)]), local(wo_hbm, wo.at[:, cols(d)])]
    dy_load = local(dy_hbm, big.at[pl.ds(0, TOKS)])
    for c in loads + own + [dy_load]:
        c.start()

    barrier = pltpu.get_barrier_semaphore()
    for peer in zpeer[1:] + [ypeer]:
        pl.semaphore_signal(barrier, inc=1, device_id={"data": peer}, device_id_type=MESH)
    for peer in (mate, across, diag):
        pl.semaphore_signal(barrier, inc=1, device_id={"model": peer}, device_id_type=MESH)
    pl.semaphore_wait(barrier, 7)

    shard = {0: wq_hbm, 1: wkv_hbm.at[:, half], 3: wo_hbm}

    def slot(a, zz):
        blk = zz * 2 + (1 - y if a in (2, 4) else y)
        return wq.at[cols(blk)] if a == 0 else wkv.at[core, cols(blk)] if a < 3 else wo.at[:, cols(blk)]

    def got(way, r):
        return z >= r if way > 0 else z + r <= 3

    def origin(way, r):
        return (z + 4 - r) % 4 if way > 0 else (z + r) % 4

    def goes(way):
        return z < 3 if way > 0 else z > 0

    def sent(way, r):
        return goes(way) if r == 1 else jnp.logical_and(got(way, r - 1), goes(way))

    hops, ys, xs, cs = {}, {}, {}, {}
    for r in HOPS:
        for way in WAYS:
            for a in range(5):
                here = origin(way, r - 1)
                src = shard[a] if r == 1 and a in shard else slot(a, here)
                to = ((z + way + 4) % 4) * 2 + y
                hops[a, way, r] = remote(src, slot(a, here), slot(a, origin(way, r)), "data", to, sent(way, r))
    keys = [None] + [(way, r) for r in HOPS for way in WAYS]
    for a in (1, 3):
        ys[a, None] = remote(shard[a], slot(a, z), slot(a + 1, z), "data", ypeer)
    for key in keys:
        zz = z if key is None else origin(*key)
        cond = None if key is None else got(*key)
        there = wq.at[cols(zz * 2 + 1 - y)]
        src = wq_hbm if key is None else slot(0, zz)
        ys[0, key] = remote(src, slot(0, zz), there, "data", ypeer, cond)
        xs[0, key] = remote(src, wqx.at[cols(zz * 2 + y)], wqx.at[cols(zz * 2 + y)], "model", across, cond)
        xs[5, key] = remote(there, wqx.at[cols(zz * 2 + 1 - y)], wqx.at[cols(zz * 2 + 1 - y)], "model", across, cond)
        for a in (3, 4):
            src = shard[a] if key is None and a == 3 else slot(a, zz)
            to = wox.at[:, cols(zz * 2 + (y if a == 3 else 1 - y))]
            xs[a, key] = remote(src, to, to, "model", across, cond)
        for a in (1, 2):
            src = shard[a] if key is None and a == 1 else slot(a, zz)
            blk = zz * 2 + (y if a == 1 else 1 - y)
            cs[a, key] = remote(src, slot(a, zz), wkv.at[1 - core, cols(blk)], "model", mate, cond)

    def on(cond, fn):
        if cond is None:
            fn()
        else:
            pl.when(cond)(fn)

    def start_hop(a, way, r):
        on(sent(way, r), lambda: hops[a, way, r][0].start())

    for way in WAYS:
        start_hop(0, way, 1)
    ys[1, None][0].start()
    ys[0, None][0].start()
    xs[0, None][0].start()
    xs[3, None][0].start()
    cs[1, None][0].start()

    for t in range(3):
        loads[t].wait()

        @pl.loop(t * 4, t * 4 + 4)
        def _(i):
            r = cols(i, SEQ)
            n, _inv = norm(xh[r, :].astype(F32))
            xh[r, :] = (n * gain[...]).astype(BF)

    for c in own:
        c.wait()

    def take(arrays, way, r):
        for a in arrays:
            hops[a, way, r][1].wait_recv()
            if r < 3:
                start_hop(a, way, r + 1)
            if a == 0:
                ys[0, (way, r)][0].start()
            if a in (1, 2):
                cs[a, (way, r)][0].start()
            else:
                xs[a, (way, r)][0].start()

    def relay(arrays, r):
        for way in WAYS:
            on(jnp.logical_and(got(way, r), goes(way)), lambda way=way: take(arrays, way, r))

    def keep(arrays, r):
        for way in WAYS:
            on(jnp.logical_and(got(way, r), jnp.logical_not(goes(way))), lambda way=way: take(arrays, way, r))

    def take_all(arrays, r):
        for way in WAYS:
            on(got(way, r), lambda way=way: take(arrays, way, r))

    def arrive(key):
        def go():
            ys[0, key][1].wait_recv()
            xs[5, key][0].start()

        on(None if key is None else got(*key), go)

    take_all((0,), 1)
    take_all((0,), 2)
    ys[1, None][1].wait_recv()
    cs[2, None][0].start()
    for way in WAYS:
        for a in (1, 2):
            start_hop(a, way, 1)
    take_all((0,), 3)
    ys[3, None][0].start()
    take_all((1, 2), 1)
    for key in keys[:5]:
        arrive(key)
    relay((1, 2), 2)
    for way in WAYS:
        start_hop(3, way, 1)
    for key in keys[5:]:
        arrive(key)

    locals_ = []

    def share(src, dst, slot_of):
        c = local(src, dst.at[slot_of(0)])
        out, back = remote(src, dst.at[slot_of(0)], dst.at[slot_of(1)], "model", mate)
        c.start()
        out.start()
        locals_.append(c)
        return c, out, back

    def colslot(base):
        other = base + 1 - 2 * (base % 2)
        return lambda n: (slice(None), cols(base if n == 0 else other, W))

    def rowslot(base):
        other = base + 1 - 2 * (base % 2)
        return lambda n: (cols(base if n == 0 else other, W),)

    def share_rows(src, dst, base):
        other = base + 1 - 2 * (base % 2)
        c = local(src.at[mine], dst.at[:, cols(base, W)])
        out, back = remote(src.at[theirs], dst.at[:, cols(base, W)], dst.at[:, cols(other, W)], "model", mate)
        c.start()
        out.start()
        locals_.append(c)
        return c, out, back

    wq_sh = share(wq, wq_all, colslot(m))

    @pl.loop(0, 3)
    def _(t):
        r = cols(t, ROWS)
        q[r, :] = dot(xh[r, :], wq[...]).astype(BF)

    ys[3, None][1].wait_recv()
    xs[4, None][0].start()
    for way in WAYS:
        start_hop(4, way, 1)
    keep((1, 2), 2)
    take_all((1, 2), 3)
    for key in keys:
        on(None if key is None else got(*key), lambda key=key: [cs[a, key][1].wait_recv() for a in (1, 2)] and None)

    @pl.loop(0, 3)
    def _(t):
        r = cols(t, ROWS)
        k[r, :] = dot(xh[r, :], wkv[0]).astype(BF)
        v[r, :] = dot(xh[r, :], wkv[1]).astype(BF)

    posm = jnp.broadcast_to(pos[...].astype(F32), (SEQ, SEQ))
    mask = (posm <= posm.T).astype(F32)
    mask2 = jnp.concatenate([mask, mask], axis=0)

    @pl.loop(0, 3)
    def _(t):
        rows = [cols(t * 4 + b, SEQ) for b in range(4)]
        qs = [stack_heads(q[r, :]) for r in rows]
        ps, os = attend(qs, [k[r, :] for r in rows], [v[r, :] for r in rows], mask2)
        for b in range(4):
            probs[t * 4 + b] = ps[b]
            wide = spread_heads(os[b])
            o[rows[b], :] = wide
            big[pl.ds(TOKS, W), rows[b]] = wide.T

    dy_load.wait()
    o_sh = share_rows(o, o_all, m)

    far = [qfar, kfar, ofar]
    ry = [qry, kry, ory]
    rz = [qrz, krz, orz]

    def piece(g, blk):
        if g == 2:
            return dot(big[pl.ds(TOKS, W), pl.ds(0, TOKS)], big[pl.ds(0, TOKS), cols(blk)])
        return t_dot(xh[:, cols(blk)], dq[...] if g == 0 else q[:, cols(m, SEQ)])

    def ysend(g, kk):
        return pltpu.make_async_remote_copy(
            src_ref=far[g].at[kk], dst_ref=ry[g].at[kk], send_sem=gss.at[g, kk], recv_sem=gsr.at[g, kk],
            device_id={"data": ypeer}, device_id_type=MESH,
        )

    upper = z // 2
    inner = jnp.logical_and(z > 0, z < 3)

    def zcopy(g, kk, place, peer):
        return pltpu.make_async_remote_copy(
            src_ref=ry[g].at[kk], dst_ref=rz[g].at[place], send_sem=gss.at[g, 4 + kk], recv_sem=gsr.at[g, 4 + place],
            device_id={"data": peer}, device_id_type=MESH,
        )

    def zsend(g, kk):
        if kk == 2:
            return zcopy(g, kk, 2 + upper, (z + 1 - 2 * upper) * 2 + y)
        return zcopy(g, kk, kk // 2, zpeer[kk])

    def merge(g):
        @pl.when(inner)
        def _():
            for kk in (3, 1):
                zcopy(g, 2, 2 + kk // 2, ypeer).wait_recv()
                ry[g][kk] = ry[g][kk] + rz[g][2 + kk // 2]
                zsend(g, kk).start()

    def send_far(g, lo, hi):
        @pl.loop(lo, hi)
        def _(i):
            kk = 2 + i + (i // 2) * (1 - 2 * i)
            far[g][kk] = piece(g, ((z + kk) % 4) * 2 + 1 - y)
            ysend(g, kk).start()

    def near(g, kk):
        ysend(g, kk).wait_recv()
        ry[g][kk] = ry[g][kk] + piece(g, zpeer[kk])
        if kk == 2:
            zsend(g, kk).start()
        elif kk:
            pl.when(jnp.logical_not(inner))(lambda: zsend(g, kk).start())

    def finish(g, st):
        for kk in (1, 3):
            zsend(g, kk).wait_recv()
        st[...] = (ry[g][0] + rz[g][0] + rz[g][1]).astype(BF)

    send_far(2, 0, 4)
    relay((3, 4), 1)
    relay((3, 4), 2)
    near(2, 2)
    keep((3, 4), 1)
    keep((3, 4), 2)
    take_all((3, 4), 3)
    wo_sh = share(wo, wo_all, rowslot(m))

    def back_tile(t, q_of, ps, do, add):
        rows = [cols(t * 4 + b, SEQ) for b in range(4)]
        qs, ks, vs = q_of, [k[r, :] for r in rows], [v[r, :] for r in rows]
        dqs, dks, dvs = attend_back(qs, ks, vs, ps, [stack_heads(do[b * SEQ : (b + 1) * SEQ]) for b in range(4)])
        to = dqx if add else dq
        for b, r in enumerate(rows):
            to[r, :] = spread_heads(dqs[b])
            dkv[r, :H] = dkv[r, :H] + dks[b] if add else dks[b]
            dkv[r, H:] = dkv[r, H:] + dvs[b] if add else dvs[b]

    @pl.loop(0, 3)
    def _(t):
        do = dot_t(big[cols(t, ROWS), :], wo[...]).astype(BF)
        qs = [stack_heads(q[cols(t * 4 + b, SEQ), :]) for b in range(4)]
        back_tile(t, qs, [probs[t * 4 + b] for b in range(4)], do, False)

    dq_sh = share_rows(dq, dq_all, m)
    send_far(0, 0, 4)
    near(2, 3)
    near(2, 1)
    merge(2)

    for key in keys:
        on(None if key is None else got(*key), lambda key=key: [xs[a, key][1].wait_recv() for a in (0, 3, 4, 5)] and None)
    wqx_sh = share(wqx, wq_all, colslot(across))
    wox_sh = share(wox, wo_all, rowslot(across))

    def dkv_send(t):
        r = cols(t, ROWS)
        return pltpu.make_async_remote_copy(
            src_ref=dkv.at[r], dst_ref=dkv_mate.at[r], send_sem=dks.at[t], recv_sem=dkr.at[t],
            device_id={"model": mate}, device_id_type=MESH,
        )

    @pl.loop(0, 3)
    def _(t):
        rows = [cols(t * 4 + b, SEQ) for b in range(4)]
        qm = dot(xh[cols(t, ROWS), :], wqx[...]).astype(BF)
        do = dot_t(big[cols(t, ROWS), :], wox[...]).astype(BF)
        qs = [stack_heads(qm[b * SEQ : (b + 1) * SEQ]) for b in range(4)]
        ps, os = attend(qs, [k[r, :] for r in rows], [v[r, :] for r in rows], mask2)
        for b in range(4):
            ox[rows[b], :] = spread_heads(os[b])
        back_tile(t, qs, ps, do, True)
        dkv_send(t).start()

    ox_sh = share_rows(ox, o_all, across)
    dqx_sh = share_rows(dqx, dq_all, across)

    tiles = []
    for t in range(3):
        dkv_send(t).wait_recv()
        tiles.append(local(dkv_mate.at[cols(t, ROWS)], dkvt.at[t % 2]))
        if t < 2:
            tiles[t].start()
    for t in range(3):
        tiles[t].wait()
        q[cols(t, ROWS), :] = (dkv[cols(t, ROWS), :] + dkvt[t % 2]).astype(BF)
        if t == 0:
            tiles[2].start()
    send_far(1, 0, 4)
    near(2, 0)
    near(0, 2)

    for sh in (wo_sh, wox_sh, o_sh, ox_sh):
        sh[0].wait()
        sh[2].wait_recv()
        drop(locals_, sh[0])
    fetch = local(o_all, tin)
    fetch.start()
    fill = [local(wo_all.at[:, cols(i, W)], big.at[:, cols(i, W)]) for i in range(4)]
    for c in fill:
        c.start()
    fetch.wait()

    def y_cols(lo, hi):
        @pl.loop(lo, hi)
        def _(i):
            stage[:, cols(i)] = dot(tin[...], big[:, cols(i)]).astype(BF)

    done = []

    def emit(dst):
        c = local(stage, dst.at[mine])
        out, back = remote(stage, dst.at[mine], dst.at[theirs], "model", mate)
        c.start()
        out.start()
        done.append((c, out, back))

    for i in range(4):
        fill[i].wait()
        y_cols(2 * i, 2 * i + 2)
        if i == 1:
            near(0, 3)
    emit(y_out)

    for sh in (wq_sh, wqx_sh, dq_sh, dqx_sh):
        sh[0].wait()
        sh[2].wait_recv()
        drop(locals_, sh[0])
    fetch = local(dq_all, tin)
    fetch.start()
    fill = [local(wq_all.at[cols(i, W)], big.at[cols(i, W)]) for i in range(4)]
    for c in fill:
        c.start()
    wox_sh[1].wait_send()
    sends[:] = [s for s in sends if s[1] is not wox_sh[1]]
    xin = [local(x_hbm.at[pl.ds(pl.multiple_of(core * CORE + p * PASS, PASS), PASS)], wox.at[pl.ds(0, PASS)]) for p in range(2)]
    xin[0].start()
    for t in range(3):
        dkv_send(t).wait_send()
    near(0, 1)
    merge(0)
    fetch.wait()
    for p in range(2):
        rows = pl.ds(pl.multiple_of(core * CORE + p * PASS, PASS), PASS)

        def dh_cols(i):
            c = cols(i, W)
            g = dot_t(tin[pl.ds(p * PASS, PASS), :], big[c, :])
            g = g + dot_t(q[rows, :H], wkv[0, c, :])
            dkv[cols(i, PASS), :] = g + dot_t(q[rows, H:], wkv[1, c, :])

        if p == 0:
            for n in range(4):
                fill[n].wait()
                pl.loop(n, n + 1)(dh_cols)
        else:
            pl.loop(0, 4)(dh_cols)

        xin[p].wait()
        if p == 0:
            done[0][0].wait()
            done[0][1].wait_send()
            sends[:] = [s for s in sends if s[1] is not done[0][1]]

        @pl.loop(0, 3)
        def _(i):
            n, inv = norm(wox[cols(i, SEQ), :].astype(F32))
            gn = jnp.concatenate([dkv[pl.ds(pl.multiple_of(c * PASS + i * SEQ, SEQ), SEQ), :] for c in range(4)], axis=1) * gain[...]
            g = inv * (gn - jnp.mean(gn, axis=-1, keepdims=True) - n * jnp.mean(gn * n, axis=-1, keepdims=True))
            stage[pl.ds(pl.multiple_of(p * PASS + i * SEQ, SEQ), SEQ), :] = g.astype(BF)

        if p == 0:
            xin[1].start()
            near(0, 0)
    emit(dx_out)

    for kk in (2, 3, 1):
        near(1, kk)
    merge(1)
    near(1, 0)
    finish(2, go_st)
    fin = [local(go_st, go_out)]
    fin[0].start()
    finish(0, gq_st)
    fin.append(local(gq_st, gq_out))
    fin[1].start()
    finish(1, gk_st)
    fin.append(local(gk_st, gkv_out.at[:, cols(m, SEQ)]))
    fin[2].start()
    backs = []
    for peer in (mate, across, diag):
        out, back = remote(gk_st, gkv_out.at[:, cols(m, SEQ)], gkv_out.at[:, cols(peer, SEQ)], "model", peer)
        out.start()
        backs.append(back)

    for b in backs:
        b.wait_recv()
    done[1][0].wait()
    for c, out, back in done:
        back.wait_recv()
    for cond, c in sends:
        on(cond, c.wait_send)
    for c in locals_ + fin:
        c.wait()
    for g in range(3):
        for kk in range(4):
            ysend(g, kk).wait_send()
            if kk:
                zsend(g, kk).wait_send()


def copy_kernel(*refs):
    srcs, dsts, bufs, rsem, wsem = refs[:5], refs[5:10], refs[10:15], refs[15], refs[16]
    ins, outs = [], []
    for a in range(5):
        rows = srcs[a].shape[0]
        parts = 8 if a < 2 else 1
        for c in range(parts):
            r = pl.ds(c * (rows // parts), rows // parts)
            i = len(ins)
            ins.append(pltpu.make_async_copy(srcs[a].at[r], bufs[a].at[r], rsem.at[i]))
            outs.append(pltpu.make_async_copy(bufs[a].at[r], dsts[a].at[r], wsem.at[i]))
    for c in ins:
        c.start()
    for i, o in zip(ins, outs):
        i.wait()
        o.start()
    for o in outs:
        o.wait()


def solution(mesh):
    sd = jax.ShapeDtypeStruct
    DMA = pltpu.SemaphoreType.DMA
    VM = pltpu.VMEM
    ANY = pl.BlockSpec(memory_space=pl.ANY)
    IN_VM = pl.BlockSpec(memory_space=pltpu.VMEM)

    def device_step(x, wq, wkv, wo, gain, positions, dy):
        results = [
            sd((TOKS, D), BF), sd((TOKS, D), BF), sd((H, W), BF), sd((H, W), BF), sd((W, H), BF),
        ]
        outs = results + [
            sd((D, D), BF), sd((D, D), BF), sd((CORE, D), BF), sd((CORE, D), BF), sd((TOKS, W), F32),
        ]
        wide, narrow = VM((TOKS, W), BF), VM((TOKS, H), BF)
        scratch = [
            VM((TOKS, D), BF), VM((D, D), BF), VM((D, W), BF), VM((2, D, H), BF), VM((W, D), BF),
            VM((D, W), BF), VM((W, D), BF), wide, narrow, narrow, VM((12, H, SEQ), F32),
            wide, wide, wide, wide, VM((TOKS, W), F32),
            VM((4, W, H), F32), VM((4, W, H), F32), VM((4, W, H), F32),
            VM((4, H, W), F32), VM((4, H, W), F32), VM((4, H, W), F32),
            VM((4, H, SEQ), F32), VM((4, H, SEQ), F32), VM((4, H, SEQ), F32),
            VM((CORE, D), BF), VM((CORE, D), BF), VM((2, W, W), F32),
            VM((W, H), BF), VM((H, W), BF), VM((H, SEQ), BF),
            DMA((48,)), DMA((112,)), DMA((112,)), DMA((3, 8)), DMA((3, 8)), DMA((3,)), DMA((3,)),
        ]
        res = pl.pallas_call(
            layer_kernel,
            name="layer",
            in_specs=[ANY, IN_VM, ANY, ANY, ANY, ANY, IN_VM],
            out_specs=[ANY] * len(outs),
            out_shape=outs,
            scratch_shapes=scratch,
            cost_estimate=pl.CostEstimate(flops=80_000_000_000, bytes_accessed=100_000_000, transcendentals=0),
            compiler_params=pltpu.CompilerParams(collective_id=0, has_side_effects=True, vmem_limit_bytes=67043328),
        )(x, gain.reshape(1, -1), wq, wkv, wo, dy, positions.reshape(1, -1))
        return pl.pallas_call(
            copy_kernel,
            name="emit",
            in_specs=[ANY] * 5,
            out_specs=[ANY] * 5,
            out_shape=results,
            scratch_shapes=[VM(r.shape, r.dtype) for r in results] + [DMA((19,)), DMA((19,))],
            cost_estimate=pl.CostEstimate(flops=1_000_000, bytes_accessed=27_000_000, transcendentals=0),
            compiler_params=pltpu.CompilerParams(vmem_limit_bytes=60 * 2**20),
        )(*res[:5])

    return jax.shard_map(
        device_step,
        mesh=mesh,
        in_specs=(P("data", None), P("data", "model"), P("data", None), P("model", "data"), P(), P(), P("data", None)),
        out_specs=(P("data", None), P("data", None), P("data", "model"), P("data", None), P("model", "data")),
        check_vma=False,
    )
```

```python
import functools

import jax
import jax.numpy as jnp
from jax import lax
from jax.experimental import pallas as pl
from jax.experimental.pallas import tpu as pltpu
from jax.sharding import PartitionSpec as P

NORM_EPS = 1e-6
ROWS = 512
TOKS = 1536
SEQ = 128
D = 2048
CORE = 768
W = 512
PASS = 384
H = 256
WAYS = (1, -1)
HOPS = (1, 2, 3)
BF = jnp.bfloat16
F32 = jnp.float32


def dot(a, b):
    return jnp.dot(a, b, preferred_element_type=F32)


def dot_t(a, b):
    return lax.dot_general(a, b, (((1,), (1,)), ((), ())), preferred_element_type=F32)


def t_dot(a, b):
    return lax.dot_general(a, b, (((0,), (0,)), ((), ())), preferred_element_type=F32)


MESH = pl.DeviceIdType.MESH


def cols(i, width=H):
    return pl.ds(pl.multiple_of(i * width, width), width)


def norm(x):
    c = x - jnp.mean(x, axis=-1, keepdims=True)
    inv = lax.rsqrt(jnp.mean(c * c, axis=-1, keepdims=True) + NORM_EPS)
    return c * inv, inv


def stack_heads(a):
    return jnp.concatenate([a[:, :H], a[:, H:]], axis=0)


def spread_heads(a):
    return jnp.concatenate([a[:SEQ], a[SEQ:]], axis=1)


def softmax(s, mask2):
    s = jnp.where(mask2 > 0, s * (H ** -0.5), -1e30)
    e = jnp.exp(s - jnp.max(s, axis=-1, keepdims=True))
    return e / jnp.sum(e, axis=-1, keepdims=True)


def attend(qs, ks, vs, mask2):
    scores = [dot_t(q, k) for q, k in zip(qs, ks)]
    probs = [softmax(s, mask2) for s in scores]
    return probs, [dot(p.astype(BF), v).astype(BF) for p, v in zip(probs, vs)]


def attend_back(qs, ks, vs, probs, dos):
    dps = [dot_t(do, v) for do, v in zip(dos, vs)]
    dvs = [t_dot(p.astype(BF), do) for p, do in zip(probs, dos)]
    dss = [p * (dp - jnp.sum(p * dp, axis=-1, keepdims=True)) for p, dp in zip(probs, dps)]
    dss = [(ds * (H ** -0.5)).astype(BF) for ds in dss]
    dqs = [dot(ds, k).astype(BF) for ds, k in zip(dss, ks)]
    dks = [t_dot(ds, q) for ds, q in zip(dss, qs)]
    return dqs, dks, dvs


def drop(items, item):
    items[:] = [i for i in items if i is not item]


def layer_kernel(
    x_hbm, gain, wq_hbm, wkv_hbm, wo_hbm, dy_hbm, pos,
    y_out, dx_out, gq_out, gkv_out, go_out, wq_all, wo_all, o_all, dq_all, dkv_mate,
    xh, big, wq, wkv, wo, wqx, wox, q, k, v, probs, o, ox, dq, dqx, dkv,
    ofar, ory, orz, qfar, qry, qrz, kfar, kry, krz, tin, stage, dkvt, go_st, gq_st, gk_st,
    lsem, ssem, rsem, gss, gsr, dks, dkr,
):
    d, m = lax.axis_index("data"), lax.axis_index("model")
    z, y = d // 2, d % 2
    core = m % 2
    zpeer = [((z + s) % 4) * 2 + y for s in range(4)]
    ypeer = z * 2 + 1 - y
    mate = m + 1 - 2 * core
    across = (m + 2) % 4
    diag = (mate + 2) % 4
    mine = pl.ds(pl.multiple_of(core * CORE, CORE), CORE)
    theirs = pl.ds(pl.multiple_of((1 - core) * CORE, CORE), CORE)
    used = {"l": 0, "r": 0}
    sends = []

    def local(src, dst):
        i = used["l"]
        used["l"] += 1
        return pltpu.make_async_copy(src, dst, lsem.at[i])

    def remote(src, dst, land, axis, peer, when=None):
        i = used["r"]
        used["r"] += 1
        args = dict(send_sem=ssem.at[i], recv_sem=rsem.at[i], device_id={axis: peer}, device_id_type=MESH)
        out = pltpu.make_async_remote_copy(src_ref=src, dst_ref=dst, **args)
        back = pltpu.make_async_remote_copy(src_ref=land, dst_ref=land, **args)
        sends.append((when, out))
        return out, back

    loads = [local(x_hbm.at[cols(t, ROWS)], xh.at[cols(t, ROWS)]) for t in range(3)]
    half = cols(core)
    own = [local(wq_hbm, wq.at[cols(d)]), local(wkv_hbm.at[:, half], wkv.at[core, cols(d)]), local(wo_hbm, wo.at[:, cols(d)])]
    dy_load = local(dy_hbm, big.at[pl.ds(0, TOKS)])
    for c in loads + own + [dy_load]:
        c.start()

    barrier = pltpu.get_barrier_semaphore()
    for peer in zpeer[1:] + [ypeer]:
        pl.semaphore_signal(barrier, inc=1, device_id={"data": peer}, device_id_type=MESH)
    for peer in (mate, across, diag):
        pl.semaphore_signal(barrier, inc=1, device_id={"model": peer}, device_id_type=MESH)
    pl.semaphore_wait(barrier, 7)

    shard = {0: wq_hbm, 1: wkv_hbm.at[:, half], 3: wo_hbm}

    def slot(a, zz):
        blk = zz * 2 + (1 - y if a in (2, 4) else y)
        return wq.at[cols(blk)] if a == 0 else wkv.at[core, cols(blk)] if a < 3 else wo.at[:, cols(blk)]

    def got(way, r):
        return z >= r if way > 0 else z + r <= 3

    def origin(way, r):
        return (z + 4 - r) % 4 if way > 0 else (z + r) % 4

    def goes(way):
        return z < 3 if way > 0 else z > 0

    def sent(way, r):
        return goes(way) if r == 1 else jnp.logical_and(got(way, r - 1), goes(way))

    hops, ys, xs, cs = {}, {}, {}, {}
    for r in HOPS:
        for way in WAYS:
            for a in (0, 1, 3, 4):
                here = origin(way, r - 1)
                src = shard[a] if r == 1 and a in shard else slot(a, here)
                to = ((z + way + 4) % 4) * 2 + y
                hops[a, way, r] = remote(src, slot(a, here), slot(a, origin(way, r)), "data", to, sent(way, r))
    keys = [None] + [(way, r) for r in HOPS for way in WAYS]
    ys[3, None] = remote(wo_hbm, slot(3, z), slot(4, z), "data", ypeer)
    for key in keys:
        zz = z if key is None else origin(*key)
        cond = None if key is None else got(*key)
        there = wq.at[cols(zz * 2 + 1 - y)]
        src = wq_hbm if key is None else slot(0, zz)
        ys[0, key] = remote(src, slot(0, zz), there, "data", ypeer, cond)
        xs[0, key] = remote(src, wqx.at[cols(zz * 2 + y)], wqx.at[cols(zz * 2 + y)], "model", across, cond)
        xs[5, key] = remote(there, wqx.at[cols(zz * 2 + 1 - y)], wqx.at[cols(zz * 2 + 1 - y)], "model", across, cond)
        for a in (3, 4):
            src = shard[a] if key is None and a == 3 else slot(a, zz)
            to = wox.at[:, cols(zz * 2 + (y if a == 3 else 1 - y))]
            xs[a, key] = remote(src, to, to, "model", across, cond)
        src = shard[1] if key is None else slot(1, zz)
        ys[1, key] = remote(src, slot(1, zz), slot(2, zz), "data", ypeer, cond)
        for a in (1, 2):
            blk = zz * 2 + (y if a == 1 else 1 - y)
            cs[a, key] = remote(src if a == 1 else slot(2, zz), slot(a, zz), wkv.at[1 - core, cols(blk)], "model", mate, cond)

    def on(cond, fn):
        if cond is None:
            fn()
        else:
            pl.when(cond)(fn)

    def start_hop(a, way, r):
        on(sent(way, r), lambda: hops[a, way, r][0].start())

    for way in WAYS:
        start_hop(0, way, 1)
    ys[0, None][0].start()
    ys[1, None][0].start()
    xs[0, None][0].start()
    xs[3, None][0].start()
    cs[1, None][0].start()

    for t in range(3):
        loads[t].wait()

        @pl.loop(t * 4, t * 4 + 4)
        def _(i):
            r = cols(i, SEQ)
            n, _inv = norm(xh[r, :].astype(F32))
            xh[r, :] = (n * gain[...]).astype(BF)

    for c in own:
        c.wait()

    def take(arrays, way, r):
        for a in arrays:
            hops[a, way, r][1].wait_recv()
            if r < 3:
                start_hop(a, way, r + 1)
            if a < 2:
                ys[a, (way, r)][0].start()
            (cs if a == 1 else xs)[a, (way, r)][0].start()

    def relay(arrays, r):
        for way in WAYS:
            on(jnp.logical_and(got(way, r), goes(way)), lambda way=way: take(arrays, way, r))

    def keep(arrays, r):
        for way in WAYS:
            on(jnp.logical_and(got(way, r), jnp.logical_not(goes(way))), lambda way=way: take(arrays, way, r))

    def take_all(arrays, r):
        for way in WAYS:
            on(got(way, r), lambda way=way: take(arrays, way, r))

    def arrive(a, key):
        def go():
            ys[a, key][1].wait_recv()
            (cs[2, key] if a else xs[5, key])[0].start()

        on(None if key is None else got(*key), go)

    take_all((0,), 1)
    take_all((0,), 2)
    for way in WAYS:
        start_hop(1, way, 1)
    take_all((0,), 3)
    take_all((1,), 1)
    for key in keys[:5]:
        arrive(0, key)
    relay((1,), 2)
    for way in WAYS:
        start_hop(3, way, 1)
    for key in keys[5:]:
        arrive(0, key)

    locals_ = []

    def share(src, dst, slot_of):
        c = local(src, dst.at[slot_of(0)])
        out, back = remote(src, dst.at[slot_of(0)], dst.at[slot_of(1)], "model", mate)
        c.start()
        out.start()
        locals_.append(c)
        return c, out, back

    def colslot(base):
        other = base + 1 - 2 * (base % 2)
        return lambda n: (slice(None), cols(base if n == 0 else other, W))

    def rowslot(base):
        other = base + 1 - 2 * (base % 2)
        return lambda n: (cols(base if n == 0 else other, W),)

    def share_rows(src, dst, base):
        other = base + 1 - 2 * (base % 2)
        c = local(src.at[mine], dst.at[:, cols(base, W)])
        out, back = remote(src.at[theirs], dst.at[:, cols(base, W)], dst.at[:, cols(other, W)], "model", mate)
        c.start()
        out.start()
        locals_.append(c)
        return c, out, back

    wq_sh = share(wq, wq_all, colslot(m))

    @pl.loop(0, 3)
    def _(t):
        r = cols(t, ROWS)
        q[r, :] = dot(xh[r, :], wq[...]).astype(BF)

    keep((1,), 2)
    take_all((1,), 3)
    ys[3, None][0].start()
    for key in keys:
        arrive(1, key)
    for key in keys:
        on(None if key is None else got(*key), lambda key=key: [cs[a, key][1].wait_recv() for a in (1, 2)] and None)

    @pl.loop(0, 3)
    def _(t):
        r = cols(t, ROWS)
        k[r, :] = dot(xh[r, :], wkv[0]).astype(BF)
        v[r, :] = dot(xh[r, :], wkv[1]).astype(BF)

    ys[3, None][1].wait_recv()
    xs[4, None][0].start()
    for way in WAYS:
        start_hop(4, way, 1)
    posm = jnp.broadcast_to(pos[...].astype(F32), (SEQ, SEQ))
    mask = (posm <= posm.T).astype(F32)
    mask2 = jnp.concatenate([mask, mask], axis=0)

    @pl.loop(0, 3)
    def _(t):
        rows = [cols(t * 4 + b, SEQ) for b in range(4)]
        qs = [stack_heads(q[r, :]) for r in rows]
        ps, os = attend(qs, [k[r, :] for r in rows], [v[r, :] for r in rows], mask2)
        for b in range(4):
            probs[t * 4 + b] = ps[b]
            wide = spread_heads(os[b])
            o[rows[b], :] = wide
            big[pl.ds(TOKS, W), rows[b]] = wide.T

    dy_load.wait()
    o_sh = share_rows(o, o_all, m)

    far = [qfar, kfar, ofar]
    ry = [qry, kry, ory]
    rz = [qrz, krz, orz]

    def piece(g, blk):
        if g == 2:
            return dot(big[pl.ds(TOKS, W), pl.ds(0, TOKS)], big[pl.ds(0, TOKS), cols(blk)])
        return t_dot(xh[:, cols(blk)], dq[...] if g == 0 else q[:, cols(m, SEQ)])

    def ysend(g, kk):
        return pltpu.make_async_remote_copy(
            src_ref=far[g].at[kk], dst_ref=ry[g].at[kk], send_sem=gss.at[g, kk], recv_sem=gsr.at[g, kk],
            device_id={"data": ypeer}, device_id_type=MESH,
        )

    upper = z // 2
    inner = jnp.logical_and(z > 0, z < 3)

    def zcopy(g, kk, place, peer):
        return pltpu.make_async_remote_copy(
            src_ref=ry[g].at[kk], dst_ref=rz[g].at[place], send_sem=gss.at[g, 4 + kk], recv_sem=gsr.at[g, 4 + place],
            device_id={"data": peer}, device_id_type=MESH,
        )

    def zsend(g, kk):
        if kk == 2 and g != 1:
            return zcopy(g, kk, 2 + upper, (z + 1 - 2 * upper) * 2 + y)
        if kk == 2:
            return zcopy(g, kk, 2, zpeer[2])
        return zcopy(g, kk, kk // 2, zpeer[kk])

    def merge(g):
        @pl.when(inner)
        def _():
            for kk in (3, 1):
                zcopy(g, 2, 2 + kk // 2, ypeer).wait_recv()
                ry[g][kk] = ry[g][kk] + rz[g][2 + kk // 2]
                zsend(g, kk).start()

    def send_far(g, lo, hi):
        @pl.loop(lo, hi)
        def _(i):
            kk = 2 + i + (i // 2) * (1 - 2 * i)
            far[g][kk] = piece(g, ((z + kk) % 4) * 2 + 1 - y)
            ysend(g, kk).start()

    def near(g, kk):
        ysend(g, kk).wait_recv()
        ry[g][kk] = ry[g][kk] + piece(g, zpeer[kk])
        if kk == 2 or kk and g == 1:
            zsend(g, kk).start()
        elif kk:
            pl.when(jnp.logical_not(inner))(lambda: zsend(g, kk).start())

    def finish(g, st):
        for kk in (1, 3):
            zsend(g, kk).wait_recv()
        total = ry[g][0] + rz[g][0] + rz[g][1]
        if g == 1:
            zsend(g, 2).wait_recv()
            total = total + rz[g][2]
        st[...] = total.astype(BF)

    send_far(2, 0, 4)
    relay((3, 4), 1)
    relay((3, 4), 2)
    near(2, 2)
    keep((3, 4), 1)
    keep((3, 4), 2)
    take_all((3, 4), 3)
    wo_sh = share(wo, wo_all, rowslot(m))

    def back_tile(t, q_of, ps, do, add):
        rows = [cols(t * 4 + b, SEQ) for b in range(4)]
        qs, ks, vs = q_of, [k[r, :] for r in rows], [v[r, :] for r in rows]
        dqs, dks, dvs = attend_back(qs, ks, vs, ps, [stack_heads(do[b * SEQ : (b + 1) * SEQ]) for b in range(4)])
        to = dqx if add else dq
        for b, r in enumerate(rows):
            to[r, :] = spread_heads(dqs[b])
            dkv[r, :H] = dkv[r, :H] + dks[b] if add else dks[b]
            dkv[r, H:] = dkv[r, H:] + dvs[b] if add else dvs[b]

    @pl.loop(0, 3)
    def _(t):
        do = dot_t(big[cols(t, ROWS), :], wo[...]).astype(BF)
        qs = [stack_heads(q[cols(t * 4 + b, SEQ), :]) for b in range(4)]
        back_tile(t, qs, [probs[t * 4 + b] for b in range(4)], do, False)

    dq_sh = share_rows(dq, dq_all, m)
    send_far(0, 0, 3)
    near(2, 3)
    near(2, 1)
    merge(2)

    for key in keys:
        on(None if key is None else got(*key), lambda key=key: [xs[a, key][1].wait_recv() for a in (0, 5)] and None)
    wqx_sh = share(wqx, wq_all, colslot(across))

    @pl.loop(0, 3)
    def _(t):
        rows = [cols(t * 4 + b, SEQ) for b in range(4)]
        qm = dot(xh[cols(t, ROWS), :], wqx[...]).astype(BF)
        qs = [stack_heads(qm[b * SEQ : (b + 1) * SEQ]) for b in range(4)]
        ps, os = attend(qs, [k[r, :] for r in rows], [v[r, :] for r in rows], mask2)
        dqx[cols(t, ROWS), :] = qm
        for b in range(4):
            probs[t * 4 + b] = ps[b]
            ox[rows[b], :] = spread_heads(os[b])

    ox_sh = share_rows(ox, o_all, across)
    for key in keys:
        on(None if key is None else got(*key), lambda key=key: [xs[a, key][1].wait_recv() for a in (3, 4)] and None)
    wox_sh = share(wox, wo_all, rowslot(across))

    def dkv_send(t):
        r = cols(t, ROWS)
        return pltpu.make_async_remote_copy(
            src_ref=dkv.at[r], dst_ref=dkv_mate.at[r], send_sem=dks.at[t], recv_sem=dkr.at[t],
            device_id={"model": mate}, device_id_type=MESH,
        )

    @pl.loop(0, 3)
    def _(t):
        do = dot_t(big[cols(t, ROWS), :], wox[...]).astype(BF)
        qs = [stack_heads(dqx[cols(t * 4 + b, SEQ), :]) for b in range(4)]
        back_tile(t, qs, [probs[t * 4 + b] for b in range(4)], do, True)
        dkv_send(t).start()

    dqx_sh = share_rows(dqx, dq_all, across)

    tiles = []
    for t in range(3):
        dkv_send(t).wait_recv()
        tiles.append(local(dkv_mate.at[cols(t, ROWS)], dkvt.at[t % 2]))
        if t < 2:
            tiles[t].start()
    for t in range(3):
        tiles[t].wait()
        q[cols(t, ROWS), :] = (dkv[cols(t, ROWS), :] + dkvt[t % 2]).astype(BF)
        if t == 0:
            tiles[2].start()
    send_far(1, 0, 4)
    send_far(0, 3, 4)
    near(2, 0)
    near(0, 2)

    for sh in (wo_sh, wox_sh, o_sh, ox_sh):
        sh[0].wait()
        sh[2].wait_recv()
        drop(locals_, sh[0])
    fetch = local(o_all, tin)
    fetch.start()
    fill = [local(wo_all.at[:, cols(i, W)], big.at[:, cols(i, W)]) for i in range(4)]
    for c in fill:
        c.start()
    fetch.wait()

    def y_cols(lo, hi):
        @pl.loop(lo, hi)
        def _(i):
            stage[:, cols(i)] = dot(tin[...], big[:, cols(i)]).astype(BF)

    done = []

    def emit(dst):
        c = local(stage, dst.at[mine])
        out, back = remote(stage, dst.at[mine], dst.at[theirs], "model", mate)
        c.start()
        out.start()
        done.append((c, out, back))

    for i in range(4):
        fill[i].wait()
        y_cols(2 * i, 2 * i + 2)
        if i == 1:
            near(0, 3)
    emit(y_out)

    for sh in (wq_sh, wqx_sh, dq_sh, dqx_sh):
        sh[0].wait()
        sh[2].wait_recv()
        drop(locals_, sh[0])
    fetch = local(dq_all, tin)
    fetch.start()
    fill = [local(wq_all.at[cols(i, W)], big.at[cols(i, W)]) for i in range(4)]
    for c in fill:
        c.start()
    wox_sh[1].wait_send()
    sends[:] = [s for s in sends if s[1] is not wox_sh[1]]
    xin = [local(x_hbm.at[pl.ds(pl.multiple_of(core * CORE + p * PASS, PASS), PASS)], wox.at[pl.ds(0, PASS)]) for p in range(2)]
    xin[0].start()
    for t in range(3):
        dkv_send(t).wait_send()
    near(0, 1)
    merge(0)
    fetch.wait()
    for p in range(2):
        rows = pl.ds(pl.multiple_of(core * CORE + p * PASS, PASS), PASS)

        def dh_cols(i):
            c = cols(i, W)
            g = dot_t(tin[pl.ds(p * PASS, PASS), :], big[c, :])
            g = g + dot_t(q[rows, :H], wkv[0, c, :])
            dkv[cols(i, PASS), :] = g + dot_t(q[rows, H:], wkv[1, c, :])

        if p == 0:
            for n in range(4):
                fill[n].wait()
                pl.loop(n, n + 1)(dh_cols)
        else:
            pl.loop(0, 4)(dh_cols)

        xin[p].wait()
        if p == 0:
            done[0][0].wait()
            done[0][1].wait_send()
            sends[:] = [s for s in sends if s[1] is not done[0][1]]

        @pl.loop(0, 3)
        def _(i):
            n, inv = norm(wox[cols(i, SEQ), :].astype(F32))
            gn = jnp.concatenate([dkv[pl.ds(pl.multiple_of(c * PASS + i * SEQ, SEQ), SEQ), :] for c in range(4)], axis=1) * gain[...]
            g = inv * (gn - jnp.mean(gn, axis=-1, keepdims=True) - n * jnp.mean(gn * n, axis=-1, keepdims=True))
            stage[pl.ds(pl.multiple_of(p * PASS + i * SEQ, SEQ), SEQ), :] = g.astype(BF)

        if p == 0:
            xin[1].start()
            for kk in (2, 3, 1, 0):
                near(1, kk)
    emit(dx_out)

    finish(2, go_st)
    fin = [local(go_st, go_out)]
    fin[0].start()
    finish(1, gk_st)
    fin.append(local(gk_st, gkv_out.at[:, cols(m, SEQ)]))
    fin[1].start()
    backs = []
    for peer in (mate, across, diag):
        out, back = remote(gk_st, gkv_out.at[:, cols(m, SEQ)], gkv_out.at[:, cols(peer, SEQ)], "model", peer)
        out.start()
        backs.append(back)

    near(0, 0)
    finish(0, gq_st)
    fin.append(local(gq_st, gq_out))
    fin[2].start()
    for b in backs:
        b.wait_recv()
    done[1][0].wait()
    for c, out, back in done:
        back.wait_recv()
    for cond, c in sends:
        on(cond, c.wait_send)
    for c in locals_ + fin:
        c.wait()
    for g in range(3):
        for kk in range(4):
            ysend(g, kk).wait_send()
            if kk:
                zsend(g, kk).wait_send()


def copy_kernel(*refs):
    srcs, dsts, bufs, rsem, wsem = refs[:5], refs[5:10], refs[10:15], refs[15], refs[16]
    ins, outs = [], []
    for a in range(5):
        rows = srcs[a].shape[0]
        parts = 8 if a < 2 else 1
        for c in range(parts):
            r = pl.ds(c * (rows // parts), rows // parts)
            i = len(ins)
            ins.append(pltpu.make_async_copy(srcs[a].at[r], bufs[a].at[r], rsem.at[i]))
            outs.append(pltpu.make_async_copy(bufs[a].at[r], dsts[a].at[r], wsem.at[i]))
    for c in ins:
        c.start()
    for i, o in zip(ins, outs):
        i.wait()
        o.start()
    for o in outs:
        o.wait()


def solution(mesh):
    sd = jax.ShapeDtypeStruct
    DMA = pltpu.SemaphoreType.DMA
    VM = pltpu.VMEM
    ANY = pl.BlockSpec(memory_space=pl.ANY)
    IN_VM = pl.BlockSpec(memory_space=pltpu.VMEM)

    def device_step(x, wq, wkv, wo, gain, positions, dy):
        results = [
            sd((TOKS, D), BF), sd((TOKS, D), BF), sd((H, W), BF), sd((H, W), BF), sd((W, H), BF),
        ]
        outs = results + [
            sd((D, D), BF), sd((D, D), BF), sd((CORE, D), BF), sd((CORE, D), BF), sd((TOKS, W), F32),
        ]
        wide, narrow = VM((TOKS, W), BF), VM((TOKS, H), BF)
        scratch = [
            VM((TOKS, D), BF), VM((D, D), BF), VM((D, W), BF), VM((2, D, H), BF), VM((W, D), BF),
            VM((D, W), BF), VM((W, D), BF), wide, narrow, narrow, VM((12, H, SEQ), F32),
            wide, wide, wide, wide, VM((TOKS, W), F32),
            VM((4, W, H), F32), VM((4, W, H), F32), VM((4, W, H), F32),
            VM((4, H, W), F32), VM((4, H, W), F32), VM((4, H, W), F32),
            VM((4, H, SEQ), F32), VM((4, H, SEQ), F32), VM((4, H, SEQ), F32),
            VM((CORE, D), BF), VM((CORE, D), BF), VM((2, W, W), F32),
            VM((W, H), BF), VM((H, W), BF), VM((H, SEQ), BF),
            DMA((48,)), DMA((112,)), DMA((112,)), DMA((3, 8)), DMA((3, 8)), DMA((3,)), DMA((3,)),
        ]
        res = pl.pallas_call(
            layer_kernel,
            name="layer",
            in_specs=[ANY, IN_VM, ANY, ANY, ANY, ANY, IN_VM],
            out_specs=[ANY] * len(outs),
            out_shape=outs,
            scratch_shapes=scratch,
            cost_estimate=pl.CostEstimate(flops=80_000_000_000, bytes_accessed=100_000_000, transcendentals=0),
            compiler_params=pltpu.CompilerParams(collective_id=0, has_side_effects=True, vmem_limit_bytes=67043328),
        )(x, gain.reshape(1, -1), wq, wkv, wo, dy, positions.reshape(1, -1))
        return pl.pallas_call(
            copy_kernel,
            name="emit",
            in_specs=[ANY] * 5,
            out_specs=[ANY] * 5,
            out_shape=results,
            scratch_shapes=[VM(r.shape, r.dtype) for r in results] + [DMA((19,)), DMA((19,))],
            cost_estimate=pl.CostEstimate(flops=1_000_000, bytes_accessed=27_000_000, transcendentals=0),
            compiler_params=pltpu.CompilerParams(vmem_limit_bytes=60 * 2**20),
        )(*res[:5])

    return jax.shard_map(
        device_step,
        mesh=mesh,
        in_specs=(P("data", None), P("data", "model"), P("data", None), P("model", "data"), P(), P(), P("data", None)),
        out_specs=(P("data", None), P("data", None), P("data", "model"), P("data", None), P("model", "data")),
        check_vma=False,
    )
```

```python
import functools

import jax
import jax.numpy as jnp
from jax import lax
from jax.experimental import pallas as pl
from jax.experimental.pallas import tpu as pltpu
from jax.sharding import PartitionSpec as P

NORM_EPS = 1e-6
ROWS = 512
TOKS = 1536
TILES = 3
SEQ = 128
D = 2048
CORE = 768
W = 512
PASS = 384
H = 256
WAYS = (1, -1)
HOPS = (1, 2, 3)
BF = jnp.bfloat16
F32 = jnp.float32


def dot(a, b):
    return jnp.dot(a, b, preferred_element_type=F32)


def dot_t(a, b):
    return lax.dot_general(a, b, (((1,), (1,)), ((), ())), preferred_element_type=F32)


def t_dot(a, b):
    return lax.dot_general(a, b, (((0,), (0,)), ((), ())), preferred_element_type=F32)


MESH = pl.DeviceIdType.MESH


def cols(i, width=H):
    return pl.ds(pl.multiple_of(i * width, width), width)


def norm(x):
    c = x - jnp.mean(x, axis=-1, keepdims=True)
    inv = lax.rsqrt(jnp.mean(c * c, axis=-1, keepdims=True) + NORM_EPS)
    return c * inv, inv


def stack_heads(a):
    return jnp.concatenate([a[:, :H], a[:, H:]], axis=0)


def spread_heads(a):
    return jnp.concatenate([a[:SEQ], a[SEQ:]], axis=1)


def softmax(s, mask2):
    s = jnp.where(mask2 > 0, s * (H ** -0.5), -1e30)
    e = jnp.exp(s - jnp.max(s, axis=-1, keepdims=True))
    return e / jnp.sum(e, axis=-1, keepdims=True)


def attend(qs, ks, vs, mask2):
    scores = [dot_t(q, k) for q, k in zip(qs, ks)]
    probs = [softmax(s, mask2) for s in scores]
    return probs, [dot(p.astype(BF), v).astype(BF) for p, v in zip(probs, vs)]


def attend_back(qs, ks, vs, probs, dos):
    dps = [dot_t(do, v) for do, v in zip(dos, vs)]
    dvs = [t_dot(p.astype(BF), do) for p, do in zip(probs, dos)]
    dss = [p * (dp - jnp.sum(p * dp, axis=-1, keepdims=True)) for p, dp in zip(probs, dps)]
    dss = [(ds * (H ** -0.5)).astype(BF) for ds in dss]
    dqs = [dot(ds, k).astype(BF) for ds, k in zip(dss, ks)]
    dks = [t_dot(ds, q) for ds, q in zip(dss, qs)]
    return dqs, dks, dvs


def drop(items, item):
    items[:] = [i for i in items if i is not item]


def layer_kernel(
    x_hbm, gain, wq_hbm, wkv_hbm, wo_hbm, dy_hbm, pos,
    y_out, dx_out, gq_out, gkv_out, go_out, wq_all, wo_all, o_all, dq_all, dkv_mate,
    xh, big, wq, wkv, wo, wqx, wox, q, k, v, probs, o, ox, dq, dqx, dkv,
    ofar, ory, orz, qfar, qry, qrz, kfar, kry, krz, tin, stage, dkvt, go_st, gq_st, gk_st,
    lsem, ssem, rsem, gss, gsr, dks, dkr,
):
    d, m = lax.axis_index("data"), lax.axis_index("model")
    z, y = d // 2, d % 2
    core = m % 2
    zpeer = [((z + s) % 4) * 2 + y for s in range(4)]
    ypeer = z * 2 + 1 - y
    mate = m + 1 - 2 * core
    across = (m + 2) % 4
    diag = (mate + 2) % 4
    mine = pl.ds(pl.multiple_of(core * CORE, CORE), CORE)
    theirs = pl.ds(pl.multiple_of((1 - core) * CORE, CORE), CORE)
    used = {"l": 0, "r": 0}
    sends = []

    def local(src, dst):
        i = used["l"]
        used["l"] += 1
        return pltpu.make_async_copy(src, dst, lsem.at[i])

    def remote(src, dst, land, axis, peer, when=None):
        i = used["r"]
        used["r"] += 1
        args = dict(send_sem=ssem.at[i], recv_sem=rsem.at[i], device_id={axis: peer}, device_id_type=MESH)
        out = pltpu.make_async_remote_copy(src_ref=src, dst_ref=dst, **args)
        back = pltpu.make_async_remote_copy(src_ref=land, dst_ref=land, **args)
        sends.append((when, out))
        return out, back

    loads = [local(x_hbm.at[cols(t, ROWS)], xh.at[cols(t, ROWS)]) for t in range(3)]
    half = cols(core)
    own = [local(wq_hbm, wq.at[cols(d)]), local(wkv_hbm.at[:, half], wkv.at[core, cols(d)]), local(wo_hbm, wo.at[:, cols(d)])]
    dy_load = local(dy_hbm, big.at[pl.ds(0, TOKS)])
    for c in loads + own + [dy_load]:
        c.start()

    barrier = pltpu.get_barrier_semaphore()
    for peer in zpeer[1:] + [ypeer]:
        pl.semaphore_signal(barrier, inc=1, device_id={"data": peer}, device_id_type=MESH)
    for peer in (mate, across, diag):
        pl.semaphore_signal(barrier, inc=1, device_id={"model": peer}, device_id_type=MESH)
    pl.semaphore_wait(barrier, 7)

    shard = {0: wq_hbm, 1: wkv_hbm.at[:, half], 3: wo_hbm}

    def slot(a, zz):
        blk = zz * 2 + (1 - y if a in (2, 4) else y)
        return wq.at[cols(blk)] if a == 0 else wkv.at[core, cols(blk)] if a < 3 else wo.at[:, cols(blk)]

    def got(way, r):
        return z >= r if way > 0 else z + r <= 3

    def origin(way, r):
        return (z + 4 - r) % 4 if way > 0 else (z + r) % 4

    def goes(way):
        return z < 3 if way > 0 else z > 0

    def sent(way, r):
        return goes(way) if r == 1 else jnp.logical_and(got(way, r - 1), goes(way))

    hops, ys, xs, cs = {}, {}, {}, {}
    for r in HOPS:
        for way in WAYS:
            for a in (0, 1, 3, 4):
                here = origin(way, r - 1)
                src = shard[a] if r == 1 and a in shard else slot(a, here)
                to = ((z + way + 4) % 4) * 2 + y
                hops[a, way, r] = remote(src, slot(a, here), slot(a, origin(way, r)), "data", to, sent(way, r))
    keys = [None] + [(way, r) for r in HOPS for way in WAYS]
    ys[3, None] = remote(wo_hbm, slot(3, z), slot(4, z), "data", ypeer)
    for key in keys:
        zz = z if key is None else origin(*key)
        cond = None if key is None else got(*key)
        there = wq.at[cols(zz * 2 + 1 - y)]
        src = wq_hbm if key is None else slot(0, zz)
        ys[0, key] = remote(src, slot(0, zz), there, "data", ypeer, cond)
        xs[0, key] = remote(src, wqx.at[cols(zz * 2 + y)], wqx.at[cols(zz * 2 + y)], "model", across, cond)
        xs[5, key] = remote(there, wqx.at[cols(zz * 2 + 1 - y)], wqx.at[cols(zz * 2 + 1 - y)], "model", across, cond)
        for a in (3, 4):
            src = shard[a] if key is None and a == 3 else slot(a, zz)
            to = wox.at[:, cols(zz * 2 + (y if a == 3 else 1 - y))]
            xs[a, key] = remote(src, to, to, "model", across, cond)
        src = shard[1] if key is None else slot(1, zz)
        ys[1, key] = remote(src, slot(1, zz), slot(2, zz), "data", ypeer, cond)
        for a in (1, 2):
            blk = zz * 2 + (y if a == 1 else 1 - y)
            cs[a, key] = remote(src if a == 1 else slot(2, zz), slot(a, zz), wkv.at[1 - core, cols(blk)], "model", mate, cond)

    def on(cond, fn):
        if cond is None:
            fn()
        else:
            pl.when(cond)(fn)

    def start_hop(a, way, r):
        on(sent(way, r), lambda: hops[a, way, r][0].start())

    for way in WAYS:
        start_hop(0, way, 1)
    ys[0, None][0].start()
    ys[1, None][0].start()
    xs[0, None][0].start()
    xs[3, None][0].start()
    cs[1, None][0].start()

    for t in range(3):
        loads[t].wait()

        @pl.loop(t * 4, t * 4 + 4)
        def _(i):
            r = cols(i, SEQ)
            n, _inv = norm(xh[r, :].astype(F32))
            xh[r, :] = (n * gain[...]).astype(BF)

    for c in own:
        c.wait()

    def take(arrays, way, r):
        for a in arrays:
            hops[a, way, r][1].wait_recv()
            if r < 3:
                start_hop(a, way, r + 1)
            if a < 2:
                ys[a, (way, r)][0].start()
            (cs if a == 1 else xs)[a, (way, r)][0].start()

    def relay(arrays, r):
        for way in WAYS:
            on(jnp.logical_and(got(way, r), goes(way)), lambda way=way: take(arrays, way, r))

    def keep(arrays, r):
        for way in WAYS:
            on(jnp.logical_and(got(way, r), jnp.logical_not(goes(way))), lambda way=way: take(arrays, way, r))

    def take_all(arrays, r):
        for way in WAYS:
            on(got(way, r), lambda way=way: take(arrays, way, r))

    def arrive(a, key):
        def go():
            ys[a, key][1].wait_recv()
            (cs[2, key] if a else xs[5, key])[0].start()

        on(None if key is None else got(*key), go)

    take_all((0,), 1)
    take_all((0,), 2)
    for way in WAYS:
        start_hop(1, way, 1)
    take_all((0,), 3)
    take_all((1,), 1)
    for key in keys[:5]:
        arrive(0, key)
    relay((1,), 2)
    for way in WAYS:
        start_hop(3, way, 1)
    for key in keys[5:]:
        arrive(0, key)

    locals_ = []

    def share(src, dst, slot_of):
        c = local(src, dst.at[slot_of(0)])
        out, back = remote(src, dst.at[slot_of(0)], dst.at[slot_of(1)], "model", mate)
        c.start()
        out.start()
        locals_.append(c)
        return c, out, back

    def colslot(base):
        other = base + 1 - 2 * (base % 2)
        return lambda n: (slice(None), cols(base if n == 0 else other, W))

    def rowslot(base):
        other = base + 1 - 2 * (base % 2)
        return lambda n: (cols(base if n == 0 else other, W),)

    def share_rows(src, dst, base):
        other = base + 1 - 2 * (base % 2)
        c = local(src.at[mine], dst.at[:, cols(base, W)])
        out, back = remote(src.at[theirs], dst.at[:, cols(base, W)], dst.at[:, cols(other, W)], "model", mate)
        c.start()
        out.start()
        locals_.append(c)
        return c, out, back

    wq_sh = share(wq, wq_all, colslot(m))

    @pl.loop(0, TILES)
    def _(t):
        r = cols(t, ROWS)
        q[r, :] = dot(xh[r, :], wq[...]).astype(BF)

    relay((3,), 1)
    keep((1,), 2)
    take_all((1,), 3)
    ys[3, None][0].start()
    for key in keys:
        arrive(1, key)
    for key in keys:
        on(None if key is None else got(*key), lambda key=key: [cs[a, key][1].wait_recv() for a in (1, 2)] and None)

    @pl.loop(0, TILES)
    def _(t):
        r = cols(t, ROWS)
        k[r, :] = dot(xh[r, :], wkv[0]).astype(BF)
        v[r, :] = dot(xh[r, :], wkv[1]).astype(BF)

    ys[3, None][1].wait_recv()
    xs[4, None][0].start()
    for way in WAYS:
        start_hop(4, way, 1)
    posm = jnp.broadcast_to(pos[...].astype(F32), (SEQ, SEQ))
    mask = (posm <= posm.T).astype(F32)
    mask2 = jnp.concatenate([mask, mask], axis=0)

    @pl.loop(0, TILES)
    def _(t):
        rows = [cols(t * 4 + b, SEQ) for b in range(4)]
        qs = [stack_heads(q[r, :]) for r in rows]
        ps, os = attend(qs, [k[r, :] for r in rows], [v[r, :] for r in rows], mask2)
        for b in range(4):
            probs[t * 4 + b] = ps[b]
            wide = spread_heads(os[b])
            o[rows[b], :] = wide
            big[pl.ds(TOKS, W), rows[b]] = wide.T

    dy_load.wait()
    o_sh = share_rows(o, o_all, m)

    far = [qfar, kfar, ofar]
    ry = [qry, kry, ory]
    rz = [qrz, krz, orz]

    def piece(g, blk):
        if g == 2:
            return dot(big[pl.ds(TOKS, W), pl.ds(0, TOKS)], big[pl.ds(0, TOKS), cols(blk)])
        return t_dot(xh[:, cols(blk)], dq[...] if g == 0 else q[:, cols(m, SEQ)])

    def ysend(g, kk):
        return pltpu.make_async_remote_copy(
            src_ref=far[g].at[kk], dst_ref=ry[g].at[kk], send_sem=gss.at[g, kk], recv_sem=gsr.at[g, kk],
            device_id={"data": ypeer}, device_id_type=MESH,
        )

    upper = z // 2
    inner = jnp.logical_and(z > 0, z < 3)

    def zcopy(g, kk, place, peer):
        return pltpu.make_async_remote_copy(
            src_ref=ry[g].at[kk], dst_ref=rz[g].at[place], send_sem=gss.at[g, 4 + kk], recv_sem=gsr.at[g, 4 + place],
            device_id={"data": peer}, device_id_type=MESH,
        )

    def zsend(g, kk):
        if kk == 2 and g != 1:
            return zcopy(g, kk, 2 + upper, (z + 1 - 2 * upper) * 2 + y)
        if kk == 2:
            return zcopy(g, kk, 2, zpeer[2])
        return zcopy(g, kk, kk // 2, zpeer[kk])

    def merge(g):
        @pl.when(inner)
        def _():
            for kk in (3, 1):
                zcopy(g, 2, 2 + kk // 2, ypeer).wait_recv()
                ry[g][kk] = ry[g][kk] + rz[g][2 + kk // 2]
                zsend(g, kk).start()

    def send_far(g, lo, hi):
        @pl.loop(lo, hi)
        def _(i):
            kk = 2 + i + (i // 2) * (1 - 2 * i)
            far[g][kk] = piece(g, ((z + kk) % 4) * 2 + 1 - y)
            pl.when(jnp.logical_or(kk > 0, g == 1))(lambda: ysend(g, kk).start())

    def near(g, kk, part=None):
        ysend(g, kk).wait_recv()
        ry[g][kk] = ry[g][kk] + (piece(g, zpeer[kk]) if part is None else part[...])
        if kk == 2 or kk and g == 1:
            zsend(g, kk).start()
        elif kk:
            pl.when(jnp.logical_not(inner))(lambda: zsend(g, kk).start())

    def finish(g, st):
        for kk in (1, 3):
            zsend(g, kk).wait_recv()
        total = ry[g][0] + rz[g][0] + rz[g][1]
        if g == 1:
            zsend(g, 2).wait_recv()
            total = total + rz[g][2]
        st[...] = total.astype(BF)

    relay((3,), 2)
    send_far(2, 0, 4)
    relay((4,), 1)
    relay((4,), 2)
    near(2, 2)
    keep((3, 4), 1)
    keep((3, 4), 2)
    take_all((3, 4), 3)
    wo_sh = share(wo, wo_all, rowslot(m))

    def back_tile(t, q_of, ps, do, add):
        rows = [cols(t * 4 + b, SEQ) for b in range(4)]
        qs, ks, vs = q_of, [k[r, :] for r in rows], [v[r, :] for r in rows]
        dqs, dks, dvs = attend_back(qs, ks, vs, ps, [stack_heads(do[b * SEQ : (b + 1) * SEQ]) for b in range(4)])
        to = dqx if add else dq
        for b, r in enumerate(rows):
            to[r, :] = spread_heads(dqs[b])
            dkv[r, :H] = dkv[r, :H] + dks[b] if add else dks[b]
            dkv[r, H:] = dkv[r, H:] + dvs[b] if add else dvs[b]

    @pl.loop(0, TILES)
    def _(t):
        do = dot_t(big[cols(t, ROWS), :], wo[...]).astype(BF)
        qs = [stack_heads(q[cols(t * 4 + b, SEQ), :]) for b in range(4)]
        back_tile(t, qs, [probs[t * 4 + b] for b in range(4)], do, False)

    dq_sh = share_rows(dq, dq_all, m)
    send_far(0, 0, 4)
    near(2, 3)
    near(2, 1)
    merge(2)

    for key in keys:
        on(None if key is None else got(*key), lambda key=key: [xs[a, key][1].wait_recv() for a in (0, 5)] and None)
    wqx_sh = share(wqx, wq_all, colslot(across))

    @pl.loop(0, TILES)
    def _(t):
        rows = [cols(t * 4 + b, SEQ) for b in range(4)]
        qm = dot(xh[cols(t, ROWS), :], wqx[...]).astype(BF)
        qs = [stack_heads(qm[b * SEQ : (b + 1) * SEQ]) for b in range(4)]
        ps, os = attend(qs, [k[r, :] for r in rows], [v[r, :] for r in rows], mask2)
        dqx[cols(t, ROWS), :] = qm
        for b in range(4):
            probs[t * 4 + b] = ps[b]
            ox[rows[b], :] = spread_heads(os[b])

    ox_sh = share_rows(ox, o_all, across)
    for key in keys:
        on(None if key is None else got(*key), lambda key=key: [xs[a, key][1].wait_recv() for a in (3, 4)] and None)
    wox_sh = share(wox, wo_all, rowslot(across))

    def dkv_send(t):
        r = cols(t, ROWS)
        return pltpu.make_async_remote_copy(
            src_ref=dkv.at[r], dst_ref=dkv_mate.at[r], send_sem=dks.at[t], recv_sem=dkr.at[t],
            device_id={"model": mate}, device_id_type=MESH,
        )

    @pl.loop(0, TILES)
    def _(t):
        do = dot_t(big[cols(t, ROWS), :], wox[...]).astype(BF)
        qs = [stack_heads(dqx[cols(t * 4 + b, SEQ), :]) for b in range(4)]
        back_tile(t, qs, [probs[t * 4 + b] for b in range(4)], do, True)
        dkv_send(t).start()

    dqx_sh = share_rows(dqx, dq_all, across)

    tiles = []
    for t in range(3):
        dkv_send(t).wait_recv()
        tiles.append(local(dkv_mate.at[cols(t, ROWS)], dkvt.at[t % 2]))
        if t < 2:
            tiles[t].start()
    for t in range(3):
        tiles[t].wait()
        q[cols(t, ROWS), :] = (dkv[cols(t, ROWS), :] + dkvt[t % 2]).astype(BF)
        if t == 0:
            tiles[2].start()
    send_far(1, 0, 4)
    ysend(2, 0).start()
    ysend(0, 0).start()
    last = dkvt.at[0, :, pl.ds(0, H)]
    last[...] = piece(2, zpeer[0])
    near(0, 2)

    for sh in (wo_sh, wox_sh, o_sh, ox_sh):
        sh[0].wait()
        sh[2].wait_recv()
        drop(locals_, sh[0])
    fetch = local(o_all, tin)
    fetch.start()
    fill = [local(wo_all.at[:, cols(i, W)], big.at[:, cols(i, W)]) for i in range(4)]
    for c in fill:
        c.start()
    fetch.wait()

    def y_cols(lo, hi):
        @pl.loop(lo, hi)
        def _(i):
            stage[:, cols(i)] = dot(tin[...], big[:, cols(i)]).astype(BF)

    done = []

    def emit(dst):
        c = local(stage, dst.at[mine])
        out, back = remote(stage, dst.at[mine], dst.at[theirs], "model", mate)
        c.start()
        out.start()
        done.append((c, out, back))

    for i in range(4):
        fill[i].wait()
        y_cols(2 * i, 2 * i + 2)
        if i == 1:
            near(0, 3)
    emit(y_out)

    for sh in (wq_sh, wqx_sh, dq_sh, dqx_sh):
        sh[0].wait()
        sh[2].wait_recv()
        drop(locals_, sh[0])
    fetch = local(dq_all, tin)
    fetch.start()
    fill = [local(wq_all.at[cols(i, W)], big.at[cols(i, W)]) for i in range(4)]
    for c in fill:
        c.start()
    wox_sh[1].wait_send()
    sends[:] = [s for s in sends if s[1] is not wox_sh[1]]
    xin = [local(x_hbm.at[pl.ds(pl.multiple_of(core * CORE + p * PASS, PASS), PASS)], wox.at[pl.ds(0, PASS)]) for p in range(2)]
    xin[0].start()
    for t in range(3):
        dkv_send(t).wait_send()
    near(0, 1)
    merge(0)
    fetch.wait()
    for p in range(2):
        rows = pl.ds(pl.multiple_of(core * CORE + p * PASS, PASS), PASS)

        def dh_cols(i):
            c = cols(i, W)
            g = dot_t(tin[pl.ds(p * PASS, PASS), :], big[c, :])
            g = g + dot_t(q[rows, :H], wkv[0, c, :])
            dkv[cols(i, PASS), :] = g + dot_t(q[rows, H:], wkv[1, c, :])

        if p == 0:
            for n in range(4):
                fill[n].wait()
                pl.loop(n, n + 1)(dh_cols)
        else:
            pl.loop(0, 4)(dh_cols)

        xin[p].wait()
        if p == 0:
            done[0][0].wait()
            done[0][1].wait_send()
            sends[:] = [s for s in sends if s[1] is not done[0][1]]

        @pl.loop(0, TILES)
        def _(i):
            n, inv = norm(wox[cols(i, SEQ), :].astype(F32))
            gn = jnp.concatenate([dkv[pl.ds(pl.multiple_of(c * PASS + i * SEQ, SEQ), SEQ), :] for c in range(4)], axis=1) * gain[...]
            g = inv * (gn - jnp.mean(gn, axis=-1, keepdims=True) - n * jnp.mean(gn * n, axis=-1, keepdims=True))
            stage[pl.ds(pl.multiple_of(p * PASS + i * SEQ, SEQ), SEQ), :] = g.astype(BF)

        if p == 0:
            xin[1].start()
            for kk in (2, 3, 1, 0):
                near(1, kk)
    emit(dx_out)

    finish(1, gk_st)
    fin = [local(gk_st, gkv_out.at[:, cols(m, SEQ)])]
    fin[0].start()
    backs = []
    for peer in (mate, across, diag):
        out, back = remote(gk_st, gkv_out.at[:, cols(m, SEQ)], gkv_out.at[:, cols(peer, SEQ)], "model", peer)
        out.start()
        backs.append(back)

    near(2, 0, last)
    finish(2, go_st)
    fin.append(local(go_st, go_out))
    fin[1].start()
    near(0, 0)
    finish(0, gq_st)
    fin.append(local(gq_st, gq_out))
    fin[2].start()
    for b in backs:
        b.wait_recv()
    done[1][0].wait()
    for c, out, back in done:
        back.wait_recv()
    for cond, c in sends:
        on(cond, c.wait_send)
    for c in locals_ + fin:
        c.wait()
    for g in range(3):
        for kk in range(4):
            ysend(g, kk).wait_send()
            if kk:
                zsend(g, kk).wait_send()


def copy_kernel(*refs):
    srcs, dsts, bufs, rsem, wsem = refs[:5], refs[5:10], refs[10:15], refs[15], refs[16]
    ins, outs = [], []
    for a in range(5):
        rows = srcs[a].shape[0]
        parts = 8 if a < 2 else 1
        for c in range(parts):
            r = pl.ds(c * (rows // parts), rows // parts)
            i = len(ins)
            ins.append(pltpu.make_async_copy(srcs[a].at[r], bufs[a].at[r], rsem.at[i]))
            outs.append(pltpu.make_async_copy(bufs[a].at[r], dsts[a].at[r], wsem.at[i]))
    for c in ins:
        c.start()
    for i, o in zip(ins, outs):
        i.wait()
        o.start()
    for o in outs:
        o.wait()


def solution(mesh):
    sd = jax.ShapeDtypeStruct
    DMA = pltpu.SemaphoreType.DMA
    VM = pltpu.VMEM
    ANY = pl.BlockSpec(memory_space=pl.ANY)
    IN_VM = pl.BlockSpec(memory_space=pltpu.VMEM)

    def device_step(x, wq, wkv, wo, gain, positions, dy):
        results = [
            sd((TOKS, D), BF), sd((TOKS, D), BF), sd((H, W), BF), sd((H, W), BF), sd((W, H), BF),
        ]
        outs = results + [
            sd((D, D), BF), sd((D, D), BF), sd((CORE, D), BF), sd((CORE, D), BF), sd((TOKS, W), F32),
        ]
        wide, narrow = VM((TOKS, W), BF), VM((TOKS, H), BF)
        scratch = [
            VM((TOKS, D), BF), VM((D, D), BF), VM((D, W), BF), VM((2, D, H), BF), VM((W, D), BF),
            VM((D, W), BF), VM((W, D), BF), wide, narrow, narrow, VM((12, H, SEQ), F32),
            wide, wide, wide, wide, VM((TOKS, W), F32),
            VM((4, W, H), F32), VM((4, W, H), F32), VM((4, W, H), F32),
            VM((4, H, W), F32), VM((4, H, W), F32), VM((4, H, W), F32),
            VM((4, H, SEQ), F32), VM((4, H, SEQ), F32), VM((4, H, SEQ), F32),
            VM((CORE, D), BF), VM((CORE, D), BF), VM((2, W, W), F32),
            VM((W, H), BF), VM((H, W), BF), VM((H, SEQ), BF),
            DMA((48,)), DMA((112,)), DMA((112,)), DMA((3, 8)), DMA((3, 8)), DMA((3,)), DMA((3,)),
        ]
        res = pl.pallas_call(
            layer_kernel,
            name="layer",
            in_specs=[ANY, IN_VM, ANY, ANY, ANY, ANY, IN_VM],
            out_specs=[ANY] * len(outs),
            out_shape=outs,
            scratch_shapes=scratch,
            cost_estimate=pl.CostEstimate(flops=80_000_000_000, bytes_accessed=100_000_000, transcendentals=0),
            compiler_params=pltpu.CompilerParams(collective_id=0, has_side_effects=True, vmem_limit_bytes=67043328),
        )(x, gain.reshape(1, -1), wq, wkv, wo, dy, positions.reshape(1, -1))
        return pl.pallas_call(
            copy_kernel,
            name="emit",
            in_specs=[ANY] * 5,
            out_specs=[ANY] * 5,
            out_shape=results,
            scratch_shapes=[VM(r.shape, r.dtype) for r in results] + [DMA((19,)), DMA((19,))],
            cost_estimate=pl.CostEstimate(flops=1_000_000, bytes_accessed=27_000_000, transcendentals=0),
            compiler_params=pltpu.CompilerParams(vmem_limit_bytes=60 * 2**20),
        )(*res[:5])

    return jax.shard_map(
        device_step,
        mesh=mesh,
        in_specs=(P("data", None), P("data", "model"), P("data", None), P("model", "data"), P(), P(), P("data", None)),
        out_specs=(P("data", None), P("data", None), P("data", "model"), P("data", None), P("model", "data")),
        check_vma=False,
    )
```

```python
import functools

import jax
import jax.numpy as jnp
from jax import lax
from jax.experimental import pallas as pl
from jax.experimental.pallas import tpu as pltpu
from jax.sharding import PartitionSpec as P

NORM_EPS = 1e-6
ROWS = 512
TOKS = 1536
TILES = 3
SEQ = 128
D = 2048
CORE = 768
W = 512
PASS = 384
H = 256
WAYS = (1, -1)
HOPS = (1, 2, 3)
BF = jnp.bfloat16
F32 = jnp.float32


def dot(a, b):
    return jnp.dot(a, b, preferred_element_type=F32)


def dot_t(a, b):
    return lax.dot_general(a, b, (((1,), (1,)), ((), ())), preferred_element_type=F32)


def t_dot(a, b):
    return lax.dot_general(a, b, (((0,), (0,)), ((), ())), preferred_element_type=F32)


MESH = pl.DeviceIdType.MESH


def cols(i, width=H):
    return pl.ds(pl.multiple_of(i * width, width), width)


def norm(x):
    c = x - jnp.mean(x, axis=-1, keepdims=True)
    inv = lax.rsqrt(jnp.mean(c * c, axis=-1, keepdims=True) + NORM_EPS)
    return c * inv, inv


def stack_heads(a):
    return jnp.concatenate([a[:, :H], a[:, H:]], axis=0)


def spread_heads(a):
    return jnp.concatenate([a[:SEQ], a[SEQ:]], axis=1)


def softmax(s, mask2):
    s = jnp.where(mask2 > 0, s * (H ** -0.5), -1e30)
    e = jnp.exp(s - jnp.max(s, axis=-1, keepdims=True))
    return e / jnp.sum(e, axis=-1, keepdims=True)


def attend(qs, ks, vs, mask2):
    scores = [dot_t(q, k) for q, k in zip(qs, ks)]
    probs = [softmax(s, mask2) for s in scores]
    return probs, [dot(p.astype(BF), v).astype(BF) for p, v in zip(probs, vs)]


def attend_back(qs, ks, vs, probs, dos):
    dps = [dot_t(do, v) for do, v in zip(dos, vs)]
    dvs = [t_dot(p.astype(BF), do) for p, do in zip(probs, dos)]
    dss = [p * (dp - jnp.sum(p * dp, axis=-1, keepdims=True)) for p, dp in zip(probs, dps)]
    dss = [(ds * (H ** -0.5)).astype(BF) for ds in dss]
    dqs = [dot(ds, k).astype(BF) for ds, k in zip(dss, ks)]
    dks = [t_dot(ds, q) for ds, q in zip(dss, qs)]
    return dqs, dks, dvs


def drop(items, item):
    items[:] = [i for i in items if i is not item]


def layer_kernel(
    x_hbm, gain, wq_hbm, wkv_hbm, wo_hbm, dy_hbm, pos,
    y_out, dx_out, gq_out, gkv_out, go_out, wq_all, wo_all, o_all, dq_all, dkv_mate,
    xh, big, wq, wkv, wo, wqx, wox, q, k, v, probs, o, ox, dq, dqx, dkv,
    ofar, ory, orz, qfar, qry, qrz, kfar, kry, krz, tin, stage, dkvt, go_st, gq_st, gk_st,
    lsem, ssem, rsem, gss, gsr, dks, dkr,
):
    d, m = lax.axis_index("data"), lax.axis_index("model")
    z, y = d // 2, d % 2
    core = m % 2
    zpeer = [((z + s) % 4) * 2 + y for s in range(4)]
    ypeer = z * 2 + 1 - y
    mate = m + 1 - 2 * core
    across = (m + 2) % 4
    diag = (mate + 2) % 4
    mine = pl.ds(pl.multiple_of(core * CORE, CORE), CORE)
    theirs = pl.ds(pl.multiple_of((1 - core) * CORE, CORE), CORE)
    used = {"l": 0, "r": 0}
    sends = []

    def local(src, dst):
        i = used["l"]
        used["l"] += 1
        return pltpu.make_async_copy(src, dst, lsem.at[i])

    def remote(src, dst, land, axis, peer, when=None):
        i = used["r"]
        used["r"] += 1
        args = dict(send_sem=ssem.at[i], recv_sem=rsem.at[i], device_id={axis: peer}, device_id_type=MESH)
        out = pltpu.make_async_remote_copy(src_ref=src, dst_ref=dst, **args)
        back = pltpu.make_async_remote_copy(src_ref=land, dst_ref=land, **args)
        sends.append((when, out))
        return out, back

    loads = [local(x_hbm.at[cols(t, ROWS)], xh.at[cols(t, ROWS)]) for t in range(3)]
    half = cols(core)
    own = [local(wq_hbm, wq.at[cols(d)]), local(wkv_hbm.at[:, half], wkv.at[core, cols(d)]), local(wo_hbm, wo.at[:, cols(d)])]
    dy_load = local(dy_hbm, big.at[pl.ds(0, TOKS)])
    for c in loads + own + [dy_load]:
        c.start()

    barrier = pltpu.get_barrier_semaphore()
    for peer in zpeer[1:] + [ypeer]:
        pl.semaphore_signal(barrier, inc=1, device_id={"data": peer}, device_id_type=MESH)
    for peer in (mate, across, diag):
        pl.semaphore_signal(barrier, inc=1, device_id={"model": peer}, device_id_type=MESH)
    pl.semaphore_wait(barrier, 7)

    shard = {0: wq_hbm, 1: wkv_hbm.at[:, half], 3: wo_hbm}

    def slot(a, zz):
        blk = zz * 2 + (1 - y if a in (2, 4) else y)
        return wq.at[cols(blk)] if a == 0 else wkv.at[core, cols(blk)] if a < 3 else wo.at[:, cols(blk)]

    def got(way, r):
        return z >= r if way > 0 else z + r <= 3

    def origin(way, r):
        return (z + 4 - r) % 4 if way > 0 else (z + r) % 4

    def goes(way):
        return z < 3 if way > 0 else z > 0

    def sent(way, r):
        return goes(way) if r == 1 else jnp.logical_and(got(way, r - 1), goes(way))

    hops, ys, xs, cs = {}, {}, {}, {}
    for r in HOPS:
        for way in WAYS:
            for a in (0, 1, 3, 4):
                here = origin(way, r - 1)
                src = shard[a] if r == 1 and a in shard else slot(a, here)
                to = ((z + way + 4) % 4) * 2 + y
                hops[a, way, r] = remote(src, slot(a, here), slot(a, origin(way, r)), "data", to, sent(way, r))
    keys = [None] + [(way, r) for r in HOPS for way in WAYS]
    ys[3, None] = remote(wo_hbm, slot(3, z), slot(4, z), "data", ypeer)
    for key in keys:
        zz = z if key is None else origin(*key)
        cond = None if key is None else got(*key)
        there = wq.at[cols(zz * 2 + 1 - y)]
        src = wq_hbm if key is None else slot(0, zz)
        ys[0, key] = remote(src, slot(0, zz), there, "data", ypeer, cond)
        xs[0, key] = remote(src, wqx.at[cols(zz * 2 + y)], wqx.at[cols(zz * 2 + y)], "model", across, cond)
        xs[5, key] = remote(there, wqx.at[cols(zz * 2 + 1 - y)], wqx.at[cols(zz * 2 + 1 - y)], "model", across, cond)
        for a in (3, 4):
            src = shard[a] if key is None and a == 3 else slot(a, zz)
            to = wox.at[:, cols(zz * 2 + (y if a == 3 else 1 - y))]
            xs[a, key] = remote(src, to, to, "model", across, cond)
        src = shard[1] if key is None else slot(1, zz)
        ys[1, key] = remote(src, slot(1, zz), slot(2, zz), "data", ypeer, cond)
        for a in (1, 2):
            blk = zz * 2 + (y if a == 1 else 1 - y)
            cs[a, key] = remote(src if a == 1 else slot(2, zz), slot(a, zz), wkv.at[1 - core, cols(blk)], "model", mate, cond)

    def on(cond, fn):
        if cond is None:
            fn()
        else:
            pl.when(cond)(fn)

    def start_hop(a, way, r):
        on(sent(way, r), lambda: hops[a, way, r][0].start())

    for way in WAYS:
        start_hop(0, way, 1)
    ys[0, None][0].start()
    ys[1, None][0].start()
    xs[0, None][0].start()
    xs[3, None][0].start()
    cs[1, None][0].start()

    for t in range(3):
        loads[t].wait()

        @pl.loop(t * 4, t * 4 + 4)
        def _(i):
            r = cols(i, SEQ)
            n, _inv = norm(xh[r, :].astype(F32))
            xh[r, :] = (n * gain[...]).astype(BF)

    for c in own:
        c.wait()

    def take(arrays, way, r):
        for a in arrays:
            hops[a, way, r][1].wait_recv()
            if r < 3:
                start_hop(a, way, r + 1)
            if a < 2:
                ys[a, (way, r)][0].start()
            (cs if a == 1 else xs)[a, (way, r)][0].start()

    def relay(arrays, r):
        for way in WAYS:
            on(jnp.logical_and(got(way, r), goes(way)), lambda way=way: take(arrays, way, r))

    def keep(arrays, r):
        for way in WAYS:
            on(jnp.logical_and(got(way, r), jnp.logical_not(goes(way))), lambda way=way: take(arrays, way, r))

    def take_all(arrays, r):
        for way in WAYS:
            on(got(way, r), lambda way=way: take(arrays, way, r))

    def arrive(a, key):
        def go():
            ys[a, key][1].wait_recv()
            (cs[2, key] if a else xs[5, key])[0].start()

        on(None if key is None else got(*key), go)

    take_all((0,), 1)
    take_all((0,), 2)
    for way in WAYS:
        start_hop(1, way, 1)
    take_all((0,), 3)
    take_all((1,), 1)
    for key in keys[:5]:
        arrive(0, key)
    relay((1,), 2)
    for way in WAYS:
        start_hop(3, way, 1)
    for key in keys[5:]:
        arrive(0, key)

    locals_ = []

    def share(src, dst, slot_of):
        c = local(src, dst.at[slot_of(0)])
        out, back = remote(src, dst.at[slot_of(0)], dst.at[slot_of(1)], "model", mate)
        c.start()
        out.start()
        locals_.append(c)
        return c, out, back

    def colslot(base):
        other = base + 1 - 2 * (base % 2)
        return lambda n: (slice(None), cols(base if n == 0 else other, W))

    def rowslot(base):
        other = base + 1 - 2 * (base % 2)
        return lambda n: (cols(base if n == 0 else other, W),)

    def share_rows(src, dst, base):
        other = base + 1 - 2 * (base % 2)
        c = local(src.at[mine], dst.at[:, cols(base, W)])
        out, back = remote(src.at[theirs], dst.at[:, cols(base, W)], dst.at[:, cols(other, W)], "model", mate)
        c.start()
        out.start()
        locals_.append(c)
        return c, out, back

    wq_sh = share(wq, wq_all, colslot(m))

    @pl.loop(0, TILES)
    def _(t):
        r = cols(t, ROWS)
        q[r, :] = dot(xh[r, :], wq[...]).astype(BF)

    relay((3,), 1)
    keep((1,), 2)
    take_all((1,), 3)
    ys[3, None][0].start()
    for key in keys:
        arrive(1, key)
    for key in keys:
        on(None if key is None else got(*key), lambda key=key: [cs[a, key][1].wait_recv() for a in (1, 2)] and None)

    @pl.loop(0, TILES)
    def _(t):
        r = cols(t, ROWS)
        k[r, :] = dot(xh[r, :], wkv[0]).astype(BF)
        v[r, :] = dot(xh[r, :], wkv[1]).astype(BF)

    ys[3, None][1].wait_recv()
    xs[4, None][0].start()
    for way in WAYS:
        start_hop(4, way, 1)
    posm = jnp.broadcast_to(pos[...].astype(F32), (SEQ, SEQ))
    mask = (posm <= posm.T).astype(F32)
    mask2 = jnp.concatenate([mask, mask], axis=0)

    @pl.loop(0, TILES)
    def _(t):
        rows = [cols(t * 4 + b, SEQ) for b in range(4)]
        qs = [stack_heads(q[r, :]) for r in rows]
        ps, os = attend(qs, [k[r, :] for r in rows], [v[r, :] for r in rows], mask2)
        for b in range(4):
            probs[t * 4 + b] = ps[b]
            wide = spread_heads(os[b])
            o[rows[b], :] = wide
            big[pl.ds(TOKS, W), rows[b]] = wide.T

    dy_load.wait()
    o_sh = share_rows(o, o_all, m)

    far = [qfar, kfar, ofar]
    ry = [qry, kry, ory]
    rz = [qrz, krz, orz]

    def piece(g, blk):
        if g == 2:
            return dot(big[pl.ds(TOKS, W), pl.ds(0, TOKS)], big[pl.ds(0, TOKS), cols(blk)])
        return t_dot(xh[:, cols(blk)], dq[...] if g == 0 else q[:, cols(m, SEQ)])

    def ysend(g, kk):
        return pltpu.make_async_remote_copy(
            src_ref=far[g].at[kk], dst_ref=ry[g].at[kk], send_sem=gss.at[g, kk], recv_sem=gsr.at[g, kk],
            device_id={"data": ypeer}, device_id_type=MESH,
        )

    upper = z // 2
    inner = jnp.logical_and(z > 0, z < 3)

    def zcopy(g, kk, place, peer):
        return pltpu.make_async_remote_copy(
            src_ref=ry[g].at[kk], dst_ref=rz[g].at[place], send_sem=gss.at[g, 4 + kk], recv_sem=gsr.at[g, 4 + place],
            device_id={"data": peer}, device_id_type=MESH,
        )

    def zsend(g, kk):
        if kk == 2 and g != 1:
            return zcopy(g, kk, 2 + upper, (z + 1 - 2 * upper) * 2 + y)
        if kk == 2:
            return zcopy(g, kk, 2, zpeer[2])
        return zcopy(g, kk, kk // 2, zpeer[kk])

    def merge(g):
        @pl.when(inner)
        def _():
            for kk in (3, 1):
                zcopy(g, 2, 2 + kk // 2, ypeer).wait_recv()
                ry[g][kk] = ry[g][kk] + rz[g][2 + kk // 2]
                zsend(g, kk).start()

    def send_far(g, lo, hi):
        @pl.loop(lo, hi)
        def _(i):
            kk = 2 + i + (i // 2) * (1 - 2 * i)
            far[g][kk] = piece(g, ((z + kk) % 4) * 2 + 1 - y)
            pl.when(jnp.logical_or(kk > 0, g == 1))(lambda: ysend(g, kk).start())

    def near(g, kk, part=None):
        ysend(g, kk).wait_recv()
        ry[g][kk] = ry[g][kk] + (piece(g, zpeer[kk]) if part is None else part[...])
        if kk == 2 or kk and g == 1:
            zsend(g, kk).start()
        elif kk:
            pl.when(jnp.logical_not(inner))(lambda: zsend(g, kk).start())

    def finish(g, st):
        for kk in (1, 3):
            zsend(g, kk).wait_recv()
        total = ry[g][0] + rz[g][0] + rz[g][1]
        if g == 1:
            zsend(g, 2).wait_recv()
            total = total + rz[g][2]
        st[...] = total.astype(BF)

    relay((3,), 2)
    send_far(2, 0, 4)
    relay((4,), 1)
    relay((4,), 2)
    near(2, 2)
    keep((3, 4), 1)
    keep((3, 4), 2)
    take_all((3, 4), 3)
    wo_sh = share(wo, wo_all, rowslot(m))

    def back_tile(t, q_of, ps, do, add):
        rows = [cols(t * 4 + b, SEQ) for b in range(4)]
        qs, ks, vs = q_of, [k[r, :] for r in rows], [v[r, :] for r in rows]
        dqs, dks, dvs = attend_back(qs, ks, vs, ps, [stack_heads(do[b * SEQ : (b + 1) * SEQ]) for b in range(4)])
        to = dqx if add else dq
        for b, r in enumerate(rows):
            to[r, :] = spread_heads(dqs[b])
            dkv[r, :H] = dkv[r, :H] + dks[b] if add else dks[b]
            dkv[r, H:] = dkv[r, H:] + dvs[b] if add else dvs[b]

    @pl.loop(0, TILES)
    def _(t):
        do = dot_t(big[cols(t, ROWS), :], wo[...]).astype(BF)
        qs = [stack_heads(q[cols(t * 4 + b, SEQ), :]) for b in range(4)]
        back_tile(t, qs, [probs[t * 4 + b] for b in range(4)], do, False)

    dq_sh = share_rows(dq, dq_all, m)
    send_far(0, 0, 4)
    near(2, 3)
    near(2, 1)
    merge(2)

    for key in keys:
        on(None if key is None else got(*key), lambda key=key: [xs[a, key][1].wait_recv() for a in (0, 5)] and None)
    wqx_sh = share(wqx, wq_all, colslot(across))

    @pl.loop(0, TILES)
    def _(t):
        rows = [cols(t * 4 + b, SEQ) for b in range(4)]
        qm = dot(xh[cols(t, ROWS), :], wqx[...]).astype(BF)
        qs = [stack_heads(qm[b * SEQ : (b + 1) * SEQ]) for b in range(4)]
        ps, os = attend(qs, [k[r, :] for r in rows], [v[r, :] for r in rows], mask2)
        dqx[cols(t, ROWS), :] = qm
        for b in range(4):
            probs[t * 4 + b] = ps[b]
            ox[rows[b], :] = spread_heads(os[b])

    ox_sh = share_rows(ox, o_all, across)
    near(0, 2)
    for key in keys:
        on(None if key is None else got(*key), lambda key=key: [xs[a, key][1].wait_recv() for a in (3, 4)] and None)
    wox_sh = share(wox, wo_all, rowslot(across))

    def dkv_send(t):
        r = cols(t, ROWS)
        return pltpu.make_async_remote_copy(
            src_ref=dkv.at[r], dst_ref=dkv_mate.at[r], send_sem=dks.at[t], recv_sem=dkr.at[t],
            device_id={"model": mate}, device_id_type=MESH,
        )

    @pl.loop(0, TILES)
    def _(t):
        do = dot_t(big[cols(t, ROWS), :], wox[...]).astype(BF)
        qs = [stack_heads(dqx[cols(t * 4 + b, SEQ), :]) for b in range(4)]
        back_tile(t, qs, [probs[t * 4 + b] for b in range(4)], do, True)
        dkv_send(t).start()

    dqx_sh = share_rows(dqx, dq_all, across)

    tiles = []
    for t in range(3):
        dkv_send(t).wait_recv()
        tiles.append(local(dkv_mate.at[cols(t, ROWS)], dkvt.at[t % 2]))
        if t < 2:
            tiles[t].start()
    for t in range(3):
        tiles[t].wait()
        q[cols(t, ROWS), :] = (dkv[cols(t, ROWS), :] + dkvt[t % 2]).astype(BF)
        if t == 0:
            tiles[2].start()
    send_far(1, 0, 4)
    ysend(2, 0).start()
    ysend(0, 0).start()
    last = dkvt.at[0, :, pl.ds(0, H)]
    last[...] = piece(2, zpeer[0])
    near(0, 3)

    for sh in (wo_sh, wox_sh, o_sh, ox_sh):
        sh[0].wait()
        sh[2].wait_recv()
        drop(locals_, sh[0])
    fetch = local(o_all, tin)
    fetch.start()
    fill = [local(wo_all.at[:, cols(i, W)], big.at[:, cols(i, W)]) for i in range(4)]
    for c in fill:
        c.start()
    fetch.wait()

    def y_cols(lo, hi):
        @pl.loop(lo, hi)
        def _(i):
            stage[:, cols(i)] = dot(tin[...], big[:, cols(i)]).astype(BF)

    done = []

    def emit(dst):
        c = local(stage, dst.at[mine])
        out, back = remote(stage, dst.at[mine], dst.at[theirs], "model", mate)
        c.start()
        out.start()
        done.append((c, out, back))

    for i in range(4):
        fill[i].wait()
        y_cols(2 * i, 2 * i + 2)
        if i == 1:
            near(0, 1)
            merge(0)
    emit(y_out)

    for sh in (wq_sh, wqx_sh, dq_sh, dqx_sh):
        sh[0].wait()
        sh[2].wait_recv()
        drop(locals_, sh[0])
    fetch = local(dq_all, tin)
    fetch.start()
    fill = [local(wq_all.at[cols(i, W)], big.at[cols(i, W)]) for i in range(4)]
    for c in fill:
        c.start()
    wox_sh[1].wait_send()
    sends[:] = [s for s in sends if s[1] is not wox_sh[1]]
    xin = [local(x_hbm.at[pl.ds(pl.multiple_of(core * CORE + p * PASS, PASS), PASS)], wox.at[pl.ds(0, PASS)]) for p in range(2)]
    xin[0].start()
    for t in range(3):
        dkv_send(t).wait_send()
    fetch.wait()
    for p in range(2):
        rows = pl.ds(pl.multiple_of(core * CORE + p * PASS, PASS), PASS)

        def dh_cols(i):
            c = cols(i, W)
            g = dot_t(tin[pl.ds(p * PASS, PASS), :], big[c, :])
            g = g + dot_t(q[rows, :H], wkv[0, c, :])
            dkv[cols(i, PASS), :] = g + dot_t(q[rows, H:], wkv[1, c, :])

        if p == 0:
            for n in range(4):
                fill[n].wait()
                pl.loop(n, n + 1)(dh_cols)
        else:
            pl.loop(0, 4)(dh_cols)

        xin[p].wait()
        if p == 0:
            done[0][0].wait()
            done[0][1].wait_send()
            sends[:] = [s for s in sends if s[1] is not done[0][1]]

        @pl.loop(0, TILES)
        def _(i):
            n, inv = norm(wox[cols(i, SEQ), :].astype(F32))
            gn = jnp.concatenate([dkv[pl.ds(pl.multiple_of(c * PASS + i * SEQ, SEQ), SEQ), :] for c in range(4)], axis=1) * gain[...]
            g = inv * (gn - jnp.mean(gn, axis=-1, keepdims=True) - n * jnp.mean(gn * n, axis=-1, keepdims=True))
            stage[pl.ds(pl.multiple_of(p * PASS + i * SEQ, SEQ), SEQ), :] = g.astype(BF)

        if p == 0:
            xin[1].start()
            for kk in (2, 3, 1, 0):
                near(1, kk)
    emit(dx_out)

    finish(1, gk_st)
    fin = [local(gk_st, gkv_out.at[:, cols(m, SEQ)])]
    fin[0].start()
    backs = []
    for peer in (mate, across, diag):
        out, back = remote(gk_st, gkv_out.at[:, cols(m, SEQ)], gkv_out.at[:, cols(peer, SEQ)], "model", peer)
        out.start()
        backs.append(back)

    near(2, 0, last)
    finish(2, go_st)
    fin.append(local(go_st, go_out))
    fin[1].start()
    near(0, 0)
    finish(0, gq_st)
    fin.append(local(gq_st, gq_out))
    fin[2].start()
    for b in backs:
        b.wait_recv()
    done[1][0].wait()
    for c, out, back in done:
        back.wait_recv()
    for cond, c in sends:
        on(cond, c.wait_send)
    for c in locals_ + fin:
        c.wait()
    for g in range(3):
        for kk in range(4):
            ysend(g, kk).wait_send()
            if kk:
                zsend(g, kk).wait_send()


def copy_kernel(*refs):
    srcs, dsts, bufs, rsem, wsem = refs[:5], refs[5:10], refs[10:15], refs[15], refs[16]
    ins, outs = [], []
    for a in range(5):
        rows = srcs[a].shape[0]
        parts = 8 if a < 2 else 1
        for c in range(parts):
            r = pl.ds(c * (rows // parts), rows // parts)
            i = len(ins)
            ins.append(pltpu.make_async_copy(srcs[a].at[r], bufs[a].at[r], rsem.at[i]))
            outs.append(pltpu.make_async_copy(bufs[a].at[r], dsts[a].at[r], wsem.at[i]))
    for c in ins:
        c.start()
    for i, o in zip(ins, outs):
        i.wait()
        o.start()
    for o in outs:
        o.wait()


def solution(mesh):
    sd = jax.ShapeDtypeStruct
    DMA = pltpu.SemaphoreType.DMA
    VM = pltpu.VMEM
    ANY = pl.BlockSpec(memory_space=pl.ANY)
    IN_VM = pl.BlockSpec(memory_space=pltpu.VMEM)

    def device_step(x, wq, wkv, wo, gain, positions, dy):
        results = [
            sd((TOKS, D), BF), sd((TOKS, D), BF), sd((H, W), BF), sd((H, W), BF), sd((W, H), BF),
        ]
        outs = results + [
            sd((D, D), BF), sd((D, D), BF), sd((CORE, D), BF), sd((CORE, D), BF), sd((TOKS, W), F32),
        ]
        wide, narrow = VM((TOKS, W), BF), VM((TOKS, H), BF)
        scratch = [
            VM((TOKS, D), BF), VM((D, D), BF), VM((D, W), BF), VM((2, D, H), BF), VM((W, D), BF),
            VM((D, W), BF), VM((W, D), BF), wide, narrow, narrow, VM((12, H, SEQ), F32),
            wide, wide, wide, wide, VM((TOKS, W), F32),
            VM((4, W, H), F32), VM((4, W, H), F32), VM((4, W, H), F32),
            VM((4, H, W), F32), VM((4, H, W), F32), VM((4, H, W), F32),
            VM((4, H, SEQ), F32), VM((4, H, SEQ), F32), VM((4, H, SEQ), F32),
            VM((CORE, D), BF), VM((CORE, D), BF), VM((2, W, W), F32),
            VM((W, H), BF), VM((H, W), BF), VM((H, SEQ), BF),
            DMA((48,)), DMA((112,)), DMA((112,)), DMA((3, 8)), DMA((3, 8)), DMA((3,)), DMA((3,)),
        ]
        res = pl.pallas_call(
            layer_kernel,
            name="layer",
            in_specs=[ANY, IN_VM, ANY, ANY, ANY, ANY, IN_VM],
            out_specs=[ANY] * len(outs),
            out_shape=outs,
            scratch_shapes=scratch,
            cost_estimate=pl.CostEstimate(flops=80_000_000_000, bytes_accessed=100_000_000, transcendentals=0),
            compiler_params=pltpu.CompilerParams(collective_id=0, has_side_effects=True, vmem_limit_bytes=67043328),
        )(x, gain.reshape(1, -1), wq, wkv, wo, dy, positions.reshape(1, -1))
        return pl.pallas_call(
            copy_kernel,
            name="emit",
            in_specs=[ANY] * 5,
            out_specs=[ANY] * 5,
            out_shape=results,
            scratch_shapes=[VM(r.shape, r.dtype) for r in results] + [DMA((19,)), DMA((19,))],
            cost_estimate=pl.CostEstimate(flops=1_000_000, bytes_accessed=27_000_000, transcendentals=0),
            compiler_params=pltpu.CompilerParams(vmem_limit_bytes=60 * 2**20),
        )(*res[:5])

    return jax.shard_map(
        device_step,
        mesh=mesh,
        in_specs=(P("data", None), P("data", "model"), P("data", None), P("model", "data"), P(), P(), P("data", None)),
        out_specs=(P("data", None), P("data", None), P("data", "model"), P("data", None), P("model", "data")),
        check_vma=False,
    )
```

```python
import functools

import jax
import jax.numpy as jnp
from jax import lax
from jax.experimental import pallas as pl
from jax.experimental.pallas import tpu as pltpu
from jax.sharding import PartitionSpec as P

NORM_EPS = 1e-6
ROWS = 512
TOKS = 1536
TILES = 3
SEQS = 4
SEQ = 128
D = 2048
CORE = 768
W = 512
PASS = 384
H = 256
WAYS = (1, -1)
HOPS = (1, 2, 3)
BF = jnp.bfloat16
F32 = jnp.float32


def dot(a, b):
    return jnp.dot(a, b, preferred_element_type=F32)


def dot_t(a, b):
    return lax.dot_general(a, b, (((1,), (1,)), ((), ())), preferred_element_type=F32)


def t_dot(a, b):
    return lax.dot_general(a, b, (((0,), (0,)), ((), ())), preferred_element_type=F32)


MESH = pl.DeviceIdType.MESH


def cols(i, width=H):
    return pl.ds(pl.multiple_of(i * width, width), width)


def norm(x):
    c = x - jnp.mean(x, axis=-1, keepdims=True)
    inv = lax.rsqrt(jnp.mean(c * c, axis=-1, keepdims=True) + NORM_EPS)
    return c * inv, inv


def stack_heads(a):
    return jnp.concatenate([a[:, :H], a[:, H:]], axis=0)


def spread_heads(a):
    return jnp.concatenate([a[:SEQ], a[SEQ:]], axis=1)


def softmax(s, mask2):
    s = jnp.where(mask2 > 0, s * (H ** -0.5), -1e30)
    e = jnp.exp(s - jnp.max(s, axis=-1, keepdims=True))
    return e / jnp.sum(e, axis=-1, keepdims=True)


def attend(qs, ks, vs, mask2):
    scores = [dot_t(q, k) for q, k in zip(qs, ks)]
    probs = [softmax(s, mask2) for s in scores]
    return probs, [dot(p.astype(BF), v).astype(BF) for p, v in zip(probs, vs)]


def attend_back(qs, ks, vs, probs, dos):
    dps = [dot_t(do, v) for do, v in zip(dos, vs)]
    dvs = [t_dot(p.astype(BF), do) for p, do in zip(probs, dos)]
    dss = [p * (dp - jnp.sum(p * dp, axis=-1, keepdims=True)) for p, dp in zip(probs, dps)]
    dss = [(ds * (H ** -0.5)).astype(BF) for ds in dss]
    dqs = [dot(ds, k).astype(BF) for ds, k in zip(dss, ks)]
    dks = [t_dot(ds, q) for ds, q in zip(dss, qs)]
    return dqs, dks, dvs


def drop(items, item):
    items[:] = [i for i in items if i is not item]


def layer_kernel(
    x_hbm, gain, wq_hbm, wkv_hbm, wo_hbm, dy_hbm, pos,
    y_out, dx_out, gq_out, gkv_out, go_out, wq_all, wo_all, o_all, dq_all, dkv_mate,
    xh, big, wq, wkv, wo, wqx, wox, q, k, v, probs, o, ox, dq, dqx, dkv,
    ofar, ory, orz, qfar, qry, qrz, kfar, kry, krz, tin, stage, dkvt, go_st, gq_st, gk_st,
    lsem, ssem, rsem, gss, gsr, dks, dkr,
):
    d, m = lax.axis_index("data"), lax.axis_index("model")
    z, y = d // 2, d % 2
    core = m % 2
    zpeer = [((z + s) % 4) * 2 + y for s in range(SEQS)]
    ypeer = z * 2 + 1 - y
    mate = m + 1 - 2 * core
    across = (m + 2) % 4
    diag = (mate + 2) % 4
    mine = pl.ds(pl.multiple_of(core * CORE, CORE), CORE)
    theirs = pl.ds(pl.multiple_of((1 - core) * CORE, CORE), CORE)
    used = {"l": 0, "r": 0}
    sends = []

    def local(src, dst):
        i = used["l"]
        used["l"] += 1
        return pltpu.make_async_copy(src, dst, lsem.at[i])

    def remote(src, dst, land, axis, peer, when=None):
        i = used["r"]
        used["r"] += 1
        args = dict(send_sem=ssem.at[i], recv_sem=rsem.at[i], device_id={axis: peer}, device_id_type=MESH)
        out = pltpu.make_async_remote_copy(src_ref=src, dst_ref=dst, **args)
        back = pltpu.make_async_remote_copy(src_ref=land, dst_ref=land, **args)
        sends.append((when, out))
        return out, back

    loads = [local(x_hbm.at[cols(t, ROWS)], xh.at[cols(t, ROWS)]) for t in range(3)]
    half = cols(core)
    own = [local(wq_hbm, wq.at[cols(d)]), local(wkv_hbm.at[:, half], wkv.at[core, cols(d)]), local(wo_hbm, wo.at[:, cols(d)])]
    dy_load = local(dy_hbm, big.at[pl.ds(0, TOKS)])
    for c in loads + own + [dy_load]:
        c.start()

    barrier = pltpu.get_barrier_semaphore()
    for peer in zpeer[1:] + [ypeer]:
        pl.semaphore_signal(barrier, inc=1, device_id={"data": peer}, device_id_type=MESH)
    for peer in (mate, across, diag):
        pl.semaphore_signal(barrier, inc=1, device_id={"model": peer}, device_id_type=MESH)
    pl.semaphore_wait(barrier, 7)

    shard = {0: wq_hbm, 1: wkv_hbm.at[:, half], 3: wo_hbm}

    def slot(a, zz):
        blk = zz * 2 + (1 - y if a in (2, 4) else y)
        return wq.at[cols(blk)] if a == 0 else wkv.at[core, cols(blk)] if a < 3 else wo.at[:, cols(blk)]

    def got(way, r):
        return z >= r if way > 0 else z + r <= 3

    def origin(way, r):
        return (z + 4 - r) % 4 if way > 0 else (z + r) % 4

    def goes(way):
        return z < 3 if way > 0 else z > 0

    def sent(way, r):
        return goes(way) if r == 1 else jnp.logical_and(got(way, r - 1), goes(way))

    hops, ys, xs, cs = {}, {}, {}, {}
    for r in HOPS:
        for way in WAYS:
            for a in (0, 1, 3, 4):
                here = origin(way, r - 1)
                src = shard[a] if r == 1 and a in shard else slot(a, here)
                to = ((z + way + 4) % 4) * 2 + y
                hops[a, way, r] = remote(src, slot(a, here), slot(a, origin(way, r)), "data", to, sent(way, r))
    keys = [None] + [(way, r) for r in HOPS for way in WAYS]
    ys[3, None] = remote(wo_hbm, slot(3, z), slot(4, z), "data", ypeer)
    for key in keys:
        zz = z if key is None else origin(*key)
        cond = None if key is None else got(*key)
        there = wq.at[cols(zz * 2 + 1 - y)]
        src = wq_hbm if key is None else slot(0, zz)
        ys[0, key] = remote(src, slot(0, zz), there, "data", ypeer, cond)
        xs[0, key] = remote(src, wqx.at[cols(zz * 2 + y)], wqx.at[cols(zz * 2 + y)], "model", across, cond)
        xs[5, key] = remote(there, wqx.at[cols(zz * 2 + 1 - y)], wqx.at[cols(zz * 2 + 1 - y)], "model", across, cond)
        for a in (3, 4):
            src = shard[a] if key is None and a == 3 else slot(a, zz)
            to = wox.at[:, cols(zz * 2 + (y if a == 3 else 1 - y))]
            xs[a, key] = remote(src, to, to, "model", across, cond)
        src = shard[1] if key is None else slot(1, zz)
        ys[1, key] = remote(src, slot(1, zz), slot(2, zz), "data", ypeer, cond)
        for a in (1, 2):
            blk = zz * 2 + (y if a == 1 else 1 - y)
            cs[a, key] = remote(src if a == 1 else slot(2, zz), slot(a, zz), wkv.at[1 - core, cols(blk)], "model", mate, cond)

    def on(cond, fn):
        if cond is None:
            fn()
        else:
            pl.when(cond)(fn)

    def start_hop(a, way, r):
        on(sent(way, r), lambda: hops[a, way, r][0].start())

    for way in WAYS:
        start_hop(0, way, 1)
    ys[0, None][0].start()
    ys[1, None][0].start()
    xs[0, None][0].start()
    xs[3, None][0].start()
    cs[1, None][0].start()

    for t in range(3):
        loads[t].wait()

        @pl.loop(t * 4, t * 4 + 4)
        def _(i):
            r = cols(i, SEQ)
            n, _inv = norm(xh[r, :].astype(F32))
            xh[r, :] = (n * gain[...]).astype(BF)

    for c in own:
        c.wait()

    def take(arrays, way, r):
        for a in arrays:
            hops[a, way, r][1].wait_recv()
            if r < 3:
                start_hop(a, way, r + 1)
            if a < 2:
                ys[a, (way, r)][0].start()
            (cs if a == 1 else xs)[a, (way, r)][0].start()

    def relay(arrays, r):
        for way in WAYS:
            on(jnp.logical_and(got(way, r), goes(way)), lambda way=way: take(arrays, way, r))

    def keep(arrays, r):
        for way in WAYS:
            on(jnp.logical_and(got(way, r), jnp.logical_not(goes(way))), lambda way=way: take(arrays, way, r))

    def take_all(arrays, r):
        for way in WAYS:
            on(got(way, r), lambda way=way: take(arrays, way, r))

    def arrive(a, key):
        def go():
            ys[a, key][1].wait_recv()
            (cs[2, key] if a else xs[5, key])[0].start()

        on(None if key is None else got(*key), go)

    take_all((0,), 1)
    for way in WAYS:
        start_hop(1, way, 1)
    take_all((0,), 2)
    take_all((1,), 1)
    take_all((0,), 3)
    for key in keys[:5]:
        arrive(0, key)
    relay((1,), 2)
    for way in WAYS:
        start_hop(3, way, 1)
    for key in keys[5:]:
        arrive(0, key)

    locals_ = []

    def share(src, dst, slot_of):
        c = local(src, dst.at[slot_of(0)])
        out, back = remote(src, dst.at[slot_of(0)], dst.at[slot_of(1)], "model", mate)
        c.start()
        out.start()
        locals_.append(c)
        return c, out, back

    def colslot(base):
        other = base + 1 - 2 * (base % 2)
        return lambda n: (slice(None), cols(base if n == 0 else other, W))

    def rowslot(base):
        other = base + 1 - 2 * (base % 2)
        return lambda n: (cols(base if n == 0 else other, W),)

    def share_rows(src, dst, base):
        other = base + 1 - 2 * (base % 2)
        c = local(src.at[mine], dst.at[:, cols(base, W)])
        out, back = remote(src.at[theirs], dst.at[:, cols(base, W)], dst.at[:, cols(other, W)], "model", mate)
        c.start()
        out.start()
        locals_.append(c)
        return c, out, back

    wq_sh = share(wq, wq_all, colslot(m))

    @pl.loop(0, TILES)
    def _(t):
        r = cols(t, ROWS)
        q[r, :] = dot(xh[r, :], wq[...]).astype(BF)

    relay((3,), 1)
    keep((1,), 2)
    take_all((1,), 3)
    ys[3, None][0].start()
    for key in keys:
        arrive(1, key)
    for key in keys:
        on(None if key is None else got(*key), lambda key=key: [cs[a, key][1].wait_recv() for a in (1, 2)] and None)

    @pl.loop(0, TILES)
    def _(t):
        r = cols(t, ROWS)
        k[r, :] = dot(xh[r, :], wkv[0]).astype(BF)
        v[r, :] = dot(xh[r, :], wkv[1]).astype(BF)

    ys[3, None][1].wait_recv()
    xs[4, None][0].start()
    for way in WAYS:
        start_hop(4, way, 1)
    posm = jnp.broadcast_to(pos[...].astype(F32), (SEQ, SEQ))
    mask = (posm <= posm.T).astype(F32)
    mask2 = jnp.concatenate([mask, mask], axis=0)

    @pl.loop(0, TILES)
    def _(t):
        rows = [cols(t * 4 + b, SEQ) for b in range(SEQS)]
        qs = [stack_heads(q[r, :]) for r in rows]
        ps, os = attend(qs, [k[r, :] for r in rows], [v[r, :] for r in rows], mask2)
        for b in range(SEQS):
            probs[t * 4 + b] = ps[b]
            wide = spread_heads(os[b])
            o[rows[b], :] = wide
            big[pl.ds(TOKS, W), rows[b]] = wide.T

    dy_load.wait()
    o_sh = share_rows(o, o_all, m)

    far = [qfar, kfar, ofar]
    ry = [qry, kry, ory]
    rz = [qrz, krz, orz]

    def piece(g, blk):
        if g == 2:
            return dot(big[pl.ds(TOKS, W), pl.ds(0, TOKS)], big[pl.ds(0, TOKS), cols(blk)])
        return t_dot(xh[:, cols(blk)], dq[...] if g == 0 else q[:, cols(m, SEQ)])

    def ysend(g, kk):
        return pltpu.make_async_remote_copy(
            src_ref=far[g].at[kk], dst_ref=ry[g].at[kk], send_sem=gss.at[g, kk], recv_sem=gsr.at[g, kk],
            device_id={"data": ypeer}, device_id_type=MESH,
        )

    upper = z // 2
    inner = jnp.logical_and(z > 0, z < 3)

    def zcopy(g, kk, place, peer):
        return pltpu.make_async_remote_copy(
            src_ref=ry[g].at[kk], dst_ref=rz[g].at[place], send_sem=gss.at[g, 4 + kk], recv_sem=gsr.at[g, 4 + place],
            device_id={"data": peer}, device_id_type=MESH,
        )

    def zsend(g, kk):
        if kk == 2 and g != 1:
            return zcopy(g, kk, 2 + upper, (z + 1 - 2 * upper) * 2 + y)
        if kk == 2:
            return zcopy(g, kk, 2, zpeer[2])
        return zcopy(g, kk, kk // 2, zpeer[kk])

    def merge(g):
        @pl.when(inner)
        def _():
            for kk in (3, 1):
                zcopy(g, 2, 2 + kk // 2, ypeer).wait_recv()
                ry[g][kk] = ry[g][kk] + rz[g][2 + kk // 2]
                zsend(g, kk).start()

    def send_far(g, lo, hi):
        @pl.loop(lo, hi)
        def _(i):
            kk = 2 + i + (i // 2) * (1 - 2 * i)
            far[g][kk] = piece(g, ((z + kk) % 4) * 2 + 1 - y)
            pl.when(jnp.logical_or(kk > 0, g == 1))(lambda: ysend(g, kk).start())

    def near(g, kk, part=None):
        ysend(g, kk).wait_recv()
        ry[g][kk] = ry[g][kk] + (piece(g, zpeer[kk]) if part is None else part[...])
        if kk == 2 or kk and g == 1:
            zsend(g, kk).start()
        elif kk:
            pl.when(jnp.logical_not(inner))(lambda: zsend(g, kk).start())

    def finish(g, st):
        for kk in (1, 3):
            zsend(g, kk).wait_recv()
        total = ry[g][0] + rz[g][0] + rz[g][1]
        if g == 1:
            zsend(g, 2).wait_recv()
            total = total + rz[g][2]
        st[...] = total.astype(BF)

    relay((3,), 2)
    send_far(2, 0, 4)
    relay((4,), 1)
    relay((4,), 2)
    near(2, 2)
    keep((3, 4), 1)
    keep((3, 4), 2)
    take_all((3, 4), 3)
    wo_sh = share(wo, wo_all, rowslot(m))

    def back_tile(t, q_of, ps, do, add):
        rows = [cols(t * 4 + b, SEQ) for b in range(SEQS)]
        qs, ks, vs = q_of, [k[r, :] for r in rows], [v[r, :] for r in rows]
        dqs, dks, dvs = attend_back(qs, ks, vs, ps, [stack_heads(do[b * SEQ : (b + 1) * SEQ]) for b in range(SEQS)])
        to = dqx if add else dq
        for b, r in enumerate(rows):
            to[r, :] = spread_heads(dqs[b])
            dkv[r, :H] = dkv[r, :H] + dks[b] if add else dks[b]
            dkv[r, H:] = dkv[r, H:] + dvs[b] if add else dvs[b]

    @pl.loop(0, TILES)
    def _(t):
        do = dot_t(big[cols(t, ROWS), :], wo[...]).astype(BF)
        qs = [stack_heads(q[cols(t * 4 + b, SEQ), :]) for b in range(SEQS)]
        back_tile(t, qs, [probs[t * 4 + b] for b in range(SEQS)], do, False)

    dq_sh = share_rows(dq, dq_all, m)
    send_far(0, 0, 4)
    near(2, 3)
    near(2, 1)
    merge(2)

    for key in keys:
        on(None if key is None else got(*key), lambda key=key: [xs[a, key][1].wait_recv() for a in (0, 5)] and None)
    wqx_sh = share(wqx, wq_all, colslot(across))

    @pl.loop(0, TILES)
    def _(t):
        rows = [cols(t * 4 + b, SEQ) for b in range(SEQS)]
        qm = dot(xh[cols(t, ROWS), :], wqx[...]).astype(BF)
        qs = [stack_heads(qm[b * SEQ : (b + 1) * SEQ]) for b in range(SEQS)]
        ps, os = attend(qs, [k[r, :] for r in rows], [v[r, :] for r in rows], mask2)
        dqx[cols(t, ROWS), :] = qm
        for b in range(SEQS):
            probs[t * 4 + b] = ps[b]
            ox[rows[b], :] = spread_heads(os[b])

    ox_sh = share_rows(ox, o_all, across)
    near(0, 2)
    for key in keys:
        on(None if key is None else got(*key), lambda key=key: [xs[a, key][1].wait_recv() for a in (3, 4)] and None)
    wox_sh = share(wox, wo_all, rowslot(across))

    def dkv_send(t):
        r = cols(t, ROWS)
        return pltpu.make_async_remote_copy(
            src_ref=dkv.at[r], dst_ref=dkv_mate.at[r], send_sem=dks.at[t], recv_sem=dkr.at[t],
            device_id={"model": mate}, device_id_type=MESH,
        )

    @pl.loop(0, TILES)
    def _(t):
        do = dot_t(big[cols(t, ROWS), :], wox[...]).astype(BF)
        qs = [stack_heads(dqx[cols(t * 4 + b, SEQ), :]) for b in range(SEQS)]
        back_tile(t, qs, [probs[t * 4 + b] for b in range(SEQS)], do, True)
        dkv_send(t).start()

    dqx_sh = share_rows(dqx, dq_all, across)

    tiles = []
    for t in range(3):
        dkv_send(t).wait_recv()
        tiles.append(local(dkv_mate.at[cols(t, ROWS)], dkvt.at[t % 2]))
        if t < 2:
            tiles[t].start()
    for t in range(3):
        tiles[t].wait()
        q[cols(t, ROWS), :] = (dkv[cols(t, ROWS), :] + dkvt[t % 2]).astype(BF)
        if t == 0:
            tiles[2].start()
    send_far(1, 0, 4)
    ysend(2, 0).start()
    ysend(0, 0).start()
    last = dkvt.at[0, :, pl.ds(0, H)]
    last[...] = piece(2, zpeer[0])
    near(0, 3)

    for sh in (wo_sh, wox_sh, o_sh, ox_sh):
        sh[0].wait()
        sh[2].wait_recv()
        drop(locals_, sh[0])
    fetch = local(o_all, tin)
    fetch.start()
    fill = [local(wo_all.at[:, cols(i, W)], big.at[:, cols(i, W)]) for i in range(SEQS)]
    for c in fill:
        c.start()
    fetch.wait()

    def y_cols(lo, hi):
        @pl.loop(lo, hi)
        def _(i):
            stage[:, cols(i)] = dot(tin[...], big[:, cols(i)]).astype(BF)

    done = []

    def emit(dst):
        c = local(stage, dst.at[mine])
        out, back = remote(stage, dst.at[mine], dst.at[theirs], "model", mate)
        c.start()
        out.start()
        done.append((c, out, back))

    for i in range(SEQS):
        fill[i].wait()
        y_cols(2 * i, 2 * i + 2)
        if i == 1:
            near(0, 1)
            merge(0)
    emit(y_out)

    for sh in (wq_sh, wqx_sh, dq_sh, dqx_sh):
        sh[0].wait()
        sh[2].wait_recv()
        drop(locals_, sh[0])
    fetch = local(dq_all, tin)
    fetch.start()
    fill = [local(wq_all.at[cols(i, W)], big.at[cols(i, W)]) for i in range(SEQS)]
    for c in fill:
        c.start()
    wox_sh[1].wait_send()
    sends[:] = [s for s in sends if s[1] is not wox_sh[1]]
    xin = [local(x_hbm.at[pl.ds(pl.multiple_of(core * CORE + p * PASS, PASS), PASS)], wox.at[pl.ds(0, PASS)]) for p in range(2)]
    xin[0].start()
    for t in range(3):
        dkv_send(t).wait_send()
    fetch.wait()
    for p in range(2):
        rows = pl.ds(pl.multiple_of(core * CORE + p * PASS, PASS), PASS)

        def dh_cols(i):
            c = cols(i, W)
            g = dot_t(tin[pl.ds(p * PASS, PASS), :], big[c, :])
            g = g + dot_t(q[rows, :H], wkv[0, c, :])
            dkv[cols(i, PASS), :] = g + dot_t(q[rows, H:], wkv[1, c, :])

        if p == 0:
            for n in range(SEQS):
                fill[n].wait()
                pl.loop(n, n + 1)(dh_cols)
        else:
            pl.loop(0, 4)(dh_cols)

        xin[p].wait()
        if p == 0:
            done[0][0].wait()
            done[0][1].wait_send()
            sends[:] = [s for s in sends if s[1] is not done[0][1]]

        @pl.loop(0, TILES)
        def _(i):
            n, inv = norm(wox[cols(i, SEQ), :].astype(F32))
            gn = jnp.concatenate([dkv[pl.ds(pl.multiple_of(c * PASS + i * SEQ, SEQ), SEQ), :] for c in range(SEQS)], axis=1) * gain[...]
            g = inv * (gn - jnp.mean(gn, axis=-1, keepdims=True) - n * jnp.mean(gn * n, axis=-1, keepdims=True))
            stage[pl.ds(pl.multiple_of(p * PASS + i * SEQ, SEQ), SEQ), :] = g.astype(BF)

        if p == 0:
            xin[1].start()
            for kk in (2, 3, 1, 0):
                near(1, kk)
    emit(dx_out)
    lastq = dkvt.at[1, pl.ds(0, H)]
    lastq[...] = piece(0, zpeer[0])

    finish(1, gk_st)
    fin = [local(gk_st, gkv_out.at[:, cols(m, SEQ)])]
    fin[0].start()
    backs = []
    for peer in (mate, across, diag):
        out, back = remote(gk_st, gkv_out.at[:, cols(m, SEQ)], gkv_out.at[:, cols(peer, SEQ)], "model", peer)
        out.start()
        backs.append(back)

    near(2, 0, last)
    finish(2, go_st)
    fin.append(local(go_st, go_out))
    fin[1].start()
    near(0, 0, lastq)
    finish(0, gq_st)
    fin.append(local(gq_st, gq_out))
    fin[2].start()
    for b in backs:
        b.wait_recv()
    done[1][0].wait()
    for c, out, back in done:
        back.wait_recv()
    for cond, c in sends:
        on(cond, c.wait_send)
    for c in locals_ + fin:
        c.wait()
    for g in range(3):
        for kk in range(SEQS):
            ysend(g, kk).wait_send()
            if kk:
                zsend(g, kk).wait_send()


def copy_kernel(*refs):
    srcs, dsts, bufs, rsem, wsem = refs[:5], refs[5:10], refs[10:15], refs[15], refs[16]
    ins, outs = [], []
    for a in range(5):
        rows = srcs[a].shape[0]
        parts = 8 if a < 2 else 1
        for c in range(parts):
            r = pl.ds(c * (rows // parts), rows // parts)
            i = len(ins)
            ins.append(pltpu.make_async_copy(srcs[a].at[r], bufs[a].at[r], rsem.at[i]))
            outs.append(pltpu.make_async_copy(bufs[a].at[r], dsts[a].at[r], wsem.at[i]))
    for c in ins:
        c.start()
    for i, o in zip(ins, outs):
        i.wait()
        o.start()
    for o in outs:
        o.wait()


def solution(mesh):
    sd = jax.ShapeDtypeStruct
    DMA = pltpu.SemaphoreType.DMA
    VM = pltpu.VMEM
    ANY = pl.BlockSpec(memory_space=pl.ANY)
    IN_VM = pl.BlockSpec(memory_space=pltpu.VMEM)

    def device_step(x, wq, wkv, wo, gain, positions, dy):
        results = [
            sd((TOKS, D), BF), sd((TOKS, D), BF), sd((H, W), BF), sd((H, W), BF), sd((W, H), BF),
        ]
        outs = results + [
            sd((D, D), BF), sd((D, D), BF), sd((CORE, D), BF), sd((CORE, D), BF), sd((TOKS, W), F32),
        ]
        wide, narrow = VM((TOKS, W), BF), VM((TOKS, H), BF)
        scratch = [
            VM((TOKS, D), BF), VM((D, D), BF), VM((D, W), BF), VM((2, D, H), BF), VM((W, D), BF),
            VM((D, W), BF), VM((W, D), BF), wide, narrow, narrow, VM((12, H, SEQ), F32),
            wide, wide, wide, wide, VM((TOKS, W), F32),
            VM((4, W, H), F32), VM((4, W, H), F32), VM((4, W, H), F32),
            VM((4, H, W), F32), VM((4, H, W), F32), VM((4, H, W), F32),
            VM((4, H, SEQ), F32), VM((4, H, SEQ), F32), VM((4, H, SEQ), F32),
            VM((CORE, D), BF), VM((CORE, D), BF), VM((2, W, W), F32),
            VM((W, H), BF), VM((H, W), BF), VM((H, SEQ), BF),
            DMA((48,)), DMA((112,)), DMA((112,)), DMA((3, 8)), DMA((3, 8)), DMA((3,)), DMA((3,)),
        ]
        res = pl.pallas_call(
            layer_kernel,
            name="layer",
            in_specs=[ANY, IN_VM, ANY, ANY, ANY, ANY, IN_VM],
            out_specs=[ANY] * len(outs),
            out_shape=outs,
            scratch_shapes=scratch,
            cost_estimate=pl.CostEstimate(flops=80_000_000_000, bytes_accessed=100_000_000, transcendentals=0),
            compiler_params=pltpu.CompilerParams(collective_id=0, has_side_effects=True, vmem_limit_bytes=67043328),
        )(x, gain.reshape(1, -1), wq, wkv, wo, dy, positions.reshape(1, -1))
        return pl.pallas_call(
            copy_kernel,
            name="emit",
            in_specs=[ANY] * 5,
            out_specs=[ANY] * 5,
            out_shape=results,
            scratch_shapes=[VM(r.shape, r.dtype) for r in results] + [DMA((19,)), DMA((19,))],
            cost_estimate=pl.CostEstimate(flops=1_000_000, bytes_accessed=27_000_000, transcendentals=0),
            compiler_params=pltpu.CompilerParams(vmem_limit_bytes=60 * 2**20),
        )(*res[:5])

    return jax.shard_map(
        device_step,
        mesh=mesh,
        in_specs=(P("data", None), P("data", "model"), P("data", None), P("model", "data"), P(), P(), P("data", None)),
        out_specs=(P("data", None), P("data", None), P("data", "model"), P("data", None), P("model", "data")),
        check_vma=False,
    )
```

```python
import functools

import jax
import jax.numpy as jnp
from jax import lax
from jax.experimental import pallas as pl
from jax.experimental.pallas import tpu as pltpu
from jax.sharding import PartitionSpec as P

NORM_EPS = 1e-6
ROWS = 512
TOKS = 1536
TILES = 3
SEQS = 4
SEQ = 128
D = 2048
CORE = 768
W = 512
PASS = 384
H = 256
WAYS = (1, -1)
HOPS = (1, 2, 3)
BF = jnp.bfloat16
F32 = jnp.float32


def dot(a, b):
    return jnp.dot(a, b, preferred_element_type=F32)


def dot_t(a, b):
    return lax.dot_general(a, b, (((1,), (1,)), ((), ())), preferred_element_type=F32)


def t_dot(a, b):
    return lax.dot_general(a, b, (((0,), (0,)), ((), ())), preferred_element_type=F32)


MESH = pl.DeviceIdType.MESH


def cols(i, width=H):
    return pl.ds(pl.multiple_of(i * width, width), width)


def norm(x):
    c = x - jnp.mean(x, axis=-1, keepdims=True)
    inv = lax.rsqrt(jnp.mean(c * c, axis=-1, keepdims=True) + NORM_EPS)
    return c * inv, inv


def stack_heads(a):
    return jnp.concatenate([a[:, :H], a[:, H:]], axis=0)


def spread_heads(a):
    return jnp.concatenate([a[:SEQ], a[SEQ:]], axis=1)


def softmax(s, mask2):
    s = jnp.where(mask2 > 0, s * (H ** -0.5), -1e30)
    e = jnp.exp(s - jnp.max(s, axis=-1, keepdims=True))
    return e / jnp.sum(e, axis=-1, keepdims=True)


def attend(qs, ks, vs, mask2):
    scores = [dot_t(q, k) for q, k in zip(qs, ks)]
    probs = [softmax(s, mask2) for s in scores]
    return probs, [dot(p.astype(BF), v).astype(BF) for p, v in zip(probs, vs)]


def attend_back(qs, ks, vs, probs, dos):
    dps = [dot_t(do, v) for do, v in zip(dos, vs)]
    dvs = [t_dot(p.astype(BF), do) for p, do in zip(probs, dos)]
    dss = [p * (dp - jnp.sum(p * dp, axis=-1, keepdims=True)) for p, dp in zip(probs, dps)]
    dss = [(ds * (H ** -0.5)).astype(BF) for ds in dss]
    dqs = [dot(ds, k).astype(BF) for ds, k in zip(dss, ks)]
    dks = [t_dot(ds, q) for ds, q in zip(dss, qs)]
    return dqs, dks, dvs


def drop(items, item):
    items[:] = [i for i in items if i is not item]


def layer_kernel(
    x_hbm, gain, wq_hbm, wkv_hbm, wo_hbm, dy_hbm, pos,
    y_out, dx_out, gq_out, gkv_out, go_out, wq_all, wo_all, o_all, dq_all, dkv_mate,
    xh, big, wq, wkv, wo, wqx, wox, q, k, v, probs, o, ox, dq, dqx, dkv,
    ofar, ory, orz, qfar, qry, qrz, kfar, kry, krz, tin, stage, dkvt, go_st, gq_st, gk_st,
    lsem, ssem, rsem, gss, gsr, dks, dkr,
):
    d, m = lax.axis_index("data"), lax.axis_index("model")
    z, y = d // 2, d % 2
    core = m % 2
    zpeer = [((z + s) % 4) * 2 + y for s in range(SEQS)]
    ypeer = z * 2 + 1 - y
    mate = m + 1 - 2 * core
    across = (m + 2) % 4
    diag = (mate + 2) % 4
    mine = pl.ds(pl.multiple_of(core * CORE, CORE), CORE)
    theirs = pl.ds(pl.multiple_of((1 - core) * CORE, CORE), CORE)
    used = {"l": 0, "r": 0}
    sends = []

    def local(src, dst):
        i = used["l"]
        used["l"] += 1
        return pltpu.make_async_copy(src, dst, lsem.at[i])

    def remote(src, dst, land, axis, peer, when=None):
        i = used["r"]
        used["r"] += 1
        args = dict(send_sem=ssem.at[i], recv_sem=rsem.at[i], device_id={axis: peer}, device_id_type=MESH)
        out = pltpu.make_async_remote_copy(src_ref=src, dst_ref=dst, **args)
        back = pltpu.make_async_remote_copy(src_ref=land, dst_ref=land, **args)
        sends.append((when, out))
        return out, back

    loads = [local(x_hbm.at[cols(t, ROWS)], xh.at[cols(t, ROWS)]) for t in range(3)]
    half = cols(core)
    own = [local(wq_hbm, wq.at[cols(d)]), local(wkv_hbm.at[:, half], wkv.at[core, cols(d)]), local(wo_hbm, wo.at[:, cols(d)])]
    dy_load = local(dy_hbm, big.at[pl.ds(0, TOKS)])
    for c in loads + own + [dy_load]:
        c.start()

    barrier = pltpu.get_barrier_semaphore()
    for peer in zpeer[1:] + [ypeer]:
        pl.semaphore_signal(barrier, inc=1, device_id={"data": peer}, device_id_type=MESH)
    for peer in (mate, across, diag):
        pl.semaphore_signal(barrier, inc=1, device_id={"model": peer}, device_id_type=MESH)
    pl.semaphore_wait(barrier, 7)

    shard = {0: wq_hbm, 1: wkv_hbm.at[:, half], 3: wo_hbm}

    def slot(a, zz):
        blk = zz * 2 + (1 - y if a in (2, 4) else y)
        return wq.at[cols(blk)] if a == 0 else wkv.at[core, cols(blk)] if a < 3 else wo.at[:, cols(blk)]

    def got(way, r):
        return z >= r if way > 0 else z + r <= 3

    def origin(way, r):
        return (z + 4 - r) % 4 if way > 0 else (z + r) % 4

    def goes(way):
        return z < 3 if way > 0 else z > 0

    def sent(way, r):
        return goes(way) if r == 1 else jnp.logical_and(got(way, r - 1), goes(way))

    hops, ys, xs, cs = {}, {}, {}, {}
    for r in HOPS:
        for way in WAYS:
            for a in (0, 1, 3, 4):
                here = origin(way, r - 1)
                src = shard[a] if r == 1 and a in shard else slot(a, here)
                to = ((z + way + 4) % 4) * 2 + y
                hops[a, way, r] = remote(src, slot(a, here), slot(a, origin(way, r)), "data", to, sent(way, r))
    keys = [None] + [(way, r) for r in HOPS for way in WAYS]
    ys[3, None] = remote(wo_hbm, slot(3, z), slot(4, z), "data", ypeer)
    for key in keys:
        zz = z if key is None else origin(*key)
        cond = None if key is None else got(*key)
        there = wq.at[cols(zz * 2 + 1 - y)]
        src = wq_hbm if key is None else slot(0, zz)
        ys[0, key] = remote(src, slot(0, zz), there, "data", ypeer, cond)
        xs[0, key] = remote(src, wqx.at[cols(zz * 2 + y)], wqx.at[cols(zz * 2 + y)], "model", across, cond)
        xs[5, key] = remote(there, wqx.at[cols(zz * 2 + 1 - y)], wqx.at[cols(zz * 2 + 1 - y)], "model", across, cond)
        for a in (3, 4):
            src = shard[a] if key is None and a == 3 else slot(a, zz)
            to = wox.at[:, cols(zz * 2 + (y if a == 3 else 1 - y))]
            xs[a, key] = remote(src, to, to, "model", across, cond)
        src = shard[1] if key is None else slot(1, zz)
        ys[1, key] = remote(src, slot(1, zz), slot(2, zz), "data", ypeer, cond)
        for a in (1, 2):
            blk = zz * 2 + (y if a == 1 else 1 - y)
            cs[a, key] = remote(src if a == 1 else slot(2, zz), slot(a, zz), wkv.at[1 - core, cols(blk)], "model", mate, cond)

    def on(cond, fn):
        if cond is None:
            fn()
        else:
            pl.when(cond)(fn)

    def start_hop(a, way, r):
        on(sent(way, r), lambda: hops[a, way, r][0].start())

    for way in WAYS:
        start_hop(0, way, 1)
    ys[0, None][0].start()
    ys[1, None][0].start()
    xs[0, None][0].start()
    xs[3, None][0].start()
    cs[1, None][0].start()

    for t in range(3):
        loads[t].wait()

        @pl.loop(t * 4, t * 4 + 4)
        def _(i):
            r = cols(i, SEQ)
            n, _inv = norm(xh[r, :].astype(F32))
            xh[r, :] = (n * gain[...]).astype(BF)

    for c in own:
        c.wait()

    def take(arrays, way, r):
        for a in arrays:
            hops[a, way, r][1].wait_recv()
            if r < 3:
                start_hop(a, way, r + 1)
            if a < 2:
                ys[a, (way, r)][0].start()
            (cs if a == 1 else xs)[a, (way, r)][0].start()

    def relay(arrays, r):
        for way in WAYS:
            on(jnp.logical_and(got(way, r), goes(way)), lambda way=way: take(arrays, way, r))

    def keep(arrays, r):
        for way in WAYS:
            on(jnp.logical_and(got(way, r), jnp.logical_not(goes(way))), lambda way=way: take(arrays, way, r))

    def take_all(arrays, r):
        for way in WAYS:
            on(got(way, r), lambda way=way: take(arrays, way, r))

    def arrive(a, key):
        def go():
            ys[a, key][1].wait_recv()
            (cs[2, key] if a else xs[5, key])[0].start()

        on(None if key is None else got(*key), go)

    take_all((0,), 1)
    for way in WAYS:
        start_hop(1, way, 1)
    take_all((0,), 2)
    take_all((1,), 1)
    take_all((0,), 3)
    for key in keys[:5]:
        arrive(0, key)
    relay((1,), 2)
    for way in WAYS:
        start_hop(3, way, 1)
    for key in keys[5:]:
        arrive(0, key)

    locals_ = []

    def share(src, dst, slot_of):
        c = local(src, dst.at[slot_of(0)])
        out, back = remote(src, dst.at[slot_of(0)], dst.at[slot_of(1)], "model", mate)
        c.start()
        out.start()
        locals_.append(c)
        return c, out, back

    def colslot(base):
        other = base + 1 - 2 * (base % 2)
        return lambda n: (slice(None), cols(base if n == 0 else other, W))

    def rowslot(base):
        other = base + 1 - 2 * (base % 2)
        return lambda n: (cols(base if n == 0 else other, W),)

    def share_rows(src, dst, base):
        other = base + 1 - 2 * (base % 2)
        c = local(src.at[mine], dst.at[:, cols(base, W)])
        out, back = remote(src.at[theirs], dst.at[:, cols(base, W)], dst.at[:, cols(other, W)], "model", mate)
        c.start()
        out.start()
        locals_.append(c)
        return c, out, back

    wq_sh = share(wq, wq_all, colslot(m))

    @pl.loop(0, TILES)
    def _(t):
        r = cols(t, ROWS)
        q[r, :] = dot(xh[r, :], wq[...]).astype(BF)

    relay((3,), 1)
    keep((1,), 2)
    take_all((1,), 3)
    ys[3, None][0].start()
    for key in keys:
        arrive(1, key)
    for key in keys:
        on(None if key is None else got(*key), lambda key=key: [cs[a, key][1].wait_recv() for a in (1, 2)] and None)

    @pl.loop(0, TILES)
    def _(t):
        r = cols(t, ROWS)
        k[r, :] = dot(xh[r, :], wkv[0]).astype(BF)
        v[r, :] = dot(xh[r, :], wkv[1]).astype(BF)

    ys[3, None][1].wait_recv()
    xs[4, None][0].start()
    for way in WAYS:
        start_hop(4, way, 1)
    posm = jnp.broadcast_to(pos[...].astype(F32), (SEQ, SEQ))
    mask = (posm <= posm.T).astype(F32)
    mask2 = jnp.concatenate([mask, mask], axis=0)

    @pl.loop(0, TILES)
    def _(t):
        rows = [cols(t * 4 + b, SEQ) for b in range(SEQS)]
        qs = [stack_heads(q[r, :]) for r in rows]
        ps, os = attend(qs, [k[r, :] for r in rows], [v[r, :] for r in rows], mask2)
        for b in range(SEQS):
            probs[t * 4 + b] = ps[b]
            wide = spread_heads(os[b])
            o[rows[b], :] = wide
            big[pl.ds(TOKS, W), rows[b]] = wide.T

    dy_load.wait()
    o_sh = share_rows(o, o_all, m)

    far = [qfar, kfar, ofar]
    ry = [qry, kry, ory]
    rz = [qrz, krz, orz]

    def piece(g, blk):
        if g == 2:
            return dot(big[pl.ds(TOKS, W), pl.ds(0, TOKS)], big[pl.ds(0, TOKS), cols(blk)])
        return t_dot(xh[:, cols(blk)], dq[...] if g == 0 else q[:, cols(m, SEQ)])

    def ysend(g, kk):
        return pltpu.make_async_remote_copy(
            src_ref=far[g].at[kk], dst_ref=ry[g].at[kk], send_sem=gss.at[g, kk], recv_sem=gsr.at[g, kk],
            device_id={"data": ypeer}, device_id_type=MESH,
        )

    upper = z // 2
    inner = jnp.logical_and(z > 0, z < 3)

    def zcopy(g, kk, place, peer):
        return pltpu.make_async_remote_copy(
            src_ref=ry[g].at[kk], dst_ref=rz[g].at[place], send_sem=gss.at[g, 4 + kk], recv_sem=gsr.at[g, 4 + place],
            device_id={"data": peer}, device_id_type=MESH,
        )

    def zsend(g, kk):
        if kk == 2 and g != 1:
            return zcopy(g, kk, 2 + upper, (z + 1 - 2 * upper) * 2 + y)
        if kk == 2:
            return zcopy(g, kk, 2, zpeer[2])
        return zcopy(g, kk, kk // 2, zpeer[kk])

    def merge(g, kk):
        @pl.when(inner)
        def _():
            zcopy(g, 2, 2 + kk // 2, ypeer).wait_recv()
            ry[g][kk] = ry[g][kk] + rz[g][2 + kk // 2]
            zsend(g, kk).start()

    def send_far(g, lo, hi):
        @pl.loop(lo, hi)
        def _(i):
            kk = 2 + i + (i // 2) * (1 - 2 * i)
            far[g][kk] = piece(g, ((z + kk) % 4) * 2 + 1 - y)
            pl.when(jnp.logical_or(kk > 0, g == 1))(lambda: ysend(g, kk).start())

    def near(g, kk, part=None):
        ysend(g, kk).wait_recv()
        ry[g][kk] = ry[g][kk] + (piece(g, zpeer[kk]) if part is None else part[...])
        if kk == 2 or kk and g == 1:
            zsend(g, kk).start()
        elif kk:
            pl.when(jnp.logical_not(inner))(lambda: zsend(g, kk).start())

    def finish(g, st):
        for kk in (1, 3):
            zsend(g, kk).wait_recv()
        total = ry[g][0] + rz[g][0] + rz[g][1]
        if g == 1:
            zsend(g, 2).wait_recv()
            total = total + rz[g][2]
        st[...] = total.astype(BF)

    relay((3,), 2)
    send_far(2, 0, 4)
    relay((4,), 1)
    relay((4,), 2)
    near(2, 2)
    keep((3, 4), 1)
    keep((3, 4), 2)
    take_all((3, 4), 3)
    wo_sh = share(wo, wo_all, rowslot(m))

    def back_tile(t, q_of, ps, do, add):
        rows = [cols(t * 4 + b, SEQ) for b in range(SEQS)]
        qs, ks, vs = q_of, [k[r, :] for r in rows], [v[r, :] for r in rows]
        dqs, dks, dvs = attend_back(qs, ks, vs, ps, [stack_heads(do[b * SEQ : (b + 1) * SEQ]) for b in range(SEQS)])
        to = dqx if add else dq
        for b, r in enumerate(rows):
            to[r, :] = spread_heads(dqs[b])
            dkv[r, :H] = dkv[r, :H] + dks[b] if add else dks[b]
            dkv[r, H:] = dkv[r, H:] + dvs[b] if add else dvs[b]

    @pl.loop(0, TILES)
    def _(t):
        do = dot_t(big[cols(t, ROWS), :], wo[...]).astype(BF)
        qs = [stack_heads(q[cols(t * 4 + b, SEQ), :]) for b in range(SEQS)]
        back_tile(t, qs, [probs[t * 4 + b] for b in range(SEQS)], do, False)

    dq_sh = share_rows(dq, dq_all, m)
    send_far(0, 0, 4)
    near(2, 3)
    merge(2, 3)
    near(2, 1)
    merge(2, 1)

    for key in keys:
        on(None if key is None else got(*key), lambda key=key: [xs[a, key][1].wait_recv() for a in (0, 5)] and None)
    wqx_sh = share(wqx, wq_all, colslot(across))

    @pl.loop(0, TILES)
    def _(t):
        rows = [cols(t * 4 + b, SEQ) for b in range(SEQS)]
        qm = dot(xh[cols(t, ROWS), :], wqx[...]).astype(BF)
        qs = [stack_heads(qm[b * SEQ : (b + 1) * SEQ]) for b in range(SEQS)]
        ps, os = attend(qs, [k[r, :] for r in rows], [v[r, :] for r in rows], mask2)
        dqx[cols(t, ROWS), :] = qm
        for b in range(SEQS):
            probs[t * 4 + b] = ps[b]
            ox[rows[b], :] = spread_heads(os[b])

    ox_sh = share_rows(ox, o_all, across)
    near(0, 2)
    for key in keys:
        on(None if key is None else got(*key), lambda key=key: [xs[a, key][1].wait_recv() for a in (3, 4)] and None)
    wox_sh = share(wox, wo_all, rowslot(across))

    def dkv_send(t):
        r = cols(t, ROWS)
        return pltpu.make_async_remote_copy(
            src_ref=dkv.at[r], dst_ref=dkv_mate.at[r], send_sem=dks.at[t], recv_sem=dkr.at[t],
            device_id={"model": mate}, device_id_type=MESH,
        )

    @pl.loop(0, TILES)
    def _(t):
        do = dot_t(big[cols(t, ROWS), :], wox[...]).astype(BF)
        qs = [stack_heads(dqx[cols(t * 4 + b, SEQ), :]) for b in range(SEQS)]
        back_tile(t, qs, [probs[t * 4 + b] for b in range(SEQS)], do, True)
        dkv_send(t).start()

    dqx_sh = share_rows(dqx, dq_all, across)

    tiles = []
    for t in range(3):
        dkv_send(t).wait_recv()
        tiles.append(local(dkv_mate.at[cols(t, ROWS)], dkvt.at[t % 2]))
        if t < 2:
            tiles[t].start()
    for t in range(3):
        tiles[t].wait()
        q[cols(t, ROWS), :] = (dkv[cols(t, ROWS), :] + dkvt[t % 2]).astype(BF)
        if t == 0:
            tiles[2].start()
    send_far(1, 0, 4)
    ysend(2, 0).start()
    ysend(0, 0).start()
    last = dkvt.at[0, :, pl.ds(0, H)]
    last[...] = piece(2, zpeer[0])
    near(0, 3)
    merge(0, 3)

    for sh in (wo_sh, wox_sh, o_sh, ox_sh):
        sh[0].wait()
        sh[2].wait_recv()
        drop(locals_, sh[0])
    fetch = local(o_all, tin)
    fetch.start()
    fill = [local(wo_all.at[:, cols(i, W)], big.at[:, cols(i, W)]) for i in range(SEQS)]
    for c in fill:
        c.start()
    fetch.wait()

    def y_cols(lo, hi):
        @pl.loop(lo, hi)
        def _(i):
            stage[:, cols(i)] = dot(tin[...], big[:, cols(i)]).astype(BF)

    done = []

    def emit(dst):
        c = local(stage, dst.at[mine])
        out, back = remote(stage, dst.at[mine], dst.at[theirs], "model", mate)
        c.start()
        out.start()
        done.append((c, out, back))

    for i in range(SEQS):
        fill[i].wait()
        y_cols(2 * i, 2 * i + 2)
        if i == 1:
            near(0, 1)
            merge(0, 1)
    emit(y_out)

    for sh in (wq_sh, wqx_sh, dq_sh, dqx_sh):
        sh[0].wait()
        sh[2].wait_recv()
        drop(locals_, sh[0])
    fetch = local(dq_all, tin)
    fetch.start()
    fill = [local(wq_all.at[cols(i, W)], big.at[cols(i, W)]) for i in range(SEQS)]
    for c in fill:
        c.start()
    wox_sh[1].wait_send()
    sends[:] = [s for s in sends if s[1] is not wox_sh[1]]
    xin = [local(x_hbm.at[pl.ds(pl.multiple_of(core * CORE + p * PASS, PASS), PASS)], wox.at[pl.ds(0, PASS)]) for p in range(2)]
    xin[0].start()
    for t in range(3):
        dkv_send(t).wait_send()
    fetch.wait()
    for p in range(2):
        rows = pl.ds(pl.multiple_of(core * CORE + p * PASS, PASS), PASS)

        def dh_cols(i):
            c = cols(i, W)
            g = dot_t(tin[pl.ds(p * PASS, PASS), :], big[c, :])
            g = g + dot_t(q[rows, :H], wkv[0, c, :])
            dkv[cols(i, PASS), :] = g + dot_t(q[rows, H:], wkv[1, c, :])

        if p == 0:
            for n in range(SEQS):
                fill[n].wait()
                pl.loop(n, n + 1)(dh_cols)
        else:
            pl.loop(0, 4)(dh_cols)

        xin[p].wait()
        if p == 0:
            done[0][0].wait()
            done[0][1].wait_send()
            sends[:] = [s for s in sends if s[1] is not done[0][1]]

        @pl.loop(0, TILES)
        def _(i):
            n, inv = norm(wox[cols(i, SEQ), :].astype(F32))
            gn = jnp.concatenate([dkv[pl.ds(pl.multiple_of(c * PASS + i * SEQ, SEQ), SEQ), :] for c in range(SEQS)], axis=1) * gain[...]
            g = inv * (gn - jnp.mean(gn, axis=-1, keepdims=True) - n * jnp.mean(gn * n, axis=-1, keepdims=True))
            stage[pl.ds(pl.multiple_of(p * PASS + i * SEQ, SEQ), SEQ), :] = g.astype(BF)

        if p == 0:
            xin[1].start()
            for kk in (2, 3, 1, 0):
                near(1, kk)
    emit(dx_out)
    lastq = dkvt.at[1, pl.ds(0, H)]
    lastq[...] = piece(0, zpeer[0])

    finish(1, gk_st)
    fin = [local(gk_st, gkv_out.at[:, cols(m, SEQ)])]
    fin[0].start()
    backs = []
    for peer in (mate, across, diag):
        out, back = remote(gk_st, gkv_out.at[:, cols(m, SEQ)], gkv_out.at[:, cols(peer, SEQ)], "model", peer)
        out.start()
        backs.append(back)

    near(2, 0, last)
    finish(2, go_st)
    fin.append(local(go_st, go_out))
    fin[1].start()
    near(0, 0, lastq)
    finish(0, gq_st)
    fin.append(local(gq_st, gq_out))
    fin[2].start()
    for b in backs:
        b.wait_recv()
    done[1][0].wait()
    for c, out, back in done:
        back.wait_recv()
    for cond, c in sends:
        on(cond, c.wait_send)
    for c in locals_ + fin:
        c.wait()
    for g in range(3):
        for kk in range(SEQS):
            ysend(g, kk).wait_send()
            if kk:
                zsend(g, kk).wait_send()


def copy_kernel(*refs):
    srcs, dsts, bufs, rsem, wsem = refs[:5], refs[5:10], refs[10:15], refs[15], refs[16]
    ins, outs = [], []
    for a in range(5):
        rows = srcs[a].shape[0]
        parts = 8 if a < 2 else 1
        for c in range(parts):
            r = pl.ds(c * (rows // parts), rows // parts)
            i = len(ins)
            ins.append(pltpu.make_async_copy(srcs[a].at[r], bufs[a].at[r], rsem.at[i]))
            outs.append(pltpu.make_async_copy(bufs[a].at[r], dsts[a].at[r], wsem.at[i]))
    for c in ins:
        c.start()
    for i, o in zip(ins, outs):
        i.wait()
        o.start()
    for o in outs:
        o.wait()


def solution(mesh):
    sd = jax.ShapeDtypeStruct
    DMA = pltpu.SemaphoreType.DMA
    VM = pltpu.VMEM
    ANY = pl.BlockSpec(memory_space=pl.ANY)
    IN_VM = pl.BlockSpec(memory_space=pltpu.VMEM)

    def device_step(x, wq, wkv, wo, gain, positions, dy):
        results = [
            sd((TOKS, D), BF), sd((TOKS, D), BF), sd((H, W), BF), sd((H, W), BF), sd((W, H), BF),
        ]
        outs = results + [
            sd((D, D), BF), sd((D, D), BF), sd((CORE, D), BF), sd((CORE, D), BF), sd((TOKS, W), F32),
        ]
        wide, narrow = VM((TOKS, W), BF), VM((TOKS, H), BF)
        scratch = [
            VM((TOKS, D), BF), VM((D, D), BF), VM((D, W), BF), VM((2, D, H), BF), VM((W, D), BF),
            VM((D, W), BF), VM((W, D), BF), wide, narrow, narrow, VM((12, H, SEQ), F32),
            wide, wide, wide, wide, VM((TOKS, W), F32),
            VM((4, W, H), F32), VM((4, W, H), F32), VM((4, W, H), F32),
            VM((4, H, W), F32), VM((4, H, W), F32), VM((4, H, W), F32),
            VM((4, H, SEQ), F32), VM((4, H, SEQ), F32), VM((4, H, SEQ), F32),
            VM((CORE, D), BF), VM((CORE, D), BF), VM((2, W, W), F32),
            VM((W, H), BF), VM((H, W), BF), VM((H, SEQ), BF),
            DMA((48,)), DMA((112,)), DMA((112,)), DMA((3, 8)), DMA((3, 8)), DMA((3,)), DMA((3,)),
        ]
        res = pl.pallas_call(
            layer_kernel,
            name="layer",
            in_specs=[ANY, IN_VM, ANY, ANY, ANY, ANY, IN_VM],
            out_specs=[ANY] * len(outs),
            out_shape=outs,
            scratch_shapes=scratch,
            cost_estimate=pl.CostEstimate(flops=80_000_000_000, bytes_accessed=100_000_000, transcendentals=0),
            compiler_params=pltpu.CompilerParams(collective_id=0, has_side_effects=True, vmem_limit_bytes=67043328),
        )(x, gain.reshape(1, -1), wq, wkv, wo, dy, positions.reshape(1, -1))
        return pl.pallas_call(
            copy_kernel,
            name="emit",
            in_specs=[ANY] * 5,
            out_specs=[ANY] * 5,
            out_shape=results,
            scratch_shapes=[VM(r.shape, r.dtype) for r in results] + [DMA((19,)), DMA((19,))],
            cost_estimate=pl.CostEstimate(flops=1_000_000, bytes_accessed=27_000_000, transcendentals=0),
            compiler_params=pltpu.CompilerParams(vmem_limit_bytes=60 * 2**20),
        )(*res[:5])

    return jax.shard_map(
        device_step,
        mesh=mesh,
        in_specs=(P("data", None), P("data", "model"), P("data", None), P("model", "data"), P(), P(), P("data", None)),
        out_specs=(P("data", None), P("data", None), P("data", "model"), P("data", None), P("model", "data")),
        check_vma=False,
    )
```
